32 devices in a mesh: gx: 2 (over y), gy: 4 (over z), gz: 4 (over x, core).
Axes of the slice: x: 2, y: 2, z: 4, core: 2. Of those that a mesh axis runs over, the one named last changes fastest.
Arguments:
- velocity: float32 [3, 32, 256, 512], P(None, 'gy', 'gx', 'gz'), may hold values from -6 to 6
- stress: float32 [6, 32, 256, 512], P(None, 'gy', 'gx', 'gz'), may hold values from -6 to 6
- buoyancy: float32 [32, 256, 512], P('gy', 'gx', 'gz'), may hold values from 0.5 to 2
- stiff_xx: float32 [32, 256, 512], P('gy', 'gx', 'gz'), may hold values from 2 to 4
- stiff_xz: float32 [32, 256, 512], P('gy', 'gx', 'gz'), may hold values from 0.5 to 1
- stiff_zz: float32 [32, 256, 512], P('gy', 'gx', 'gz'), may hold values from 1.5 to 3
- shear_vert: float32 [32, 256, 512], P('gy', 'gx', 'gz'), may hold values from 0.5 to 1
- shear_horiz: float32 [32, 256, 512], P('gy', 'gx', 'gz'), may hold values from 0.6 to 1.2
- prestress: float32 [2, 32, 512], P(None, 'gy', 'gz'), may hold values from -24 to 24
- fault_mask: int32 [32, 512], P('gy', 'gz'), may hold values 0 or 1
- region_ids: int32 [32, 512], P('gy', 'gz'), may hold values from 0 to 7
- inverse_rate: float32 [32, 512], P('gy', 'gz'), may hold values from 100 to 10000
- slip_prev: float32 [32, 512], P('gy', 'gz'), may hold values from 0.01 to 2
- region_a: float32 [8], replicated, may hold values from 0.01 to 0.04
- region_normal: float32 [8], replicated, may hold values from 20 to 60
Outputs:
- new_velocity: float32 [3, 32, 256, 512], P(None, 'gy', 'gx', 'gz')
- new_stress: float32 [6, 32, 256, 512], P(None, 'gy', 'gx', 'gz')
- slip_rate: float32 [32, 512], P('gy', 'gz')
The draws below stay inside these ranges and needn't reach their ends.
All inputs are finite; a program needn't handle non-finite values. No bound on the sum of `fault_mask` on one device may be relied on, other than what follows from the above.
Results may differ from the reference program's by a relative error of at most 0.0003.
Values sent between devices are 32-bit elements; how exact they have to be, the bound alone decides.
No kernel may reach another device: no remote copies, remote signals or barrier semaphores. Data moves between devices by JAX's collectives and lax.ppermute only.
A program may use at most 128 MiB of HBM per device.

```python
import math
import jax
import jax.numpy as jnp
from jax import lax

STEPS = 3
NEWTON = 3
REGIONS = 8
NY = 32
NX = 256
NZ = 512


def touch_ends(values, key, least, top_value):
    extent = values.shape
    spot = [jax.random.randint(jax.random.fold_in(key, axis), (), 0, extent[axis]) for axis in range(len(extent))]
    values = values.at[tuple(spot)].set(least)
    longest = extent.index(max(extent))
    spot[longest] = (spot[longest] + 1) % extent[longest]
    return values.at[tuple(spot)].set(top_value)


def steps_of(stream_key, dims, cuts, low, largest):
    loudness, own = 1.0, jax.random.fold_in(stream_key, 6)
    for axis_at, parts in cuts:
        heights = jnp.exp(jax.random.uniform(jax.random.fold_in(own, axis_at), (parts,), jnp.float32, low / len(cuts), largest / len(cuts)))
        loudness = loudness * jnp.repeat(heights, dims[axis_at] // parts).reshape([-1 if axis == axis_at else 1 for axis in range(len(dims))])
    return loudness


def noise(key, shape, deviation, reach, cuts=(), held_as=jnp.bfloat16):
    entries = deviation * jax.random.normal(key, shape, jnp.float32)
    if cuts:
        entries = entries * steps_of(key, shape, cuts, -0.22, 0.18)
    return jnp.clip(entries, -reach, reach).astype(held_as)


def setup_inputs(seed: int = 0) -> dict:
    splits = jax.random.split(jax.random.key(seed), 16)
    return {
        "velocity": noise(splits[0], (3, NY, NX, NZ), 1.0, 6.0, ((1, 4), (2, 2), (3, 4)), jnp.float32),
        "stress": noise(splits[1], (6, NY, NX, NZ), 1.0, 6.0, ((1, 4), (2, 2), (3, 4)), jnp.float32),
        "buoyancy": jnp.clip(jnp.exp(math.log(2.0) - 1.3862944 * jax.random.uniform(splits[2], (NY, NX, NZ), jnp.float32) ** steps_of(splits[2], (NY, NX, NZ), ((0, 4), (1, 2), (2, 4)), -0.2, 0.2)), 0.5, 2.0),
        "stiff_xx": jnp.clip(2.0 + 2.0 * jax.random.uniform(splits[3], (NY, NX, NZ), jnp.float32) ** steps_of(splits[3], (NY, NX, NZ), ((0, 4), (1, 2), (2, 4)), -0.2, 0.2), 2.0, 4.0),
        "stiff_xz": jnp.clip(0.5 + 0.5 * jax.random.uniform(splits[4], (NY, NX, NZ), jnp.float32) ** steps_of(splits[4], (NY, NX, NZ), ((0, 4), (1, 2), (2, 4)), -0.2, 0.2), 0.5, 1.0),
        "stiff_zz": jnp.clip(1.5 + 1.5 * jax.random.uniform(splits[5], (NY, NX, NZ), jnp.float32) ** steps_of(splits[5], (NY, NX, NZ), ((0, 4), (1, 2), (2, 4)), -0.2, 0.2), 1.5, 3.0),
        "shear_vert": jnp.clip(0.5 + 0.5 * jax.random.uniform(splits[6], (NY, NX, NZ), jnp.float32) ** steps_of(splits[6], (NY, NX, NZ), ((0, 4), (1, 2), (2, 4)), -0.2, 0.2), 0.5, 1.0),
        "shear_horiz": jnp.clip(0.6 + 0.6 * jax.random.uniform(splits[7], (NY, NX, NZ), jnp.float32) ** steps_of(splits[7], (NY, NX, NZ), ((0, 4), (1, 2), (2, 4)), -0.2, 0.2), 0.6, 1.2),
        "prestress": noise(splits[8], (2, NY, NZ), 6.0, 24.0, ((1, 4), (2, 4)), jnp.float32),
        "fault_mask": touch_ends((jax.random.randint(splits[9], (NY, NZ), 0, 4) < 3).astype(jnp.int32), jax.random.fold_in(splits[9], 1), 0, 1),
        "region_ids": touch_ends(jax.random.randint(splits[10], (NY, NZ), 0, REGIONS), jax.random.fold_in(splits[10], 1), 0, REGIONS - 1).astype(jnp.int32),
        "inverse_rate": jnp.clip(jnp.exp(math.log(10000.0) - 4.6051702 * jax.random.uniform(splits[11], (NY, NZ), jnp.float32) ** steps_of(splits[11], (NY, NZ), ((0, 4), (1, 4)), -0.2, 0.2)), 100.0, 10000.0),
        "slip_prev": jnp.clip(jnp.exp(math.log(2.0) - 5.2983174 * jax.random.uniform(splits[12], (NY, NZ), jnp.float32) ** steps_of(splits[12], (NY, NZ), ((0, 4), (1, 4)), -0.2, 0.2)), 0.01, 2.0),
        "region_a": jnp.clip(jnp.exp(jax.random.uniform(splits[13], (REGIONS,), jnp.float32, math.log(0.01), math.log(0.04))), 0.01, 0.04),
        "region_normal": jnp.clip(jax.random.uniform(splits[14], (REGIONS,), jnp.float32, 20.0, 60.0), 20.0, 60.0),
    }


step_dt = 0.2

def inverse_sinh(values):
    size_abs = jnp.abs(values)
    return jnp.sign(values) * jnp.log(size_abs + jnp.sqrt(size_abs * size_abs + 1.0))

def lower_diff(values, along, mask_cut):
    length = values.shape[along]
    beneath = jnp.concatenate([jnp.zeros_like(lax.slice_in_dim(values, 0, 1, axis=along)), lax.slice_in_dim(values, 0, length - 1, axis=along)], axis=along)
    if mask_cut is not None:
        beneath = beneath * mask_cut
    return values - beneath

def upper_diff(values, along, mask_cut):
    length = values.shape[along]
    overhead = jnp.concatenate([lax.slice_in_dim(values, 1, length, axis=along), jnp.zeros_like(lax.slice_in_dim(values, 0, 1, axis=along))], axis=along)
    if mask_cut is not None:
        overhead = overhead * mask_cut
    return overhead - values

def friction(minus_side, plus_side, minus_buoy, plus_buoy, prestress, fault_mask, region_ids, inverse_rate, slip_prev, region_a, region_normal):
    impedance = 1.0 / (step_dt * (minus_buoy + plus_buoy))
    jump_vec = plus_side - minus_side
    normal_part = impedance * jump_vec[0]
    locked_y = prestress[0] + impedance * jump_vec[1]
    locked_z = prestress[1] + impedance * jump_vec[2]
    magnitude = jnp.sqrt(locked_y * locked_y + locked_z * locked_z + 1.0)
    labels = jnp.arange(region_a.shape[0], dtype=jnp.int32)
    picked = (region_ids[None] == labels[:, None, None]).astype(minus_buoy.dtype)
    strength = lax.optimization_barrier(jnp.sum(picked * region_a[:, None, None], axis=0)) * lax.optimization_barrier(jnp.sum(picked * region_normal[:, None, None], axis=0))
    velocity_slip = slip_prev
    for turn in range(NEWTON):
        scaled = inverse_rate * velocity_slip
        residual = magnitude - impedance * velocity_slip - strength * inverse_sinh(scaled)
        tangent = -impedance - strength * inverse_rate / jnp.sqrt(1.0 + scaled * scaled)
        velocity_slip = velocity_slip - residual / tangent
    velocity_slip = velocity_slip * fault_mask.astype(minus_buoy.dtype)
    retained = 1.0 - impedance * velocity_slip / magnitude
    traction = jnp.stack([normal_part, retained * locked_y - prestress[0], retained * locked_z - prestress[1]])
    return (traction, velocity_slip)

def one_step(velocity, stress, buoyancy, stiff_xx, stiff_xz, stiff_zz, shear_vert, shear_horiz, prestress, fault_mask, region_ids, inverse_rate, slip_prev, region_a, region_normal):
    middle = velocity.shape[2] // 2
    normal_index = jnp.arange(velocity.shape[2], dtype=jnp.int32)[None, :, None]
    cut_lower = (normal_index != middle).astype(velocity.dtype)
    cut_upper = (normal_index != middle - 1).astype(velocity.dtype)
    stress_xx, stress_yy, stress_zz, stress_yz, stress_xz, stress_xy = stress
    trial_x = velocity[0] + step_dt * buoyancy * (lower_diff(stress_xx, 1, cut_lower) + lower_diff(stress_xy, 0, None) + lower_diff(stress_xz, 2, None))
    trial_y = velocity[1] + step_dt * buoyancy * (lower_diff(stress_xy, 1, cut_lower) + lower_diff(stress_yy, 0, None) + lower_diff(stress_yz, 2, None))
    trial_z = velocity[2] + step_dt * buoyancy * (lower_diff(stress_xz, 1, cut_lower) + lower_diff(stress_yz, 0, None) + lower_diff(stress_zz, 2, None))
    trial = jnp.stack([trial_x, trial_y, trial_z])
    minus_buoy = buoyancy[:, middle - 1, :]
    plus_buoy = buoyancy[:, middle, :]
    traction, slip_rate = friction(trial[:, :, middle - 1, :], trial[:, :, middle, :], minus_buoy, plus_buoy, prestress, fault_mask, region_ids, inverse_rate, slip_prev, region_a, region_normal)
    moved = trial.at[:, :, middle - 1, :].add(step_dt * minus_buoy * traction)
    moved = moved.at[:, :, middle, :].add(-(step_dt * plus_buoy * traction))
    moved_x, moved_y, moved_z = moved
    strain_xx = upper_diff(moved_x, 1, cut_upper)
    strain_yy = upper_diff(moved_y, 0, None)
    strain_zz = upper_diff(moved_z, 2, None)
    lame = stiff_xx - 2.0 * shear_horiz
    new_xx = stress_xx + step_dt * (stiff_xx * strain_xx + lame * strain_yy + stiff_xz * strain_zz)
    new_yy = stress_yy + step_dt * (lame * strain_xx + stiff_xx * strain_yy + stiff_xz * strain_zz)
    new_zz = stress_zz + step_dt * (stiff_xz * (strain_xx + strain_yy) + stiff_zz * strain_zz)
    new_yz = stress_yz + step_dt * shear_vert * (upper_diff(moved_y, 2, None) + upper_diff(moved_z, 0, None))
    new_xz = stress_xz + step_dt * shear_vert * (upper_diff(moved_x, 2, None) + upper_diff(moved_z, 1, cut_upper))
    new_xy = stress_xy + step_dt * shear_horiz * (upper_diff(moved_x, 0, None) + upper_diff(moved_y, 1, cut_upper))
    return (moved, jnp.stack([new_xx, new_yy, new_zz, new_yz, new_xz, new_xy]), slip_rate)

def reference(velocity, stress, buoyancy, stiff_xx, stiff_xz, stiff_zz, shear_vert, shear_horiz, prestress, fault_mask, region_ids, inverse_rate, slip_prev, region_a, region_normal):
    slip_rate = slip_prev
    for count in range(STEPS):
        velocity, stress, slip_rate = one_step(velocity, stress, buoyancy, stiff_xx, stiff_xz, stiff_zz, shear_vert, shear_horiz, prestress, fault_mask, region_ids, inverse_rate, slip_rate, region_a, region_normal)
    return (velocity, stress, slip_rate)
```

```python
import functools

import jax
import jax.numpy as jnp
from jax import lax
from jax.experimental import pallas as pl
from jax.experimental.pallas import tpu as pltpu
from jax.sharding import PartitionSpec as P

STEPS = 3
NEWTON = 3
DT = 0.2

PAD = 8
HALO = 3
STRIP = 8

XX, YY, ZZ, YZ, XZ, XY = range(6)
ALONG_Y = (XY, YY, YZ)
B, C11, C13, C33, C44, C66 = range(6)
FIELDS = [("v", c) for c in range(3)] + [("s", c) for c in range(6)] + [("m", c) for c in range(6)]
PRE_Y, PRE_Z, MASK, STRENGTH, RATE, SLIP, OWN_B, OTHER_B = range(8)

VMEM = pltpu.MemorySpace.VMEM
HBM = pltpu.MemorySpace.HBM
SMEM = pltpu.MemorySpace.SMEM


def in_vmem():
    return pl.BlockSpec(memory_space=VMEM)


def in_hbm():
    return pl.BlockSpec(memory_space=HBM)


def in_smem():
    return pl.BlockSpec(memory_space=SMEM)


def roll(values, by):
    by = by % values.shape[-1]
    return values if by == 0 else pltpu.roll(values, by, values.ndim - 1)


def at(ref, field, tile, y, row):
    return ref[field, tile, y, pl.ds(PAD + row, 8), :]


def z_below(pair, lanes):
    one, two = roll(pair[0], 1), roll(pair[1], 1)
    first = lanes == 0
    return jnp.where(first, two, one), jnp.where(first, one, two)


def z_above(pair, lanes):
    one, two = roll(pair[0], -1), roll(pair[1], -1)
    last = lanes == pair[0].shape[-1] - 1
    return jnp.where(last, two, one), jnp.where(last, one, two)


def trial_tile(v, s, m, y, row, below, lanes):
    both = (0, 1)
    behind = {c: z_below([at(s, c, t, y, row) for t in both], lanes) for c in (XZ, YZ, ZZ)}
    out = []
    for t in both:
        own = {c: at(s, c, t, y, row) for c in range(6)}
        lower_x = {c: own[c] - at(s, c, t, y, row - 1) for c in (XX, XY, XZ)}
        if below is None:
            lower_y = {c: own[c] for c in ALONG_Y}
        else:
            lower_y = {c: own[c] - below(c, t) for c in ALONG_Y}
        scale = DT * m[B, t, y, pl.ds(row, 8), :]
        total = (
            lower_x[XX] + lower_y[XY] + (own[XZ] - behind[XZ][t]),
            lower_x[XY] + lower_y[YY] + (own[YZ] - behind[YZ][t]),
            lower_x[XZ] + lower_y[YZ] + (own[ZZ] - behind[ZZ][t]),
        )
        out.append([at(v, c, t, y, row) + scale * total[c] for c in range(3)])
    return out


def stress_tile(v, s, m, y, row, lanes):
    both = (0, 1)
    own = [[at(v, c, t, y, row) for t in both] for c in range(3)]
    ahead = [z_above(own[c], lanes) for c in range(3)]
    for t in both:
        vx, vy, vz = own[0][t], own[1][t], own[2][t]
        over_x = [at(v, c, t, y, row + 1) for c in range(3)]
        over_y = [at(v, c, t, y + 1, row) for c in range(3)]
        exx, eyy, ezz = over_x[0] - vx, over_y[1] - vy, ahead[2][t] - vz
        c11, c13, c33, c44, c66 = (m[k, t, y, pl.ds(row, 8), :] for k in (C11, C13, C33, C44, C66))
        c12 = c11 - 2.0 * c66
        third = c13 * ezz
        change = {
            XX: c11 * exx + c12 * eyy + third,
            YY: c12 * exx + c11 * eyy + third,
            ZZ: c13 * (exx + eyy) + c33 * ezz,
            YZ: c44 * ((ahead[1][t] - vy) + (over_y[2] - vz)),
            XZ: c44 * ((ahead[0][t] - vx) + (over_x[2] - vz)),
            XY: c66 * ((over_y[0] - vx) + (over_x[1] - vy)),
        }
        for c, gain in change.items():
            s[c, t, y, pl.ds(PAD + row, 8), :] = at(s, c, t, y, row) + DT * gain


def lane_index(like):
    return lax.broadcasted_iota(jnp.int32, like, len(like) - 1)


def strip_pack(pieces, eighths):
    packed = jnp.zeros_like(pieces[0])
    for k, piece in enumerate(pieces):
        packed = jnp.where(eighths == k, roll(piece, STRIP * k + HALO), packed)
    return packed


def strip_take(packed, k):
    return roll(packed, -(STRIP * k + HALO))


def field_ref(kind, v, s, m):
    return {"v": v, "s": s, "m": m}[kind]


def slot_of(index, width):
    per_plane = (width - 5) // HALO
    return index // per_plane, index % per_plane


def z_slots(ny, width):
    slots = {}
    for f in range(len(FIELDS)):
        for y in range(ny):
            slots[f, y] = slot_of(f * ny + y, width)
    return slots, 1 + max(p for p, _ in slots.values())


def load_kernel(
    flags,
    region_a,
    region_normal,
    ids,
    mask,
    inverse_rate,
    slip,
    prestress,
    thirds,
    velocity,
    stress,
    *rest,
):
    raw_m = rest[:6]
    v, s, m, fault, z_a, z_b = rest[6:12]
    sems = rest[12]
    ny, nx, width = velocity.shape[1:]
    copies = []
    for c in range(3):
        copies.append((velocity.at[c], v.at[c, 0, pl.ds(0, ny), pl.ds(PAD, nx), :]))
    for c in range(6):
        copies.append((stress.at[c], s.at[c, 0, :, pl.ds(PAD, nx), :]))
    for c in range(6):
        copies.append((raw_m[c], m.at[c, 0]))
    copies = [pltpu.make_async_copy(a, b, sems.at[k]) for k, (a, b) in enumerate(copies)]
    for copy in copies:
        copy.start()
    zeros = jnp.zeros((PAD, width), jnp.float32)
    for t in range(2):
        for y in range(ny):
            for c in (XX, XY, XZ):
                s[c, t, y, 0:PAD, :] = zeros
            for c in range(3):
                v[c, t, y, PAD + nx : PAD + nx + PAD, :] = zeros
    kinds = ids[...]
    a_part = jnp.zeros((ny, width), jnp.float32)
    n_part = jnp.zeros((ny, width), jnp.float32)
    for k in range(region_a.shape[0]):
        a_part = jnp.where(kinds == k, region_a[k], a_part)
        n_part = jnp.where(kinds == k, region_normal[k], n_part)
    fault[PRE_Y, 0, 0:ny, :] = prestress[0]
    fault[PRE_Z, 0, 0:ny, :] = prestress[1]
    fault[MASK, 0, 0:ny, :] = mask[...].astype(jnp.float32)
    fault[STRENGTH, 0, 0:ny, :] = a_part * n_part
    fault[RATE, 0, 0:ny, :] = inverse_rate[...]
    fault[SLIP, 0, 0:ny, :] = slip[...]
    for copy in copies:
        copy.wait()

    slots, planes = z_slots(ny, width)
    odd = flags[2] == 1

    def emit(pieces, row):
        group = thirds[...]
        up = [jnp.zeros((8, width), jnp.float32) for _ in range(planes)]
        down = [jnp.zeros((8, width), jnp.float32) for _ in range(planes)]
        for plane, pos, piece in pieces:
            moved = roll(piece, HALO * pos + HALO)
            up[plane] = jnp.where(group == pos, moved, up[plane])
            down[plane] = jnp.where(group == pos + 1, moved, down[plane])
        for plane in range(planes):
            z_a[plane, pl.ds(row, 8), :] = jnp.where(odd, down[plane], up[plane])
            z_b[plane, pl.ds(row, 8), :] = jnp.where(odd, up[plane], down[plane])

    def pack(i, carry):
        row = pl.multiple_of(i * 8, 8)
        pieces = []
        for f, (kind, c) in enumerate(FIELDS):
            shift = 0 if kind == "m" else PAD
            for y in range(ny):
                ref = field_ref(kind, v, s, m)
                pieces.append((*slots[f, y], ref[c, 0, y, pl.ds(row + shift, 8), :]))
        emit(pieces, row)
        return carry

    lax.fori_loop(0, nx // 8, pack, 0)
    emit([(0, k, fault[k, 0, 0:8, :]) for k in range(6)], nx)


def write_messages(v, s, eighths, odd, row, y_a, y_b, extra):
    last = s.shape[2] - 1
    up = [at(s, c, 0, last, row) for c in ALONG_Y]
    down = [at(v, c, 0, 0, row) for c in range(3)]
    up_strip = [at(s, c, 1, last, row) for c in ALONG_Y]
    down_strip = [at(v, c, 1, 0, row) for c in range(3)]
    if extra is not None:
        both = extra[B, 0, 0, pl.ds(row, 8), :]
        up.append(both)
        down.append(both)
        both = extra[B, 1, 0, pl.ds(row, 8), :]
        up_strip.append(both)
        down_strip.append(both)
    up.append(strip_pack(up_strip, eighths))
    down.append(strip_pack(down_strip, eighths))
    for k in range(len(up)):
        y_a[k, pl.ds(row, 8), :] = jnp.where(odd, down[k], up[k])
        y_b[k, pl.ds(row, 8), :] = jnp.where(odd, up[k], down[k])


def partial_trials(v, s, m, nx, lanes):
    for row in range(0, nx, 8):
        new = trial_tile(v, s, m, 0, row, None, lanes)
        for t in range(2):
            for c in range(3):
                v[c, t, 0, pl.ds(PAD + row, 8), :] = new[t][c]


def widen_kernel(flags, thirds, eighths, r_a, r_b, v_in, s_in, m_in, f_in, v, s, m, fault, y_a, y_b):
    ny, nx, width = m.shape[2:]
    slots, planes = z_slots(ny, width)
    odd_z, odd_y = flags[2] == 1, flags[1] == 1
    lanes = lane_index((8, width))

    def take(row, wanted):
        group = thirds[...]
        from_a = [r_a[p, pl.ds(row, 8), :] for p in range(planes)]
        from_b = [r_b[p, pl.ds(row, 8), :] for p in range(planes)]
        low = [jnp.where(odd_z, a, b) for a, b in zip(from_a, from_b)]
        high = [jnp.where(odd_z, b, a) for a, b in zip(from_a, from_b)]
        for (plane, pos), store in wanted:
            store(roll(jnp.where(group == pos, low[plane], high[plane]), -(HALO * pos + HALO)))

    def unpack(i, carry):
        row = pl.multiple_of(i * 8, 8)

        def store_to(ref, c, y, shift):
            def store(value):
                ref[c, 1, y, pl.ds(row + shift, 8), :] = value

            return store

        wanted = []
        for f, (kind, c) in enumerate(FIELDS):
            shift = 0 if kind == "m" else PAD
            for y in range(ny):
                wanted.append((slots[f, y], store_to(field_ref(kind, v, s, m), c, y, shift)))
        take(row, wanted)
        return carry

    lax.fori_loop(0, nx // 8, unpack, 0)

    def store_fault(k):
        def store(value):
            fault[k, 1, 0:8, :] = value

        return store

    take(nx, [((0, k), store_fault(k)) for k in range(6)])
    partial_trials(v, s, m, nx, lanes)
    for row in range(0, nx, 8):
        write_messages(v, s, eighths[...], odd_y, row, y_a, y_b, m)
    for k in range(6):
        for t in range(2):
            line = fault[k, t, 0:1, :]
            y_a[t, nx + k : nx + k + 1, :] = line
            y_b[t, nx + k : nx + k + 1, :] = line


def inner_kernel(s_in, v_in, m, v, s):
    ny, nx, width = m.shape[2:]
    lanes = lane_index((8, width))

    def trials(y, carry):
        for row in range(0, nx, 8):
            new = trial_tile(
                v, s, m, y, row, lambda c, t, row=row: at(s, c, t, y - 1, row), lanes
            )
            for t in range(2):
                for c in range(3):
                    v[c, t, y, pl.ds(PAD + row, 8), :] = new[t][c]
        return carry

    lax.fori_loop(1, ny, trials, 0)

    def stresses(y, carry):
        for row in range(8, nx - 8, 8):
            stress_tile(v, s, m, y, row, lanes)
        return carry

    lax.fori_loop(1, ny - 1, stresses, 0)


def finish_kernel(first, flags, eighths, r_a, r_b, s, m, *rest):
    if first:
        v_in, f_in, v, fault, ahead_b, f_msg, rows = rest
    else:
        v_in, ahead_b, v, f_msg, rows = rest
    ny, nx, width = m.shape[2:]
    minus, odd = flags[0] == 0, flags[1] == 1
    n = 4 if first else 3

    if first:
        for t in range(2):
            line = jnp.where(odd, r_b[t, nx : nx + 8, :], r_a[t, nx : nx + 8, :])
            for k in range(6):
                fault[k, t, ny : ny + 1, :] = line[k : k + 1, :]
    for row in range(0, nx, 8):
        from_a = [r_a[k, pl.ds(row, 8), :] for k in range(n + 1)]
        from_b = [r_b[k, pl.ds(row, 8), :] for k in range(n + 1)]
        low = [jnp.where(odd, a, b) for a, b in zip(from_a, from_b)]
        high = [jnp.where(odd, b, a) for a, b in zip(from_a, from_b)]
        if first:
            ahead_b[0, pl.ds(row, 8), :] = high[3]
            ahead_b[1, pl.ds(row, 8), :] = strip_take(high[n], 3)
        for t in range(2):
            scale = DT * m[B, t, 0, pl.ds(row, 8), :]
            scale_ahead = DT * ahead_b[t, pl.ds(row, 8), :]
            for c in range(3):
                low_c = low[c] if t == 0 else strip_take(low[n], c)
                high_c = high[c] if t == 0 else strip_take(high[n], c)
                v[c, t, 0, pl.ds(PAD + row, 8), :] = at(v, c, t, 0, row) - scale * low_c
                v[c, t, ny, pl.ds(PAD + row, 8), :] = high_c - scale_ahead * at(
                    s, ALONG_Y[c], t, ny - 1, row
                )
    f_msg[...] = jnp.zeros_like(f_msg)
    rows[...] = jnp.zeros_like(rows)
    for c in range(3):
        for y in range(ny + 1):
            for t in range(2):
                line = jnp.where(
                    minus,
                    v[c, t, y, PAD + nx - 1 : PAD + nx, :],
                    v[c, t, y, PAD : PAD + 1, :],
                )
                if t == 0:
                    f_msg[c, y : y + 1, :] = line
                else:
                    rows[c, y : y + 1, :] = line
    if first:
        for t in range(2):
            for y in range(ny + 1):
                if y < ny:
                    line = jnp.where(minus, m[B, t, y, nx - 1 : nx, :], m[B, t, y, 0:1, :])
                else:
                    line = jnp.where(minus, ahead_b[t, nx - 1 : nx, :], ahead_b[t, 0:1, :])
                fault[OWN_B, t, y : y + 1, :] = line
                if t == 0:
                    f_msg[3, y : y + 1, :] = line
                else:
                    rows[3, y : y + 1, :] = line
    for half in range(0, f_msg.shape[1], 8):
        f_msg[n, half : half + 8, :] = strip_pack(
            [rows[k, half : half + 8, :] for k in range(n)], eighths[...]
        )


def rim_kernel(v, m, s_in, s):
    ny, nx, width = m.shape[2:]
    lanes = lane_index((8, width))

    def planes(i, carry):
        for row in range(8, nx - 8, 8):
            stress_tile(v, s, m, i * (ny - 1), row, lanes)
        return carry

    lax.fori_loop(0, 2, planes, 0)


def inverse_sinh(values):
    size = jnp.abs(values)
    sign = jnp.where(values > 0.0, 1.0, jnp.where(values < 0.0, -1.0, 0.0))
    return sign * jnp.log(size + jnp.sqrt(size * size + 1.0))


def friction(minus_side, plus_side, minus_b, plus_b, par):
    total = DT * (minus_b + plus_b)
    impedance = 1.0 / jnp.where(total > 0.0, total, 1.0)
    jump = [p - q for p, q in zip(plus_side, minus_side)]
    locked_y = par[PRE_Y] + impedance * jump[1]
    locked_z = par[PRE_Z] + impedance * jump[2]
    magnitude = jnp.sqrt(locked_y * locked_y + locked_z * locked_z + 1.0)
    rate, strength, slip = par[RATE], par[STRENGTH], par[SLIP]
    for _ in range(NEWTON):
        scaled = rate * slip
        residual = magnitude - impedance * slip - strength * inverse_sinh(scaled)
        tangent = -impedance - strength * rate / jnp.sqrt(1.0 + scaled * scaled)
        slip = slip - residual / tangent
    slip = slip * par[MASK]
    retained = 1.0 - impedance * slip / magnitude
    traction = (
        impedance * jump[0],
        retained * locked_y - par[PRE_Y],
        retained * locked_z - par[PRE_Z],
    )
    return traction, slip


def fault_kernel(first, final, flags, eighths, f_own, f_other, m, *rest):
    v_in, s_in, fault_in, v, s, fault = rest[:6]
    if final:
        new_v, new_s, slip_out, rows, sems = rest[6:]
    else:
        y_a, y_b, rows = rest[6:]
    ny, nx, width = m.shape[2:]
    minus, odd = flags[0] == 0, flags[1] == 1
    lanes = lane_index((8, width))
    n = 4 if first else 3
    high = f_own.shape[1]
    sign = jnp.where(minus, DT, -DT)
    for t in range(2):
        for half in range(0, high, 8):
            span = slice(half, half + 8)

            def piece(ref, k):
                return ref[k, span, :] if t == 0 else strip_take(ref[n, span, :], k)

            if first:
                fault[OTHER_B, t, span, :] = piece(f_other, 3)
            own = [piece(f_own, c) for c in range(3)]
            other = [piece(f_other, c) for c in range(3)]
            par = [fault[k, t, span, :] for k in range(8)]
            m_side = [jnp.where(minus, a, b) for a, b in zip(own, other)]
            p_side = [jnp.where(minus, b, a) for a, b in zip(own, other)]
            m_b = jnp.where(minus, par[OWN_B], par[OTHER_B])
            p_b = jnp.where(minus, par[OTHER_B], par[OWN_B])
            traction, slip = friction(m_side, p_side, m_b, p_b, par)
            fault[SLIP, t, span, :] = slip
            for c in range(3):
                rows[c, t, span, :] = own[c] + sign * par[OWN_B] * traction[c]
    for side, row in ((0, PAD + nx - 1), (1, PAD)):

        @pl.when(flags[0] == side)
        def _(row=row):
            for c in range(3):
                for t in range(2):
                    for y in range(ny + 1):
                        v[c, t, y, row : row + 1, :] = rows[c, t, y : y + 1, :]

    def ends(y, carry):
        for row in (0, nx - 8):
            stress_tile(v, s, m, y, row, lanes)
        return carry

    lax.fori_loop(0, ny, ends, 0)
    if final:
        slip_out[...] = fault[SLIP, 0, 0:ny, :]
        copies = []
        for c in range(3):
            copies.append((v.at[c, 0, pl.ds(0, ny), pl.ds(PAD, nx), :], new_v.at[c]))
        for c in range(6):
            copies.append((s.at[c, 0, :, pl.ds(PAD, nx), :], new_s.at[c]))
        copies = [pltpu.make_async_copy(a, b, sems.at[k]) for k, (a, b) in enumerate(copies)]
        for copy in copies:
            copy.start()
        for copy in copies:
            copy.wait()
    else:
        partial_trials(v, s, m, nx, lanes)
        for row in range(0, nx, 8):
            write_messages(v, s, eighths[...], odd, row, y_a, y_b, None)


def f32(*shape):
    return VMEM(shape, jnp.float32)


def call(kernel, name, outs, in_specs, aliases, scratch=(), flops=0, out_specs=None):
    return pl.pallas_call(
        kernel,
        out_shape=tuple(outs),
        in_specs=in_specs,
        out_specs=tuple(out_specs or [in_vmem() for _ in outs]),
        input_output_aliases=aliases,
        scratch_shapes=list(scratch),
        compiler_params=pltpu.CompilerParams(vmem_limit_bytes=8 << 20),
        cost_estimate=pl.CostEstimate(flops=flops, bytes_accessed=0, transcendentals=0),
        name=name,
    )


def pair_swaps(a, b, axis):
    size = lax.axis_size(axis)
    out = []
    for value, start in ((a, 0), (b, 1)):
        pairs = []
        for i in range(start, size - 1, 2):
            pairs += [(i, i + 1), (i + 1, i)]
        out.append(lax.ppermute(value, axis, pairs))
    return out


def local(
    velocity,
    stress,
    buoyancy,
    stiff_xx,
    stiff_xz,
    stiff_zz,
    shear_vert,
    shear_horiz,
    prestress,
    fault_mask,
    region_ids,
    inverse_rate,
    slip_prev,
    region_a,
    region_normal,
):
    ny, nx, width = buoyancy.shape
    across, along, dip = (lax.axis_index(k) for k in ("gx", "gy", "gz"))
    flags = jnp.stack([across, along % 2, dip % 2]).astype(jnp.int32)
    lanes = jnp.broadcast_to(jnp.arange(width, dtype=jnp.int32), (8, width))
    thirds, eighths = lanes // HALO, lanes // STRIP
    rows = nx + 2 * PAD
    high = 8 * ((ny + 1 + 7) // 8)
    v_shape = f32(3, 2, ny + 1, rows, width)
    s_shape = f32(6, 2, ny, rows, width)
    m_shape = f32(6, 2, ny, nx, width)
    fault_shape = f32(8, 2, high, width)
    planes = z_slots(ny, width)[1]
    z_shape = f32(planes, nx + 8, width)
    unit = ny * nx * width
    vm, hb, sm = in_vmem(), in_hbm(), in_smem()

    v, s, m, fault, z_a, z_b = call(
        load_kernel,
        "load",
        (v_shape, s_shape, m_shape, fault_shape, z_shape, z_shape),
        [sm, sm, sm, vm, vm, vm, vm, vm, vm] + [hb] * 8,
        {},
        [pltpu.SemaphoreType.DMA((15,))],
        flops=100 * unit,
    )(
        flags,
        region_a,
        region_normal,
        region_ids,
        fault_mask,
        inverse_rate,
        slip_prev,
        prestress,
        thirds,
        velocity,
        stress,
        buoyancy,
        stiff_xx,
        stiff_xz,
        stiff_zz,
        shear_vert,
        shear_horiz,
    )
    z_a, z_b = pair_swaps(z_a, z_b, "gz")
    y_shape = f32(5, nx + 8, width)
    v, s, m, fault, y_a, y_b = call(
        widen_kernel,
        "widen",
        (v_shape, s_shape, m_shape, fault_shape, y_shape, y_shape),
        [sm] + [vm] * 8,
        {5: 0, 6: 1, 7: 2, 8: 3},
        flops=50 * unit,
    )(flags, thirds, eighths, z_a, z_b, v, s, m, fault)
    y_shape = f32(4, nx, width)
    ahead_b = None
    for step in range(STEPS):
        first, final = step == 0, step == STEPS - 1
        y_a, y_b = pair_swaps(y_a, y_b, "gy")
        v, s = call(
            inner_kernel, "inner", (v_shape, s_shape), [vm] * 3, {1: 0, 0: 1}, flops=200 * unit
        )(s, v, m)
        f_shape = f32(5 if first else 4, high, width)
        scratch = [pltpu.VMEM((4, high, width), jnp.float32)]
        if first:
            v, fault, ahead_b, f_own = call(
                functools.partial(finish_kernel, True),
                "finish",
                (v_shape, fault_shape, f32(2, nx, width), f_shape),
                [sm] + [vm] * 7,
                {6: 0, 7: 1},
                scratch,
                flops=unit,
            )(flags, eighths, y_a, y_b, s, m, v, fault)
        else:
            v, f_own = call(
                functools.partial(finish_kernel, False),
                "finish",
                (v_shape, f_shape),
                [sm] + [vm] * 7,
                {6: 0},
                scratch,
                flops=unit,
            )(flags, eighths, y_a, y_b, s, m, v, ahead_b)
        f_other = lax.ppermute(f_own, "gx", [(i, i ^ 1) for i in range(lax.axis_size("gx"))])
        (s,) = call(rim_kernel, "rim", (s_shape,), [vm] * 3, {2: 0}, flops=50 * unit)(v, m, s)
        outs = [v_shape, s_shape, fault_shape]
        specs = [vm, vm, vm]
        scratch = [pltpu.VMEM((3, 2, high, width), jnp.float32)]
        if final:
            outs += [
                jax.ShapeDtypeStruct((3, ny, nx, width), jnp.float32),
                jax.ShapeDtypeStruct((6, ny, nx, width), jnp.float32),
                jax.ShapeDtypeStruct((ny, width), jnp.float32),
            ]
            specs += [hb, hb, vm]
            scratch.append(pltpu.SemaphoreType.DMA((9,)))
        else:
            outs += [y_shape, y_shape]
            specs += [vm, vm]
        v, s, fault, *more = call(
            functools.partial(fault_kernel, first, final),
            "fault",
            outs,
            [sm] + [vm] * 7,
            {5: 0, 6: 1, 7: 2},
            scratch,
            flops=50 * unit,
            out_specs=specs,
        )(flags, eighths, f_own, f_other, m, v, s, fault)
        if final:
            return tuple(more)
        y_a, y_b = more


def solution(mesh):
    in_specs = (
        P(None, "gy", "gx", "gz"),
        P(None, "gy", "gx", "gz"),
        P("gy", "gx", "gz"),
        P("gy", "gx", "gz"),
        P("gy", "gx", "gz"),
        P("gy", "gx", "gz"),
        P("gy", "gx", "gz"),
        P("gy", "gx", "gz"),
        P(None, "gy", "gz"),
        P("gy", "gz"),
        P("gy", "gz"),
        P("gy", "gz"),
        P("gy", "gz"),
        P(),
        P(),
    )
    out_specs = (P(None, "gy", "gx", "gz"), P(None, "gy", "gx", "gz"), P("gy", "gz"))
    return jax.shard_map(local, mesh=mesh, in_specs=in_specs, out_specs=out_specs, check_vma=False)
```

```python
import functools

import jax
import jax.numpy as jnp
from jax import lax
from jax.experimental import pallas as pl
from jax.experimental.pallas import tpu as pltpu
from jax.sharding import PartitionSpec as P

STEPS = 3
NEWTON = 3
DT = 0.2

PAD = 8
HALO = 3
STRIP = 8

XX, YY, ZZ, YZ, XZ, XY = range(6)
ALONG_Y = (XY, YY, YZ)
B, C11, C13, C33, C44, C66 = range(6)
FIELDS = [("v", c) for c in range(3)] + [("s", c) for c in range(6)] + [("m", c) for c in range(6)]
PRE_Y, PRE_Z, MASK, STRENGTH, RATE, SLIP, OWN_B, OTHER_B = range(8)

VMEM = pltpu.MemorySpace.VMEM
HBM = pltpu.MemorySpace.HBM
SMEM = pltpu.MemorySpace.SMEM


def in_vmem():
    return pl.BlockSpec(memory_space=VMEM)


def in_hbm():
    return pl.BlockSpec(memory_space=HBM)


def in_smem():
    return pl.BlockSpec(memory_space=SMEM)


def roll(values, by):
    by = by % values.shape[-1]
    return values if by == 0 else pltpu.roll(values, by, values.ndim - 1)


def at(ref, field, tile, y, row):
    return ref[field, tile, y, pl.ds(PAD + row, 8), :]


def z_below(pair, lanes):
    one, two = roll(pair[0], 1), roll(pair[1], 1)
    first = lanes == 0
    return jnp.where(first, two, one), jnp.where(first, one, two)


def z_above(pair, lanes):
    one, two = roll(pair[0], -1), roll(pair[1], -1)
    last = lanes == pair[0].shape[-1] - 1
    return jnp.where(last, two, one), jnp.where(last, one, two)


def trial_tile(v, s, m, y, row, below, lanes):
    both = (0, 1)
    behind = {c: z_below([at(s, c, t, y, row) for t in both], lanes) for c in (XZ, YZ, ZZ)}
    out = []
    for t in both:
        own = {c: at(s, c, t, y, row) for c in range(6)}
        lower_x = {c: own[c] - at(s, c, t, y, row - 1) for c in (XX, XY, XZ)}
        if below is None:
            lower_y = {c: own[c] for c in ALONG_Y}
        else:
            lower_y = {c: own[c] - below(c, t) for c in ALONG_Y}
        scale = DT * m[B, t, y, pl.ds(row, 8), :]
        total = (
            lower_x[XX] + lower_y[XY] + (own[XZ] - behind[XZ][t]),
            lower_x[XY] + lower_y[YY] + (own[YZ] - behind[YZ][t]),
            lower_x[XZ] + lower_y[YZ] + (own[ZZ] - behind[ZZ][t]),
        )
        out.append([at(v, c, t, y, row) + scale * total[c] for c in range(3)])
    return out


def stress_tile(v, s, m, y, row, lanes):
    both = (0, 1)
    own = [[at(v, c, t, y, row) for t in both] for c in range(3)]
    ahead = [z_above(own[c], lanes) for c in range(3)]
    for t in both:
        vx, vy, vz = own[0][t], own[1][t], own[2][t]
        over_x = [at(v, c, t, y, row + 1) for c in range(3)]
        over_y = [at(v, c, t, y + 1, row) for c in range(3)]
        exx, eyy, ezz = over_x[0] - vx, over_y[1] - vy, ahead[2][t] - vz
        c11, c13, c33, c44, c66 = (m[k, t, y, pl.ds(row, 8), :] for k in (C11, C13, C33, C44, C66))
        c12 = c11 - 2.0 * c66
        third = c13 * ezz
        change = {
            XX: c11 * exx + c12 * eyy + third,
            YY: c12 * exx + c11 * eyy + third,
            ZZ: c13 * (exx + eyy) + c33 * ezz,
            YZ: c44 * ((ahead[1][t] - vy) + (over_y[2] - vz)),
            XZ: c44 * ((ahead[0][t] - vx) + (over_x[2] - vz)),
            XY: c66 * ((over_y[0] - vx) + (over_x[1] - vy)),
        }
        for c, gain in change.items():
            s[c, t, y, pl.ds(PAD + row, 8), :] = at(s, c, t, y, row) + DT * gain


def lane_index(like):
    return lax.broadcasted_iota(jnp.int32, like, len(like) - 1)


def strip_pack(pieces, eighths):
    packed = jnp.zeros_like(pieces[0])
    for k, piece in enumerate(pieces):
        packed = jnp.where(eighths == k, roll(piece, STRIP * k + HALO), packed)
    return packed


def strip_take(packed, k):
    return roll(packed, -(STRIP * k + HALO))


def field_ref(kind, v, s, m):
    return {"v": v, "s": s, "m": m}[kind]


def fields_per_plane(ny, width):
    return (width - 5) // HALO // ny


def z_slots(ny, width):
    per_plane = fields_per_plane(ny, width)
    slots = {}
    for f in range(len(FIELDS)):
        for y in range(ny):
            slots[f, y] = (f // per_plane, f % per_plane * ny + y)
    return slots, -(-len(FIELDS) // per_plane)


def load_kernel(
    flags,
    thirds,
    velocity,
    stress,
    *rest,
):
    raw_m, small = rest[:6], rest[6:13]
    v, s, m, fault, z_a, z_b = rest[13:19]
    pre, ids, mask, rate, slip, region_a, region_normal, sems = rest[19:]
    ny, nx, width = velocity.shape[1:]
    big = {}
    for c in range(3):
        big["v", c] = (velocity.at[c], v.at[c, 0, pl.ds(0, ny), pl.ds(PAD, nx), :])
    for c in range(6):
        big["s", c] = (stress.at[c], s.at[c, 0, :, pl.ds(PAD, nx), :])
    for c in range(6):
        big["m", c] = (raw_m[c], m.at[c, 0])
    big = {
        key: pltpu.make_async_copy(a, b, sems.at[k]) for k, (key, (a, b)) in enumerate(big.items())
    }
    held = (pre, ids, mask, rate, slip, region_a, region_normal)
    little = [
        pltpu.make_async_copy(a, b, sems.at[len(big) + k])
        for k, (a, b) in enumerate(zip(small, held))
    ]
    for copy in big.values():
        copy.start()
    for copy in little:
        copy.start()
    zeros = jnp.zeros((PAD, width), jnp.float32)
    for t in range(2):
        for y in range(ny):
            for c in (XX, XY, XZ):
                s[c, t, y, 0:PAD, :] = zeros
            for c in range(3):
                v[c, t, y, PAD + nx : PAD + nx + PAD, :] = zeros

    slots, planes = z_slots(ny, width)
    odd = flags[2] == 1
    per_plane = fields_per_plane(ny, width)

    def emit(pieces, plane, row):
        group = thirds[...]
        up = jnp.zeros((8, width), jnp.float32)
        down = jnp.zeros((8, width), jnp.float32)
        for pos, piece in pieces:
            moved = roll(piece, HALO * pos + HALO)
            up = jnp.where(group == pos, moved, up)
            down = jnp.where(group == pos + 1, moved, down)
        z_a[plane, pl.ds(row, 8), :] = jnp.where(odd, down, up)
        z_b[plane, pl.ds(row, 8), :] = jnp.where(odd, up, down)

    for plane in range(planes):
        chosen = FIELDS[plane * per_plane : (plane + 1) * per_plane]
        for key in chosen:
            big[key].wait()

        def pack(i, carry, plane=plane, chosen=chosen):
            row = pl.multiple_of(i * 8, 8)
            pieces = []
            for f, (kind, c) in enumerate(chosen):
                shift = 0 if kind == "m" else PAD
                ref = field_ref(kind, v, s, m)
                for y in range(ny):
                    pieces.append((f * ny + y, ref[c, 0, y, pl.ds(row + shift, 8), :]))
            emit(pieces, plane, row)
            return carry

        lax.fori_loop(0, nx // 8, pack, 0)
    for copy in little:
        copy.wait()
    kinds = ids[...]
    a_part = jnp.zeros((ny, width), jnp.float32)
    n_part = jnp.zeros((ny, width), jnp.float32)
    for k in range(region_a.shape[0]):
        a_part = jnp.where(kinds == k, region_a[k], a_part)
        n_part = jnp.where(kinds == k, region_normal[k], n_part)
    fault[PRE_Y, 0, 0:ny, :] = pre[0]
    fault[PRE_Z, 0, 0:ny, :] = pre[1]
    fault[MASK, 0, 0:ny, :] = mask[...].astype(jnp.float32)
    fault[STRENGTH, 0, 0:ny, :] = a_part * n_part
    fault[RATE, 0, 0:ny, :] = rate[...]
    fault[SLIP, 0, 0:ny, :] = slip[...]
    emit([(k, fault[k, 0, 0:8, :]) for k in range(6)], 0, nx)
    for plane in range(1, planes):
        z_a[plane, pl.ds(nx, 8), :] = zeros
        z_b[plane, pl.ds(nx, 8), :] = zeros


def write_messages(v, s, eighths, odd, row, y_a, y_b, extra):
    last = s.shape[2] - 1
    up = [at(s, c, 0, last, row) for c in ALONG_Y]
    down = [at(v, c, 0, 0, row) for c in range(3)]
    up_strip = [at(s, c, 1, last, row) for c in ALONG_Y]
    down_strip = [at(v, c, 1, 0, row) for c in range(3)]
    if extra is not None:
        both = extra[B, 0, 0, pl.ds(row, 8), :]
        up.append(both)
        down.append(both)
        both = extra[B, 1, 0, pl.ds(row, 8), :]
        up_strip.append(both)
        down_strip.append(both)
    up.append(strip_pack(up_strip, eighths))
    down.append(strip_pack(down_strip, eighths))
    for k in range(len(up)):
        y_a[k, pl.ds(row, 8), :] = jnp.where(odd, down[k], up[k])
        y_b[k, pl.ds(row, 8), :] = jnp.where(odd, up[k], down[k])


def partial_trials(v, s, m, nx, lanes):
    for row in range(0, nx, 8):
        new = trial_tile(v, s, m, 0, row, None, lanes)
        for t in range(2):
            for c in range(3):
                v[c, t, 0, pl.ds(PAD + row, 8), :] = new[t][c]


def widen_kernel(flags, thirds, eighths, r_a, r_b, v_in, s_in, m_in, f_in, v, s, m, fault, y_a, y_b):
    ny, nx, width = m.shape[2:]
    slots, planes = z_slots(ny, width)
    odd_z, odd_y = flags[2] == 1, flags[1] == 1
    lanes = lane_index((8, width))

    def take(row, wanted):
        group = thirds[...]
        from_a = [r_a[p, pl.ds(row, 8), :] for p in range(planes)]
        from_b = [r_b[p, pl.ds(row, 8), :] for p in range(planes)]
        low = [jnp.where(odd_z, a, b) for a, b in zip(from_a, from_b)]
        high = [jnp.where(odd_z, b, a) for a, b in zip(from_a, from_b)]
        for (plane, pos), store in wanted:
            store(roll(jnp.where(group == pos, low[plane], high[plane]), -(HALO * pos + HALO)))

    def unpack(i, carry):
        row = pl.multiple_of(i * 8, 8)

        def store_to(ref, c, y, shift):
            def store(value):
                ref[c, 1, y, pl.ds(row + shift, 8), :] = value

            return store

        wanted = []
        for f, (kind, c) in enumerate(FIELDS):
            shift = 0 if kind == "m" else PAD
            for y in range(ny):
                wanted.append((slots[f, y], store_to(field_ref(kind, v, s, m), c, y, shift)))
        take(row, wanted)
        return carry

    lax.fori_loop(0, nx // 8, unpack, 0)

    def store_fault(k):
        def store(value):
            fault[k, 1, 0:8, :] = value

        return store

    take(nx, [((0, k), store_fault(k)) for k in range(6)])
    partial_trials(v, s, m, nx, lanes)
    for row in range(0, nx, 8):
        write_messages(v, s, eighths[...], odd_y, row, y_a, y_b, m)
    for k in range(6):
        for t in range(2):
            line = fault[k, t, 0:1, :]
            y_a[t, nx + k : nx + k + 1, :] = line
            y_b[t, nx + k : nx + k + 1, :] = line


def inner_kernel(s_in, v_in, m, v, s):
    ny, nx, width = m.shape[2:]
    lanes = lane_index((8, width))

    def trials(y, carry):
        for row in range(0, nx, 8):
            new = trial_tile(
                v, s, m, y, row, lambda c, t, row=row: at(s, c, t, y - 1, row), lanes
            )
            for t in range(2):
                for c in range(3):
                    v[c, t, y, pl.ds(PAD + row, 8), :] = new[t][c]
        return carry

    lax.fori_loop(1, ny, trials, 0)

    def stresses(y, carry):
        for row in range(8, nx - 8, 8):
            stress_tile(v, s, m, y, row, lanes)
        return carry

    lax.fori_loop(1, ny - 1, stresses, 0)


def finish_kernel(first, flags, eighths, r_a, r_b, s, m, *rest):
    if first:
        v_in, f_in, v, fault, ahead_b, f_msg, rows = rest
    else:
        v_in, ahead_b, v, f_msg, rows = rest
    ny, nx, width = m.shape[2:]
    minus, odd = flags[0] == 0, flags[1] == 1
    n = 4 if first else 3

    if first:
        for t in range(2):
            line = jnp.where(odd, r_b[t, nx : nx + 8, :], r_a[t, nx : nx + 8, :])
            for k in range(6):
                fault[k, t, ny : ny + 1, :] = line[k : k + 1, :]
    for row in range(0, nx, 8):
        from_a = [r_a[k, pl.ds(row, 8), :] for k in range(n + 1)]
        from_b = [r_b[k, pl.ds(row, 8), :] for k in range(n + 1)]
        low = [jnp.where(odd, a, b) for a, b in zip(from_a, from_b)]
        high = [jnp.where(odd, b, a) for a, b in zip(from_a, from_b)]
        if first:
            ahead_b[0, pl.ds(row, 8), :] = high[3]
            ahead_b[1, pl.ds(row, 8), :] = strip_take(high[n], 3)
        for t in range(2):
            scale = DT * m[B, t, 0, pl.ds(row, 8), :]
            scale_ahead = DT * ahead_b[t, pl.ds(row, 8), :]
            for c in range(3):
                low_c = low[c] if t == 0 else strip_take(low[n], c)
                high_c = high[c] if t == 0 else strip_take(high[n], c)
                v[c, t, 0, pl.ds(PAD + row, 8), :] = at(v, c, t, 0, row) - scale * low_c
                v[c, t, ny, pl.ds(PAD + row, 8), :] = high_c - scale_ahead * at(
                    s, ALONG_Y[c], t, ny - 1, row
                )
    f_msg[...] = jnp.zeros_like(f_msg)
    rows[...] = jnp.zeros_like(rows)
    for c in range(3):
        for y in range(ny + 1):
            for t in range(2):
                line = jnp.where(
                    minus,
                    v[c, t, y, PAD + nx - 1 : PAD + nx, :],
                    v[c, t, y, PAD : PAD + 1, :],
                )
                if t == 0:
                    f_msg[c, y : y + 1, :] = line
                else:
                    rows[c, y : y + 1, :] = line
    if first:
        for t in range(2):
            for y in range(ny + 1):
                if y < ny:
                    line = jnp.where(minus, m[B, t, y, nx - 1 : nx, :], m[B, t, y, 0:1, :])
                else:
                    line = jnp.where(minus, ahead_b[t, nx - 1 : nx, :], ahead_b[t, 0:1, :])
                fault[OWN_B, t, y : y + 1, :] = line
                if t == 0:
                    f_msg[3, y : y + 1, :] = line
                else:
                    rows[3, y : y + 1, :] = line
    for half in range(0, f_msg.shape[1], 8):
        f_msg[n, half : half + 8, :] = strip_pack(
            [rows[k, half : half + 8, :] for k in range(n)], eighths[...]
        )


def rim_kernel(v, m, s_in, s):
    ny, nx, width = m.shape[2:]
    lanes = lane_index((8, width))

    def planes(i, carry):
        for row in range(8, nx - 8, 8):
            stress_tile(v, s, m, i * (ny - 1), row, lanes)
        return carry

    lax.fori_loop(0, 2, planes, 0)


def inverse_sinh(values):
    size = jnp.abs(values)
    sign = jnp.where(values > 0.0, 1.0, jnp.where(values < 0.0, -1.0, 0.0))
    return sign * jnp.log(size + jnp.sqrt(size * size + 1.0))


def friction(minus_side, plus_side, minus_b, plus_b, par):
    total = DT * (minus_b + plus_b)
    impedance = 1.0 / jnp.where(total > 0.0, total, 1.0)
    jump = [p - q for p, q in zip(plus_side, minus_side)]
    locked_y = par[PRE_Y] + impedance * jump[1]
    locked_z = par[PRE_Z] + impedance * jump[2]
    magnitude = jnp.sqrt(locked_y * locked_y + locked_z * locked_z + 1.0)
    rate, strength, slip = par[RATE], par[STRENGTH], par[SLIP]
    for _ in range(NEWTON):
        scaled = rate * slip
        residual = magnitude - impedance * slip - strength * inverse_sinh(scaled)
        tangent = -impedance - strength * rate / jnp.sqrt(1.0 + scaled * scaled)
        slip = slip - residual / tangent
    slip = slip * par[MASK]
    retained = 1.0 - impedance * slip / magnitude
    traction = (
        impedance * jump[0],
        retained * locked_y - par[PRE_Y],
        retained * locked_z - par[PRE_Z],
    )
    return traction, slip


def fault_kernel(first, final, flags, eighths, f_own, f_other, m, *rest):
    v_in, s_in, fault_in, v, s, fault = rest[:6]
    if final:
        new_v, new_s, slip_out, rows, sems = rest[6:]
    else:
        y_a, y_b, rows = rest[6:]
    ny, nx, width = m.shape[2:]
    minus, odd = flags[0] == 0, flags[1] == 1
    lanes = lane_index((8, width))
    n = 4 if first else 3
    high = f_own.shape[1]
    sign = jnp.where(minus, DT, -DT)
    for t in range(2):
        for half in range(0, high, 8):
            span = slice(half, half + 8)

            def piece(ref, k):
                return ref[k, span, :] if t == 0 else strip_take(ref[n, span, :], k)

            if first:
                fault[OTHER_B, t, span, :] = piece(f_other, 3)
            own = [piece(f_own, c) for c in range(3)]
            other = [piece(f_other, c) for c in range(3)]
            par = [fault[k, t, span, :] for k in range(8)]
            m_side = [jnp.where(minus, a, b) for a, b in zip(own, other)]
            p_side = [jnp.where(minus, b, a) for a, b in zip(own, other)]
            m_b = jnp.where(minus, par[OWN_B], par[OTHER_B])
            p_b = jnp.where(minus, par[OTHER_B], par[OWN_B])
            traction, slip = friction(m_side, p_side, m_b, p_b, par)
            fault[SLIP, t, span, :] = slip
            for c in range(3):
                rows[c, t, span, :] = own[c] + sign * par[OWN_B] * traction[c]
    for side, row in ((0, PAD + nx - 1), (1, PAD)):

        @pl.when(flags[0] == side)
        def _(row=row):
            for c in range(3):
                for t in range(2):
                    for y in range(ny + 1):
                        v[c, t, y, row : row + 1, :] = rows[c, t, y : y + 1, :]

    def ends(y, carry):
        for row in (0, nx - 8):
            stress_tile(v, s, m, y, row, lanes)
        return carry

    lax.fori_loop(0, ny, ends, 0)
    if final:
        slip_out[...] = fault[SLIP, 0, 0:ny, :]
        copies = []
        for c in range(3):
            copies.append((v.at[c, 0, pl.ds(0, ny), pl.ds(PAD, nx), :], new_v.at[c]))
        for c in range(6):
            copies.append((s.at[c, 0, :, pl.ds(PAD, nx), :], new_s.at[c]))
        copies = [pltpu.make_async_copy(a, b, sems.at[k]) for k, (a, b) in enumerate(copies)]
        for copy in copies:
            copy.start()
        for copy in copies:
            copy.wait()
    else:
        partial_trials(v, s, m, nx, lanes)
        for row in range(0, nx, 8):
            write_messages(v, s, eighths[...], odd, row, y_a, y_b, None)


def f32(*shape):
    return VMEM(shape, jnp.float32)


def call(kernel, name, outs, in_specs, aliases, scratch=(), flops=0, out_specs=None):
    return pl.pallas_call(
        kernel,
        out_shape=tuple(outs),
        in_specs=in_specs,
        out_specs=tuple(out_specs or [in_vmem() for _ in outs]),
        input_output_aliases=aliases,
        scratch_shapes=list(scratch),
        compiler_params=pltpu.CompilerParams(vmem_limit_bytes=8 << 20),
        cost_estimate=pl.CostEstimate(flops=flops, bytes_accessed=0, transcendentals=0),
        name=name,
    )


def pair_swaps(a, b, axis):
    size = lax.axis_size(axis)
    out = []
    for value, start in ((a, 0), (b, 1)):
        pairs = []
        for i in range(start, size - 1, 2):
            pairs += [(i, i + 1), (i + 1, i)]
        out.append(lax.ppermute(value, axis, pairs))
    return out


def local(
    velocity,
    stress,
    buoyancy,
    stiff_xx,
    stiff_xz,
    stiff_zz,
    shear_vert,
    shear_horiz,
    prestress,
    fault_mask,
    region_ids,
    inverse_rate,
    slip_prev,
    region_a,
    region_normal,
):
    ny, nx, width = buoyancy.shape
    across, along, dip = (lax.axis_index(k) for k in ("gx", "gy", "gz"))
    flags = jnp.stack([across, along % 2, dip % 2]).astype(jnp.int32)
    lanes = jnp.broadcast_to(jnp.arange(width, dtype=jnp.int32), (8, width))
    thirds, eighths = lanes // HALO, lanes // STRIP
    rows = nx + 2 * PAD
    high = 8 * ((ny + 1 + 7) // 8)
    v_shape = f32(3, 2, ny + 1, rows, width)
    s_shape = f32(6, 2, ny, rows, width)
    m_shape = f32(6, 2, ny, nx, width)
    fault_shape = f32(8, 2, high, width)
    planes = z_slots(ny, width)[1]
    z_shape = f32(planes, nx + 8, width)
    unit = ny * nx * width
    vm, hb, sm = in_vmem(), in_hbm(), in_smem()

    raw = [velocity, stress, buoyancy, stiff_xx, stiff_xz, stiff_zz, shear_vert, shear_horiz]
    raw += [prestress, region_ids, fault_mask, inverse_rate, slip_prev, region_a, region_normal]
    raw = [pltpu.with_memory_space_constraint(k, HBM) for k in raw]
    v, s, m, fault, z_a, z_b = call(
        load_kernel,
        "load",
        (v_shape, s_shape, m_shape, fault_shape, z_shape, z_shape),
        [sm, vm] + [hb] * 15,
        {},
        [
            pltpu.VMEM(prestress.shape, jnp.float32),
            pltpu.VMEM(region_ids.shape, jnp.int32),
            pltpu.VMEM(fault_mask.shape, jnp.int32),
            pltpu.VMEM(inverse_rate.shape, jnp.float32),
            pltpu.VMEM(slip_prev.shape, jnp.float32),
            pltpu.SMEM(region_a.shape, jnp.float32),
            pltpu.SMEM(region_normal.shape, jnp.float32),
            pltpu.SemaphoreType.DMA((22,)),
        ],
        flops=100 * unit,
    )(flags, thirds, *raw)
    z_a, z_b = pair_swaps(z_a, z_b, "gz")
    y_shape = f32(5, nx + 8, width)
    v, s, m, fault, y_a, y_b = call(
        widen_kernel,
        "widen",
        (v_shape, s_shape, m_shape, fault_shape, y_shape, y_shape),
        [sm] + [vm] * 8,
        {5: 0, 6: 1, 7: 2, 8: 3},
        flops=50 * unit,
    )(flags, thirds, eighths, z_a, z_b, v, s, m, fault)
    y_shape = f32(4, nx, width)
    ahead_b = None
    for step in range(STEPS):
        first, final = step == 0, step == STEPS - 1
        y_a, y_b = pair_swaps(y_a, y_b, "gy")
        v, s = call(
            inner_kernel, "inner", (v_shape, s_shape), [vm] * 3, {1: 0, 0: 1}, flops=200 * unit
        )(s, v, m)
        f_shape = f32(5 if first else 4, high, width)
        scratch = [pltpu.VMEM((4, high, width), jnp.float32)]
        if first:
            v, fault, ahead_b, f_own = call(
                functools.partial(finish_kernel, True),
                "finish",
                (v_shape, fault_shape, f32(2, nx, width), f_shape),
                [sm] + [vm] * 7,
                {6: 0, 7: 1},
                scratch,
                flops=unit,
            )(flags, eighths, y_a, y_b, s, m, v, fault)
        else:
            v, f_own = call(
                functools.partial(finish_kernel, False),
                "finish",
                (v_shape, f_shape),
                [sm] + [vm] * 7,
                {6: 0},
                scratch,
                flops=unit,
            )(flags, eighths, y_a, y_b, s, m, v, ahead_b)
        f_other = lax.ppermute(f_own, "gx", [(i, i ^ 1) for i in range(lax.axis_size("gx"))])
        (s,) = call(rim_kernel, "rim", (s_shape,), [vm] * 3, {2: 0}, flops=50 * unit)(v, m, s)
        outs = [v_shape, s_shape, fault_shape]
        specs = [vm, vm, vm]
        scratch = [pltpu.VMEM((3, 2, high, width), jnp.float32)]
        if final:
            outs += [
                jax.ShapeDtypeStruct((3, ny, nx, width), jnp.float32),
                jax.ShapeDtypeStruct((6, ny, nx, width), jnp.float32),
                jax.ShapeDtypeStruct((ny, width), jnp.float32),
            ]
            specs += [hb, hb, vm]
            scratch.append(pltpu.SemaphoreType.DMA((9,)))
        else:
            outs += [y_shape, y_shape]
            specs += [vm, vm]
        v, s, fault, *more = call(
            functools.partial(fault_kernel, first, final),
            "fault",
            outs,
            [sm] + [vm] * 7,
            {5: 0, 6: 1, 7: 2},
            scratch,
            flops=50 * unit,
            out_specs=specs,
        )(flags, eighths, f_own, f_other, m, v, s, fault)
        if final:
            return tuple(more)
        y_a, y_b = more


def solution(mesh):
    in_specs = (
        P(None, "gy", "gx", "gz"),
        P(None, "gy", "gx", "gz"),
        P("gy", "gx", "gz"),
        P("gy", "gx", "gz"),
        P("gy", "gx", "gz"),
        P("gy", "gx", "gz"),
        P("gy", "gx", "gz"),
        P("gy", "gx", "gz"),
        P(None, "gy", "gz"),
        P("gy", "gz"),
        P("gy", "gz"),
        P("gy", "gz"),
        P("gy", "gz"),
        P(),
        P(),
    )
    out_specs = (P(None, "gy", "gx", "gz"), P(None, "gy", "gx", "gz"), P("gy", "gz"))
    return jax.shard_map(local, mesh=mesh, in_specs=in_specs, out_specs=out_specs, check_vma=False)
```

```python
import functools

import jax
import jax.numpy as jnp
from jax import lax
from jax.experimental import pallas as pl
from jax.experimental.pallas import tpu as pltpu
from jax.sharding import PartitionSpec as P

STEPS = 3
NEWTON = 3
DT = 0.2

PAD = 8
HALO = 3
CROSS = 4
STRIP = 8

XX, YY, ZZ, YZ, XZ, XY = range(6)
ALONG_Y = (XY, YY, YZ)
B, C11, C13, C33, C44, C66 = range(6)
FIELDS = [("v", c) for c in range(3)] + [("s", c) for c in range(6)] + [("m", c) for c in range(6)]
PRE_Y, PRE_Z, MASK, STRENGTH, RATE, SLIP, OWN_B, OTHER_B = range(8)

VMEM = pltpu.MemorySpace.VMEM
HBM = pltpu.MemorySpace.HBM
SMEM = pltpu.MemorySpace.SMEM


def in_vmem():
    return pl.BlockSpec(memory_space=VMEM)


def in_hbm():
    return pl.BlockSpec(memory_space=HBM)


def in_smem():
    return pl.BlockSpec(memory_space=SMEM)


def roll(values, by):
    by = by % values.shape[-1]
    return values if by == 0 else pltpu.roll(values, by, values.ndim - 1)


def at(ref, field, tile, y, row):
    return ref[field, tile, y, pl.ds(PAD + row, 8), :]


def z_below(pair, lanes):
    one, two = roll(pair[0], 1), roll(pair[1], 1)
    first = lanes == 0
    return jnp.where(first, two, one), jnp.where(first, one, two)


def z_above(pair, lanes):
    one, two = roll(pair[0], -1), roll(pair[1], -1)
    last = lanes == pair[0].shape[-1] - 1
    return jnp.where(last, two, one), jnp.where(last, one, two)


def trial_tile(v, s, m, y, row, below, lanes):
    both = (0, 1)
    behind = {c: z_below([at(s, c, t, y, row) for t in both], lanes) for c in (XZ, YZ, ZZ)}
    out = []
    for t in both:
        own = {c: at(s, c, t, y, row) for c in range(6)}
        lower_x = {c: own[c] - at(s, c, t, y, row - 1) for c in (XX, XY, XZ)}
        if below is None:
            lower_y = {c: own[c] for c in ALONG_Y}
        else:
            lower_y = {c: own[c] - below(c, t) for c in ALONG_Y}
        scale = DT * m[B, t, y, pl.ds(row, 8), :]
        total = (
            lower_x[XX] + lower_y[XY] + (own[XZ] - behind[XZ][t]),
            lower_x[XY] + lower_y[YY] + (own[YZ] - behind[YZ][t]),
            lower_x[XZ] + lower_y[YZ] + (own[ZZ] - behind[ZZ][t]),
        )
        out.append([at(v, c, t, y, row) + scale * total[c] for c in range(3)])
    return out


def stress_tile(v, s, m, y, row, lanes):
    both = (0, 1)
    own = [[at(v, c, t, y, row) for t in both] for c in range(3)]
    ahead = [z_above(own[c], lanes) for c in range(3)]
    for t in both:
        vx, vy, vz = own[0][t], own[1][t], own[2][t]
        over_x = [at(v, c, t, y, row + 1) for c in range(3)]
        over_y = [at(v, c, t, y + 1, row) for c in range(3)]
        exx, eyy, ezz = over_x[0] - vx, over_y[1] - vy, ahead[2][t] - vz
        c11, c13, c33, c44, c66 = (m[k, t, y, pl.ds(row, 8), :] for k in (C11, C13, C33, C44, C66))
        c12 = c11 - 2.0 * c66
        third = c13 * ezz
        change = {
            XX: c11 * exx + c12 * eyy + third,
            YY: c12 * exx + c11 * eyy + third,
            ZZ: c13 * (exx + eyy) + c33 * ezz,
            YZ: c44 * ((ahead[1][t] - vy) + (over_y[2] - vz)),
            XZ: c44 * ((ahead[0][t] - vx) + (over_x[2] - vz)),
            XY: c66 * ((over_y[0] - vx) + (over_x[1] - vy)),
        }
        for c, gain in change.items():
            s[c, t, y, pl.ds(PAD + row, 8), :] = at(s, c, t, y, row) + DT * gain


def lane_index(like):
    return lax.broadcasted_iota(jnp.int32, like, len(like) - 1)


def strip_pack(pieces, eighths):
    packed = jnp.zeros_like(pieces[0])
    for k, piece in enumerate(pieces):
        packed = jnp.where(eighths == k, roll(piece, STRIP * k + HALO), packed)
    return packed


def strip_take(packed, k):
    return roll(packed, -(STRIP * k + HALO))


def field_ref(kind, v, s, m):
    return {"v": v, "s": s, "m": m}[kind]


def fields_per_plane(ny, width):
    return (width - 5) // HALO // ny


def z_slots(ny, width):
    per_plane = fields_per_plane(ny, width)
    slots = {}
    for f in range(len(FIELDS)):
        for y in range(ny):
            slots[f, y] = (f // per_plane, f % per_plane * ny + y)
    return slots, -(-len(FIELDS) // per_plane)


def row_tiles(nx):
    return [*range(0, nx, 8), cross_row(nx)]


def cross_row(nx):
    return nx + PAD


def packed_row(row, nx):
    return row if row < nx else nx


def edge_kernel(flags, velocity, stress, *rest):
    raw_m, out, sem = rest[:6], rest[6], rest[7]
    ny, nx = velocity.shape[1:3]
    sources = [velocity.at[c] for c in range(3)] + [stress.at[c] for c in range(6)] + list(raw_m)
    for side, row in ((0, nx - CROSS), (1, 0)):

        @pl.when(flags[0] == side)
        def _(row=row):
            copies = []
            for f, source in enumerate(sources):
                for half in range(2):
                    part = source.at[pl.ds(half * (ny // 2), ny // 2), pl.ds(row, CROSS), :]
                    to = out.at[f, :, pl.ds(half * CROSS, CROSS), :]
                    copies.append(pltpu.make_async_copy(part, to, sem.at[2 * f + half]))
            for copy in copies:
                copy.start()
            for copy in copies:
                copy.wait()


def load_kernel(flags, velocity, stress, *rest):
    raw_m, small = rest[:6], rest[6:13]
    v, s, m, fault, y_a, y_b = rest[13:19]
    pre, ids, mask, rate, slip, region_a, region_normal, sems = rest[19:]
    ny, nx, width = velocity.shape[1:]
    cross = cross_row(nx)
    big = {}
    for c in range(6):
        big["s", c] = (stress.at[c], s.at[c, 0, :, pl.ds(PAD, nx), :])
    for c in range(3):
        big["v", c] = (velocity.at[c], v.at[c, 0, pl.ds(0, ny), pl.ds(PAD, nx), :])
    for c in range(6):
        big["m", c] = (raw_m[c], m.at[c, 0, :, pl.ds(0, nx), :])
    big = {
        key: pltpu.make_async_copy(a, b, sems.at[k]) for k, (key, (a, b)) in enumerate(big.items())
    }
    held = (pre, ids, mask, rate, slip, region_a, region_normal)
    little = [
        pltpu.make_async_copy(a, b, sems.at[len(big) + k])
        for k, (a, b) in enumerate(zip(small, held))
    ]
    for copy in big.values():
        copy.start()
    for copy in little:
        copy.start()
    zeros = jnp.zeros((PAD, width), jnp.float32)
    for t in range(2):
        for y in range(ny):
            for c in (XX, XY, XZ):
                s[c, t, y, 0:PAD, :] = zeros
                s[c, t, y, cross : cross + PAD, :] = zeros
            for c in range(3):
                v[c, t, y, PAD + nx : PAD + nx + PAD, :] = zeros
                v[c, t, y, PAD + cross + 8 : 2 * PAD + cross + 8, :] = zeros
    for copy in little:
        copy.wait()
    kinds = ids[...]
    a_part = jnp.zeros((ny, width), jnp.float32)
    n_part = jnp.zeros((ny, width), jnp.float32)
    for k in range(region_a.shape[0]):
        a_part = jnp.where(kinds == k, region_a[k], a_part)
        n_part = jnp.where(kinds == k, region_normal[k], n_part)
    fault[PRE_Y, 0, 0:ny, :] = pre[0]
    fault[PRE_Z, 0, 0:ny, :] = pre[1]
    fault[MASK, 0, 0:ny, :] = mask[...].astype(jnp.float32)
    fault[STRENGTH, 0, 0:ny, :] = a_part * n_part
    fault[RATE, 0, 0:ny, :] = rate[...]
    fault[SLIP, 0, 0:ny, :] = slip[...]
    for copy in big.values():
        copy.wait()

    odd = flags[1] == 1
    lanes = lane_index((8, width))
    first = lanes == 0
    last = ny - 1
    for row in range(0, nx, 8):
        up = [at(s, c, 0, last, row) for c in ALONG_Y]
        own = {c: at(s, c, 0, 0, row) for c in range(6)}
        behind = {c: jnp.where(first, 0.0, roll(own[c], 1)) for c in (XZ, YZ, ZZ)}
        lower_x = {c: own[c] - at(s, c, 0, 0, row - 1) for c in (XX, XY, XZ)}
        buoyancy = m[B, 0, 0, pl.ds(row, 8), :]
        total = (
            lower_x[XX] + own[XY] + (own[XZ] - behind[XZ]),
            lower_x[XY] + own[YY] + (own[YZ] - behind[YZ]),
            lower_x[XZ] + own[YZ] + (own[ZZ] - behind[ZZ]),
        )
        for c in range(3):
            down = at(v, c, 0, 0, row) + DT * buoyancy * total[c]
            y_a[c, pl.ds(row, 8), :] = jnp.where(odd, down, up[c])
            y_b[c, pl.ds(row, 8), :] = jnp.where(odd, up[c], down)
        y_a[3, pl.ds(row, 8), :] = buoyancy
        y_b[3, pl.ds(row, 8), :] = buoyancy


def z_emit(z_a, z_b, odd, group, pieces, plane, row):
    up = jnp.zeros_like(pieces[0][1])
    down = up
    for pos, piece in pieces:
        moved = roll(piece, HALO * pos + HALO)
        up = jnp.where(group == pos, moved, up)
        down = jnp.where(group == pos + 1, moved, down)
    z_a[plane, pl.ds(row, 8), :] = jnp.where(odd, down, up)
    z_b[plane, pl.ds(row, 8), :] = jnp.where(odd, up, down)


def z_pieces(plane, v, s, m, row):
    ny, width = m.shape[2], m.shape[4]
    per_plane = fields_per_plane(ny, width)
    pieces = []
    for f, (kind, c) in enumerate(FIELDS[plane * per_plane : (plane + 1) * per_plane]):
        shift = 0 if kind == "m" else PAD
        ref = field_ref(kind, v, s, m)
        for y in range(ny):
            pieces.append((f * ny + y, ref[c, 0, y, pl.ds(row + shift, 8), :]))
    return pieces


UNROLL = 4


def pack_kernel(flags, thirds, v, s, m, z_a, z_b):
    ny, width = m.shape[2], m.shape[4]
    nx = z_a.shape[1] - 16
    planes = z_slots(ny, width)[1]
    odd = flags[2] == 1
    group = thirds[...]

    def pack(i, carry):
        for part in range(UNROLL):
            row = pl.multiple_of((i * UNROLL + part) * 8, 8)
            for plane in range(planes):
                z_emit(z_a, z_b, odd, group, z_pieces(plane, v, s, m, row), plane, row)
        return carry

    lax.fori_loop(0, nx // (8 * UNROLL), pack, 0)


def cross_kernel(flags, thirds, f_other, fault, v_in, s_in, m_in, za_in, zb_in, v, s, m, z_a, z_b):
    ny, width = m.shape[2], m.shape[4]
    nx = z_a.shape[1] - 16
    cross = cross_row(nx)
    odd = flags[2] == 1
    group = thirds[...]
    planes = z_slots(ny, width)[1]
    rows = lax.broadcasted_iota(jnp.int32, (8, width), 0)
    minus = flags[0] == 0
    keep = jnp.where(minus, 7 - rows, rows) >= 8 - CROSS
    for f, (kind, c) in enumerate(FIELDS):
        shift = 0 if kind == "m" else PAD
        ref = field_ref(kind, v, s, m)
        for y in range(ny // 2):
            tile = f_other[f, y]
            turned = pltpu.roll(tile, CROSS, 0)
            ref[c, 0, y, cross + shift : cross + shift + 8, :] = jnp.where(
                keep, jnp.where(minus, tile, turned), 0.0
            )
            ref[c, 0, y + ny // 2, cross + shift : cross + shift + 8, :] = jnp.where(
                keep, jnp.where(minus, turned, tile), 0.0
            )
    for plane in range(planes):
        z_emit(z_a, z_b, odd, group, z_pieces(plane, v, s, m, cross), plane, nx)
    z_emit(z_a, z_b, odd, group, [(k, fault[k, 0, 0:8, :]) for k in range(6)], 0, nx + 8)
    zeros = jnp.zeros((8, width), jnp.float32)
    for plane in range(1, planes):
        z_a[plane, pl.ds(nx + 8, 8), :] = zeros
        z_b[plane, pl.ds(nx + 8, 8), :] = zeros


def write_messages(v, s, eighths, odd, y_a, y_b, nx):
    last = s.shape[2] - 1
    span = nx + 8
    for row in row_tiles(nx):
        up = [at(s, c, 0, last, row) for c in ALONG_Y]
        down = [at(v, c, 0, 0, row) for c in range(3)]
        up.append(strip_pack([at(s, c, 1, last, row) for c in ALONG_Y], eighths))
        down.append(strip_pack([at(v, c, 1, 0, row) for c in range(3)], eighths))
        for k in range(4):
            to = pl.ds(k * span + packed_row(row, nx), 8)
            y_a[to, :] = jnp.where(odd, down[k], up[k])
            y_b[to, :] = jnp.where(odd, up[k], down[k])


def partial_trials(v, s, m, nx, lanes):
    for row in row_tiles(nx):
        new = trial_tile(v, s, m, 0, row, None, lanes)
        for t in range(2):
            for c in range(3):
                v[c, t, 0, pl.ds(PAD + row, 8), :] = new[t][c]


def widen_kernel(flags, thirds, eighths, r_a, r_b, v_in, s_in, m_in, f_in, v, s, m, fault, y_a, y_b):
    ny, width = m.shape[2], m.shape[4]
    nx = r_a.shape[1] - 16
    cross = cross_row(nx)
    slots, planes = z_slots(ny, width)
    odd_z, odd_y = flags[2] == 1, flags[1] == 1
    lanes = lane_index((8, width))
    group = thirds[...]

    def take(row, wanted):
        from_a = [r_a[p, pl.ds(row, 8), :] for p in range(planes)]
        from_b = [r_b[p, pl.ds(row, 8), :] for p in range(planes)]
        low = [jnp.where(odd_z, a, b) for a, b in zip(from_a, from_b)]
        high = [jnp.where(odd_z, b, a) for a, b in zip(from_a, from_b)]
        for (plane, pos), store in wanted:
            store(roll(jnp.where(group == pos, low[plane], high[plane]), -(HALO * pos + HALO)))

    def store_to(ref, c, y, row):
        def store(value):
            ref[c, 1, y, pl.ds(row, 8), :] = value

        return store

    def fields(row):
        wanted = []
        for f, (kind, c) in enumerate(FIELDS):
            shift = 0 if kind == "m" else PAD
            ref = field_ref(kind, v, s, m)
            for y in range(ny):
                wanted.append((slots[f, y], store_to(ref, c, y, row + shift)))
        return wanted

    def unpack(i, carry):
        for part in range(UNROLL):
            row = pl.multiple_of((i * UNROLL + part) * 8, 8)
            take(row, fields(row))
        return carry

    lax.fori_loop(0, nx // (8 * UNROLL), unpack, 0)
    take(nx, fields(cross))

    def store_fault(k):
        def store(value):
            fault[k, 1, 0:8, :] = value

        return store

    take(nx + 8, [((0, k), store_fault(k)) for k in range(6)])
    partial_trials(v, s, m, nx, lanes)
    last = ny - 1
    halos = eighths[...]
    for row in row_tiles(nx):
        buoyancy = m[B, 1, 0, pl.ds(row, 8), :]
        up = [at(s, c, 1, last, row) for c in ALONG_Y] + [buoyancy]
        down = [
            jnp.where(lanes == HALO, roll(at(v, c, 0, 0, row), HALO), at(v, c, 1, 0, row))
            for c in range(3)
        ] + [buoyancy]
        up, down = strip_pack(up, halos), strip_pack(down, halos)
        to = pl.ds(packed_row(row, nx), 8)
        y_a[to, :] = jnp.where(odd_y, down, up)
        y_b[to, :] = jnp.where(odd_y, up, down)
    up = [at(s, c, 0, last, cross) for c in ALONG_Y]
    down = [at(v, c, 0, 0, cross) for c in range(3)]
    buoyancy = m[B, 0, 0, pl.ds(cross, 8), :]
    for c in range(4):
        to = pl.ds(nx + 8 + 8 * c, 8)
        y_a[to, :] = buoyancy if c == 3 else jnp.where(odd_y, down[c], up[c])
        y_b[to, :] = buoyancy if c == 3 else jnp.where(odd_y, up[c], down[c])
    for t in range(2):
        for k in range(8):
            line = fault[min(k, 5), t, 0:1, :]
            row = nx + 40 + 8 * t + k
            y_a[row : row + 1, :] = line
            y_b[row : row + 1, :] = line


def inner_kernel(first, final, m, v_in, s_in, v, s, *outs):
    ny, width = m.shape[2], m.shape[4]
    nx = m.shape[3] - 16
    lanes = lane_index((8, width))

    if not first:

        def ends(y, carry):
            for row in (0, nx - 8, cross_row(nx)):
                stress_tile(v, s, m, y, row, lanes)
            return carry

        lax.fori_loop(1, ny - 1, ends, 0)

    def trials(y, carry):
        for row in row_tiles(nx):
            new = trial_tile(
                v, s, m, y, row, lambda c, t, row=row: at(s, c, t, y - 1, row), lanes
            )
            for t in range(2):
                for c in range(3):
                    v[c, t, y, pl.ds(PAD + row, 8), :] = new[t][c]
        return carry

    lax.fori_loop(1, ny, trials, 0)
    copies = []
    if final:
        new_v, new_s, sems = outs
        for c in range(3):
            part = v.at[c, 0, pl.ds(1, ny - 1), pl.ds(PAD + 8, nx - 16), :]
            to = new_v.at[c, pl.ds(1, ny - 1), pl.ds(8, nx - 16), :]
            copies.append(pltpu.make_async_copy(part, to, sems.at[c]))
            copies[-1].start()

    def stresses(y, carry):
        for row in range(8, nx - 8, 8):
            stress_tile(v, s, m, y, row, lanes)
        return carry

    lax.fori_loop(1, ny - 1, stresses, 0)
    if final:
        for c in range(6):
            part = s.at[c, 0, pl.ds(1, ny - 2), pl.ds(PAD + 8, nx - 16), :]
            to = new_s.at[c, pl.ds(1, ny - 2), pl.ds(8, nx - 16), :]
            copies.append(pltpu.make_async_copy(part, to, sems.at[3 + c]))
            copies[-1].start()
        for copy in copies:
            copy.wait()


def boundary_kernel(first, final, flags, eighths, *refs):
    refs = list(refs)

    def pop(n):
        out = refs[:n]
        del refs[:n]
        return out

    early_a, early_b = pop(2) if first else (None, None)
    r_a, r_b, m = pop(3)
    if not first:
        (ahead_b,) = pop(1)
    pop(3)
    if final:
        pop(2)
    v, s, fault = pop(3)
    if first:
        (ahead_b,) = pop(1)
    if final:
        new_v, new_s, slip_out, rows, sems = refs
    else:
        y_a, y_b, rows = refs
    ny, width = m.shape[2], m.shape[4]
    nx = m.shape[3] - 16
    cross = cross_row(nx)
    span = nx + 8
    odd = flags[1] == 1
    lanes = lane_index((8, width))
    halos = eighths[...]

    def received(row):
        at_row = packed_row(row, nx)
        if not first:
            from_a = [r_a[pl.ds(k * span + at_row, 8), :] for k in range(4)]
            from_b = [r_b[pl.ds(k * span + at_row, 8), :] for k in range(4)]
        else:
            if row < nx:
                from_a = [early_a[k, pl.ds(row, 8), :] for k in range(4)]
                from_b = [early_b[k, pl.ds(row, 8), :] for k in range(4)]
            else:
                from_a = [r_a[pl.ds(span + 8 * k, 8), :] for k in range(4)]
                from_b = [r_b[pl.ds(span + 8 * k, 8), :] for k in range(4)]
            from_a.append(r_a[pl.ds(at_row, 8), :])
            from_b.append(r_b[pl.ds(at_row, 8), :])
        low = [jnp.where(odd, a, b) for a, b in zip(from_a, from_b)]
        high = [jnp.where(odd, b, a) for a, b in zip(from_a, from_b)]
        if first and row < nx:
            for c in range(3):
                column = roll(high[-1], -(STRIP * c + 2 * HALO))
                high[c] = jnp.where(lanes == 0, column, high[c])
        return low, high

    if first:
        for t in range(2):
            to = pl.ds(span + 32 + 8 * t, 8)
            lines = jnp.where(odd, r_b[to, :], r_a[to, :])
            for k in range(6):
                fault[k, t, ny : ny + 1, :] = lines[k : k + 1, :]
    for row in row_tiles(nx):
        low, high = received(row)
        if first:
            ahead_b[0, pl.ds(row, 8), :] = high[3]
            ahead_b[1, pl.ds(row, 8), :] = strip_take(high[-1], 3)
        for t in range(2):
            scale = DT * m[B, t, 0, pl.ds(row, 8), :]
            scale_ahead = DT * ahead_b[t, pl.ds(row, 8), :]
            for c in range(3):
                low_c = low[c] if t == 0 else strip_take(low[-1], c)
                high_c = high[c] if t == 0 else strip_take(high[-1], c)
                v[c, t, 0, pl.ds(PAD + row, 8), :] = at(v, c, t, 0, row) - scale * low_c
                v[c, t, ny, pl.ds(PAD + row, 8), :] = high_c - scale_ahead * at(
                    s, ALONG_Y[c], t, ny - 1, row
                )

    places = ((0, (nx - 1, cross)), (1, (0, cross + 7)))
    for side, pair in places:

        @pl.when(flags[0] == side)
        def _(pair=pair):
            for which, row in enumerate(pair):
                for t in range(2):
                    for y in range(ny + 1):
                        for c in range(3):
                            rows[which, c, t, y : y + 1, :] = v[
                                c, t, y, PAD + row : PAD + row + 1, :
                            ]
                        if first:
                            if y < ny:
                                line = m[B, t, y, row : row + 1, :]
                            else:
                                line = ahead_b[t, row : row + 1, :]
                            fault[OWN_B + which, t, y : y + 1, :] = line

    minus = flags[0] == 0
    sign = jnp.where(minus, DT, -DT)
    for t in range(2):
        for half in range(0, fault.shape[2], 8):
            part = slice(half, half + 8)
            own = [rows[0, c, t, part, :] for c in range(3)]
            other = [rows[1, c, t, part, :] for c in range(3)]
            par = [fault[k, t, part, :] for k in range(8)]
            m_side = [jnp.where(minus, a, b) for a, b in zip(own, other)]
            p_side = [jnp.where(minus, b, a) for a, b in zip(own, other)]
            m_b = jnp.where(minus, par[OWN_B], par[OTHER_B])
            p_b = jnp.where(minus, par[OTHER_B], par[OWN_B])
            traction, slip = friction(m_side, p_side, m_b, p_b, par)
            fault[SLIP, t, part, :] = slip
            for c in range(3):
                rows[0, c, t, part, :] = own[c] + sign * par[OWN_B] * traction[c]
                rows[1, c, t, part, :] = other[c] - sign * par[OTHER_B] * traction[c]
    for side, pair in places:

        @pl.when(flags[0] == side)
        def _(pair=pair):
            for which, row in enumerate(pair):
                for c in range(3):
                    for t in range(2):
                        for y in range(ny + 1):
                            v[c, t, y, PAD + row : PAD + row + 1, :] = rows[
                                which, c, t, y : y + 1, :
                            ]

    def planes(i, carry):
        for row in row_tiles(nx)[:-1] if final else row_tiles(nx):
            stress_tile(v, s, m, i * (ny - 1), row, lanes)
        return carry

    lax.fori_loop(0, 2, planes, 0)
    if not final:
        partial_trials(v, s, m, nx, lanes)
        write_messages(v, s, halos, odd, y_a, y_b, nx)
        return

    def ends(y, carry):
        for row in (0, nx - 8):
            stress_tile(v, s, m, y, row, lanes)
        return carry

    lax.fori_loop(1, ny - 1, ends, 0)
    slip_out[...] = fault[SLIP, 0, 0:ny, :]
    copies = []
    for ref, out, fields, whole in ((v, new_v, 3, (0,)), (s, new_s, 6, (0, ny - 1))):
        inside = ny - len(whole)
        for c in range(fields):
            for y in whole:
                copies.append((ref.at[c, 0, y, pl.ds(PAD, nx), :], out.at[c, y]))
            for row in (0, nx - 8):
                copies.append(
                    (
                        ref.at[c, 0, pl.ds(1, inside), pl.ds(PAD + row, 8), :],
                        out.at[c, pl.ds(1, inside), pl.ds(row, 8), :],
                    )
                )
    copies = [pltpu.make_async_copy(a, b, sems.at[k]) for k, (a, b) in enumerate(copies)]
    for copy in copies:
        copy.start()
    for copy in copies:
        copy.wait()


def inverse_sinh(values):
    size = jnp.abs(values)
    sign = jnp.where(values > 0.0, 1.0, jnp.where(values < 0.0, -1.0, 0.0))
    return sign * jnp.log(size + jnp.sqrt(size * size + 1.0))


def friction(minus_side, plus_side, minus_b, plus_b, par):
    total = DT * (minus_b + plus_b)
    impedance = 1.0 / jnp.where(total > 0.0, total, 1.0)
    jump = [p - q for p, q in zip(plus_side, minus_side)]
    locked_y = par[PRE_Y] + impedance * jump[1]
    locked_z = par[PRE_Z] + impedance * jump[2]
    magnitude = jnp.sqrt(locked_y * locked_y + locked_z * locked_z + 1.0)
    rate, strength, slip = par[RATE], par[STRENGTH], par[SLIP]
    for _ in range(NEWTON):
        scaled = rate * slip
        residual = magnitude - impedance * slip - strength * inverse_sinh(scaled)
        tangent = -impedance - strength * rate / jnp.sqrt(1.0 + scaled * scaled)
        slip = slip - residual / tangent
    slip = slip * par[MASK]
    retained = 1.0 - impedance * slip / magnitude
    traction = (
        impedance * jump[0],
        retained * locked_y - par[PRE_Y],
        retained * locked_z - par[PRE_Z],
    )
    return traction, slip


def f32(*shape):
    return VMEM(shape, jnp.float32)


def call(kernel, name, outs, in_specs, aliases, scratch=(), flops=0, out_specs=None):
    return pl.pallas_call(
        kernel,
        out_shape=tuple(outs),
        in_specs=in_specs,
        out_specs=tuple(out_specs or [in_vmem() for _ in outs]),
        input_output_aliases=aliases,
        scratch_shapes=list(scratch),
        compiler_params=pltpu.CompilerParams(vmem_limit_bytes=8 << 20),
        cost_estimate=pl.CostEstimate(flops=flops, bytes_accessed=0, transcendentals=0),
        name=name,
    )


def pair_swaps(a, b, axis):
    size = lax.axis_size(axis)
    out = []
    for value, start in ((a, 0), (b, 1)):
        pairs = []
        for i in range(start, size - 1, 2):
            pairs += [(i, i + 1), (i + 1, i)]
        out.append(lax.ppermute(value, axis, pairs))
    return out


def local(
    velocity,
    stress,
    buoyancy,
    stiff_xx,
    stiff_xz,
    stiff_zz,
    shear_vert,
    shear_horiz,
    prestress,
    fault_mask,
    region_ids,
    inverse_rate,
    slip_prev,
    region_a,
    region_normal,
):
    ny, nx, width = buoyancy.shape
    across, along, dip = (lax.axis_index(k) for k in ("gx", "gy", "gz"))
    flags = jnp.stack([across, along % 2, dip % 2]).astype(jnp.int32)
    lanes = jnp.broadcast_to(jnp.arange(width, dtype=jnp.int32), (8, width))
    thirds, eighths = lanes // HALO, lanes // STRIP
    rows = cross_row(nx) + 8
    high = 8 * ((ny + 1 + 7) // 8)
    v_shape = f32(3, 2, ny + 1, rows + 2 * PAD, width)
    s_shape = f32(6, 2, ny, rows + 2 * PAD, width)
    m_shape = f32(6, 2, ny, rows, width)
    fault_shape = f32(8, 2, high, width)
    planes = z_slots(ny, width)[1]
    z_shape = f32(planes, nx + 16, width)
    unit = ny * nx * width
    vm, hb, sm = in_vmem(), in_hbm(), in_smem()
    raw = [velocity, stress, buoyancy, stiff_xx, stiff_xz, stiff_zz, shear_vert, shear_horiz]
    raw += [prestress, region_ids, fault_mask, inverse_rate, slip_prev, region_a, region_normal]
    raw = [pltpu.with_memory_space_constraint(k, HBM) for k in raw]

    f_shape = f32(len(FIELDS), ny // 2, 8, width)
    (f_own,) = call(
        edge_kernel,
        "edge",
        (f_shape,),
        [sm] + [hb] * 8,
        {},
        [pltpu.SemaphoreType.DMA((2 * len(FIELDS),))],
        flops=unit,
    )(flags, *raw[:8])
    f_other = lax.ppermute(f_own, "gx", [(i, i ^ 1) for i in range(lax.axis_size("gx"))])
    y_shape = f32(4, nx, width)
    v, s, m, fault, early_a, early_b = call(
        load_kernel,
        "load",
        (v_shape, s_shape, m_shape, fault_shape, y_shape, y_shape),
        [sm] + [hb] * 15,
        {},
        [
            pltpu.VMEM(prestress.shape, jnp.float32),
            pltpu.VMEM(region_ids.shape, jnp.int32),
            pltpu.VMEM(fault_mask.shape, jnp.int32),
            pltpu.VMEM(inverse_rate.shape, jnp.float32),
            pltpu.VMEM(slip_prev.shape, jnp.float32),
            pltpu.SMEM(region_a.shape, jnp.float32),
            pltpu.SMEM(region_normal.shape, jnp.float32),
            pltpu.SemaphoreType.DMA((22,)),
        ],
        flops=100 * unit,
    )(flags, *raw)
    early_a, early_b = pair_swaps(early_a, early_b, "gy")
    z_a, z_b = call(
        pack_kernel, "pack", (z_shape, z_shape), [sm] + [vm] * 4, {}, flops=50 * unit
    )(flags, thirds, v, s, m)
    v, s, m, z_a, z_b = call(
        cross_kernel,
        "cross",
        (v_shape, s_shape, m_shape, z_shape, z_shape),
        [sm] + [vm] * 8,
        {4: 0, 5: 1, 6: 2, 7: 3, 8: 4},
        flops=10 * unit,
    )(flags, thirds, f_other, fault, v, s, m, z_a, z_b)
    z_a, z_b = pair_swaps(z_a, z_b, "gz")
    y_shape = f32(nx + 8 + 32 + 16, width)
    v, s, m, fault, y_a, y_b = call(
        widen_kernel,
        "widen",
        (v_shape, s_shape, m_shape, fault_shape, y_shape, y_shape),
        [sm] + [vm] * 8,
        {5: 0, 6: 1, 7: 2, 8: 3},
        flops=50 * unit,
    )(flags, thirds, eighths, z_a, z_b, v, s, m, fault)
    y_shape = f32(4 * (nx + 8), width)
    ahead_b = None
    out_shapes = (HBM((3, ny, nx, width), jnp.float32), HBM((6, ny, nx, width), jnp.float32))
    for step in range(STEPS):
        first, final = step == 0, step == STEPS - 1
        y_a, y_b = pair_swaps(y_a, y_b, "gy")
        v, s, *outs = call(
            functools.partial(inner_kernel, first, final),
            "inner",
            (v_shape, s_shape) + (out_shapes if final else ()),
            [vm] * 3,
            {1: 0, 2: 1},
            [pltpu.SemaphoreType.DMA((9,))] if final else [],
            flops=200 * unit,
            out_specs=[vm, vm] + ([hb, hb] if final else []),
        )(m, v, s)
        args = [flags, eighths] + ([early_a, early_b] if first else []) + [y_a, y_b, m]
        args += ([] if first else [ahead_b]) + [v, s, fault] + outs
        at_state = len(args) - len(outs) - 3
        aliases = {at_state + k: k for k in range(3)}
        shapes, specs = [v_shape, s_shape, fault_shape], [vm, vm, vm]
        scratch = [pltpu.VMEM((2, 3, 2, high, width), jnp.float32)]
        if first:
            shapes.append(f32(2, rows, width))
            specs.append(vm)
        if final:
            shapes += [*out_shapes, jax.ShapeDtypeStruct((ny, width), jnp.float32)]
            specs += [hb, hb, vm]
            scratch.append(pltpu.SemaphoreType.DMA((3 * 3 + 6 * 4,)))
            aliases.update({at_state + 3: 3, at_state + 4: 4})
        else:
            shapes += [y_shape, y_shape]
            specs += [vm, vm]
        v, s, fault, *more = call(
            functools.partial(boundary_kernel, first, final),
            "boundary",
            shapes,
            [sm] + [vm] * (len(args) - 1 - len(outs)) + [hb] * len(outs),
            aliases,
            scratch,
            flops=50 * unit,
            out_specs=specs,
        )(*args)
        if final:
            return tuple(more)
        if first:
            ahead_b, *more = more
        y_a, y_b = more


def solution(mesh):
    in_specs = (
        P(None, "gy", "gx", "gz"),
        P(None, "gy", "gx", "gz"),
        P("gy", "gx", "gz"),
        P("gy", "gx", "gz"),
        P("gy", "gx", "gz"),
        P("gy", "gx", "gz"),
        P("gy", "gx", "gz"),
        P("gy", "gx", "gz"),
        P(None, "gy", "gz"),
        P("gy", "gz"),
        P("gy", "gz"),
        P("gy", "gz"),
        P("gy", "gz"),
        P(),
        P(),
    )
    out_specs = (P(None, "gy", "gx", "gz"), P(None, "gy", "gx", "gz"), P("gy", "gz"))
    return jax.shard_map(local, mesh=mesh, in_specs=in_specs, out_specs=out_specs, check_vma=False)
```

```python
import functools

import jax
import jax.numpy as jnp
from jax import lax
from jax.experimental import pallas as pl
from jax.experimental.pallas import tpu as pltpu
from jax.sharding import PartitionSpec as P

STEPS = 3
NEWTON = 3
DT = 0.2

PAD = 8
HALO = 3
CROSS = 4
STRIP = 8

XX, YY, ZZ, YZ, XZ, XY = range(6)
ALONG_Y = (XY, YY, YZ)
B, C11, C13, C33, C44, C66 = range(6)
FIELDS = [("v", c) for c in range(3)] + [("s", c) for c in range(6)] + [("m", c) for c in range(6)]
PRE_Y, PRE_Z, MASK, STRENGTH, RATE, SLIP, OWN_B, OTHER_B = range(8)

VMEM = pltpu.MemorySpace.VMEM
HBM = pltpu.MemorySpace.HBM
SMEM = pltpu.MemorySpace.SMEM


def in_vmem():
    return pl.BlockSpec(memory_space=VMEM)


def in_hbm():
    return pl.BlockSpec(memory_space=HBM)


def in_smem():
    return pl.BlockSpec(memory_space=SMEM)


def roll(values, by):
    by = by % values.shape[-1]
    return values if by == 0 else pltpu.roll(values, by, values.ndim - 1)


def at(ref, field, tile, y, row):
    return ref[field, tile, y, pl.ds(PAD + row, 8), :]


def z_below(pair, lanes):
    one, two = roll(pair[0], 1), roll(pair[1], 1)
    first = lanes == 0
    return jnp.where(first, two, one), jnp.where(first, one, two)


def z_above(pair, lanes):
    one, two = roll(pair[0], -1), roll(pair[1], -1)
    last = lanes == pair[0].shape[-1] - 1
    return jnp.where(last, two, one), jnp.where(last, one, two)


def trial_tile(v, s, m, y, row, below, lanes):
    both = (0, 1)
    behind = {c: z_below([at(s, c, t, y, row) for t in both], lanes) for c in (XZ, YZ, ZZ)}
    out = []
    for t in both:
        own = {c: at(s, c, t, y, row) for c in range(6)}
        lower_x = {c: own[c] - at(s, c, t, y, row - 1) for c in (XX, XY, XZ)}
        if below is None:
            lower_y = {c: own[c] for c in ALONG_Y}
        else:
            lower_y = {c: own[c] - below(c, t) for c in ALONG_Y}
        scale = DT * m[B, t, y, pl.ds(row, 8), :]
        total = (
            lower_x[XX] + lower_y[XY] + (own[XZ] - behind[XZ][t]),
            lower_x[XY] + lower_y[YY] + (own[YZ] - behind[YZ][t]),
            lower_x[XZ] + lower_y[YZ] + (own[ZZ] - behind[ZZ][t]),
        )
        out.append([at(v, c, t, y, row) + scale * total[c] for c in range(3)])
    return out


def stress_tile(v, s, m, y, row, lanes):
    both = (0, 1)
    own = [[at(v, c, t, y, row) for t in both] for c in range(3)]
    ahead = [z_above(own[c], lanes) for c in range(3)]
    for t in both:
        vx, vy, vz = own[0][t], own[1][t], own[2][t]
        over_x = [at(v, c, t, y, row + 1) for c in range(3)]
        over_y = [at(v, c, t, y + 1, row) for c in range(3)]
        exx, eyy, ezz = over_x[0] - vx, over_y[1] - vy, ahead[2][t] - vz
        c11, c13, c33, c44, c66 = (m[k, t, y, pl.ds(row, 8), :] for k in (C11, C13, C33, C44, C66))
        c12 = c11 - 2.0 * c66
        third = c13 * ezz
        change = {
            XX: c11 * exx + c12 * eyy + third,
            YY: c12 * exx + c11 * eyy + third,
            ZZ: c13 * (exx + eyy) + c33 * ezz,
            YZ: c44 * ((ahead[1][t] - vy) + (over_y[2] - vz)),
            XZ: c44 * ((ahead[0][t] - vx) + (over_x[2] - vz)),
            XY: c66 * ((over_y[0] - vx) + (over_x[1] - vy)),
        }
        for c, gain in change.items():
            s[c, t, y, pl.ds(PAD + row, 8), :] = at(s, c, t, y, row) + DT * gain


def lane_index(like):
    return lax.broadcasted_iota(jnp.int32, like, len(like) - 1)


def strip_pack(pieces, eighths):
    packed = jnp.zeros_like(pieces[0])
    for k, piece in enumerate(pieces):
        packed = jnp.where(eighths == k, roll(piece, STRIP * k + HALO), packed)
    return packed


def strip_take(packed, k):
    return roll(packed, -(STRIP * k + HALO))


def field_ref(kind, v, s, m):
    return {"v": v, "s": s, "m": m}[kind]


def fields_per_plane(ny, width):
    return (width - 5) // HALO // ny


def z_slots(ny, width):
    per_plane = fields_per_plane(ny, width)
    slots = {}
    for f in range(len(FIELDS)):
        for y in range(ny):
            slots[f, y] = (f // per_plane, f % per_plane * ny + y)
    return slots, -(-len(FIELDS) // per_plane)


def row_tiles(nx):
    return [*range(0, nx, 8), cross_row(nx)]


def cross_row(nx):
    return nx + PAD


def packed_row(row, nx):
    return row if row < nx else nx


def edge_kernel(flags, velocity, stress, *rest):
    raw_m, out, sem = rest[:6], rest[6], rest[7]
    ny, nx = velocity.shape[1:3]
    sources = [velocity.at[c] for c in range(3)] + [stress.at[c] for c in range(6)] + list(raw_m)
    for side, row in ((0, nx - CROSS), (1, 0)):

        @pl.when(flags[0] == side)
        def _(row=row):
            copies = []
            for f, source in enumerate(sources):
                for half in range(2):
                    part = source.at[pl.ds(half * (ny // 2), ny // 2), pl.ds(row, CROSS), :]
                    to = out.at[f, :, pl.ds(half * CROSS, CROSS), :]
                    copies.append(pltpu.make_async_copy(part, to, sem.at[2 * f + half]))
            for copy in copies:
                copy.start()
            for copy in copies:
                copy.wait()


def load_kernel(flags, thirds, velocity, stress, *rest):
    raw_m, small = rest[:6], rest[6:13]
    v, s, m, fault, z_a, z_b = rest[13:19]
    pre, ids, mask, rate, slip, region_a, region_normal, sems = rest[19:]
    ny, nx, width = velocity.shape[1:]
    cross = cross_row(nx)
    big = {}
    for c in range(3):
        big["v", c] = (velocity.at[c], v.at[c, 0, pl.ds(0, ny), pl.ds(PAD, nx), :])
    for c in range(6):
        big["s", c] = (stress.at[c], s.at[c, 0, :, pl.ds(PAD, nx), :])
    for c in range(6):
        big["m", c] = (raw_m[c], m.at[c, 0, :, pl.ds(0, nx), :])
    big = {
        key: pltpu.make_async_copy(a, b, sems.at[k]) for k, (key, (a, b)) in enumerate(big.items())
    }
    held = (pre, ids, mask, rate, slip, region_a, region_normal)
    little = [
        pltpu.make_async_copy(a, b, sems.at[len(big) + k])
        for k, (a, b) in enumerate(zip(small, held))
    ]
    for copy in big.values():
        copy.start()
    for copy in little:
        copy.start()
    zeros = jnp.zeros((PAD, width), jnp.float32)
    for t in range(2):
        for y in range(ny):
            for c in (XX, XY, XZ):
                s[c, t, y, 0:PAD, :] = zeros
                s[c, t, y, cross : cross + PAD, :] = zeros
            for c in range(3):
                v[c, t, y, PAD + nx : PAD + nx + PAD, :] = zeros
                v[c, t, y, PAD + cross + 8 : 2 * PAD + cross + 8, :] = zeros

    per_plane = fields_per_plane(ny, width)
    odd = flags[2] == 1
    group = thirds[...]
    for plane in range(z_slots(ny, width)[1]):
        for key in FIELDS[plane * per_plane : (plane + 1) * per_plane]:
            big[key].wait()

        def pack(i, carry, plane=plane):
            for part in range(UNROLL):
                row = pl.multiple_of((i * UNROLL + part) * 8, 8)
                z_emit(z_a, z_b, odd, group, z_pieces(plane, v, s, m, row), plane, row)
            return carry

        lax.fori_loop(0, nx // (8 * UNROLL), pack, 0)
    for copy in little:
        copy.wait()
    kinds = ids[...]
    a_part = jnp.zeros((ny, width), jnp.float32)
    n_part = jnp.zeros((ny, width), jnp.float32)
    for k in range(region_a.shape[0]):
        a_part = jnp.where(kinds == k, region_a[k], a_part)
        n_part = jnp.where(kinds == k, region_normal[k], n_part)
    fault[PRE_Y, 0, 0:ny, :] = pre[0]
    fault[PRE_Z, 0, 0:ny, :] = pre[1]
    fault[MASK, 0, 0:ny, :] = mask[...].astype(jnp.float32)
    fault[STRENGTH, 0, 0:ny, :] = a_part * n_part
    fault[RATE, 0, 0:ny, :] = rate[...]
    fault[SLIP, 0, 0:ny, :] = slip[...]


def early_kernel(flags, v, s, m, y_a, y_b):
    ny, width = m.shape[2], m.shape[4]
    nx = m.shape[3] - 16
    odd = flags[1] == 1
    lanes = lane_index((8, width))
    first = lanes == 0
    span = nx + 8
    for row in row_tiles(nx):
        up = [at(s, c, 0, ny - 1, row) for c in ALONG_Y]
        own = {c: at(s, c, 0, 0, row) for c in range(6)}
        behind = {c: jnp.where(first, 0.0, roll(own[c], 1)) for c in (XZ, YZ, ZZ)}
        lower_x = {c: own[c] - at(s, c, 0, 0, row - 1) for c in (XX, XY, XZ)}
        buoyancy = m[B, 0, 0, pl.ds(row, 8), :]
        total = (
            lower_x[XX] + own[XY] + (own[XZ] - behind[XZ]),
            lower_x[XY] + own[YY] + (own[YZ] - behind[YZ]),
            lower_x[XZ] + own[YZ] + (own[ZZ] - behind[ZZ]),
        )
        at_row = packed_row(row, nx)
        for c in range(3):
            down = at(v, c, 0, 0, row) + DT * buoyancy * total[c]
            to = pl.ds(c * span + at_row, 8)
            y_a[to, :] = jnp.where(odd, down, up[c])
            y_b[to, :] = jnp.where(odd, up[c], down)
        to = pl.ds(3 * span + at_row, 8)
        y_a[to, :] = buoyancy
        y_b[to, :] = buoyancy


UNROLL = 4


def z_emit(z_a, z_b, odd, group, pieces, plane, row):
    up = jnp.zeros_like(pieces[0][1])
    down = up
    for pos, piece in pieces:
        moved = roll(piece, HALO * pos + HALO)
        up = jnp.where(group == pos, moved, up)
        down = jnp.where(group == pos + 1, moved, down)
    z_a[plane, pl.ds(row, 8), :] = jnp.where(odd, down, up)
    z_b[plane, pl.ds(row, 8), :] = jnp.where(odd, up, down)


def z_pieces(plane, v, s, m, row):
    ny, width = m.shape[2], m.shape[4]
    per_plane = fields_per_plane(ny, width)
    pieces = []
    for f, (kind, c) in enumerate(FIELDS[plane * per_plane : (plane + 1) * per_plane]):
        shift = 0 if kind == "m" else PAD
        ref = field_ref(kind, v, s, m)
        for y in range(ny):
            pieces.append((f * ny + y, ref[c, 0, y, pl.ds(row + shift, 8), :]))
    return pieces


def cross_kernel(flags, thirds, f_other, fault, v_in, s_in, m_in, za_in, zb_in, v, s, m, z_a, z_b):
    ny, width = m.shape[2], m.shape[4]
    nx = z_a.shape[1] - 16
    cross = cross_row(nx)
    odd = flags[2] == 1
    group = thirds[...]
    planes = z_slots(ny, width)[1]
    rows = lax.broadcasted_iota(jnp.int32, (8, width), 0)
    minus = flags[0] == 0
    keep = jnp.where(minus, 7 - rows, rows) >= 8 - CROSS
    for f, (kind, c) in enumerate(FIELDS):
        shift = 0 if kind == "m" else PAD
        ref = field_ref(kind, v, s, m)
        for y in range(ny // 2):
            tile = f_other[f, y]
            turned = pltpu.roll(tile, CROSS, 0)
            ref[c, 0, y, cross + shift : cross + shift + 8, :] = jnp.where(
                keep, jnp.where(minus, tile, turned), 0.0
            )
            ref[c, 0, y + ny // 2, cross + shift : cross + shift + 8, :] = jnp.where(
                keep, jnp.where(minus, turned, tile), 0.0
            )
    for plane in range(planes):
        z_emit(z_a, z_b, odd, group, z_pieces(plane, v, s, m, cross), plane, nx)
    z_emit(z_a, z_b, odd, group, [(k, fault[k, 0, 0:8, :]) for k in range(6)], 0, nx + 8)
    zeros = jnp.zeros((8, width), jnp.float32)
    for plane in range(1, planes):
        z_a[plane, pl.ds(nx + 8, 8), :] = zeros
        z_b[plane, pl.ds(nx + 8, 8), :] = zeros


def write_messages(v, s, eighths, odd, y_a, y_b, nx):
    last = s.shape[2] - 1
    span = nx + 8
    for row in row_tiles(nx):
        up = [at(s, c, 0, last, row) for c in ALONG_Y]
        down = [at(v, c, 0, 0, row) for c in range(3)]
        up.append(strip_pack([at(s, c, 1, last, row) for c in ALONG_Y], eighths))
        down.append(strip_pack([at(v, c, 1, 0, row) for c in range(3)], eighths))
        for k in range(4):
            to = pl.ds(k * span + packed_row(row, nx), 8)
            y_a[to, :] = jnp.where(odd, down[k], up[k])
            y_b[to, :] = jnp.where(odd, up[k], down[k])


def partial_trials(v, s, m, nx, lanes):
    for row in row_tiles(nx):
        new = trial_tile(v, s, m, 0, row, None, lanes)
        for t in range(2):
            for c in range(3):
                v[c, t, 0, pl.ds(PAD + row, 8), :] = new[t][c]


class ZHalo:
    def __init__(self, odd, group, r_a, r_b, planes):
        self.odd, self.group, self.r_a, self.r_b, self.planes = odd, group, r_a, r_b, planes

    def take(self, row, wanted):
        for plane in range(self.planes):
            chosen = [(pos, store) for (p, pos), store in wanted if p == plane]
            if chosen:
                from_a = self.r_a[plane, pl.ds(row, 8), :]
                from_b = self.r_b[plane, pl.ds(row, 8), :]
                low = jnp.where(self.odd, from_a, from_b)
                high = jnp.where(self.odd, from_b, from_a)
                for pos, store in chosen:
                    both = jnp.where(self.group == pos, low, high)
                    store(roll(both, -(HALO * pos + HALO)))


def needed_first(kind, c, y, ny):
    if y == 0:
        return kind != "m" or c == B
    return y == ny - 1 and kind == "s" and c in ALONG_Y


def unpack_fields(halo, v, s, m, nx, first):
    ny, width = m.shape[2], m.shape[4]
    slots = z_slots(ny, width)[0]

    def store_to(ref, c, y, row):
        def store(value):
            ref[c, 1, y, pl.ds(row, 8), :] = value

        return store

    def fields(row):
        wanted = []
        for f, (kind, c) in enumerate(FIELDS):
            shift = 0 if kind == "m" else PAD
            ref = field_ref(kind, v, s, m)
            for y in range(ny):
                if needed_first(kind, c, y, ny) == first:
                    wanted.append((slots[f, y], store_to(ref, c, y, row + shift)))
        return wanted

    def unpack(i, carry):
        for part in range(UNROLL):
            row = pl.multiple_of((i * UNROLL + part) * 8, 8)
            halo.take(row, fields(row))
        return carry

    lax.fori_loop(0, nx // (8 * UNROLL), unpack, 0)
    halo.take(nx, fields(cross_row(nx)))


def rest_kernel(flags, thirds, r_a, r_b, v_in, s_in, m_in, v, s, m):
    nx = r_a.shape[1] - 16
    planes = z_slots(m.shape[2], m.shape[4])[1]
    halo = ZHalo(flags[2] == 1, thirds[...], r_a, r_b, planes)
    unpack_fields(halo, v, s, m, nx, False)


def widen_kernel(flags, thirds, eighths, r_a, r_b, v_in, s_in, m_in, f_in, v, s, m, fault, y_a, y_b):
    ny, width = m.shape[2], m.shape[4]
    nx = r_a.shape[1] - 16
    planes = z_slots(ny, width)[1]
    odd_y = flags[1] == 1
    lanes = lane_index((8, width))
    halo = ZHalo(flags[2] == 1, thirds[...], r_a, r_b, planes)
    unpack_fields(halo, v, s, m, nx, True)

    def store_fault(k):
        def store(value):
            fault[k, 1, 0:8, :] = value

        return store

    halo.take(nx + 8, [((0, k), store_fault(k)) for k in range(6)])
    partial_trials(v, s, m, nx, lanes)
    last = ny - 1
    halos = eighths[...]
    for row in row_tiles(nx):
        buoyancy = m[B, 1, 0, pl.ds(row, 8), :]
        up = [at(s, c, 1, last, row) for c in ALONG_Y] + [buoyancy]
        down = [
            jnp.where(lanes == HALO, roll(at(v, c, 0, 0, row), HALO), at(v, c, 1, 0, row))
            for c in range(3)
        ] + [buoyancy]
        up, down = strip_pack(up, halos), strip_pack(down, halos)
        to = pl.ds(packed_row(row, nx), 8)
        y_a[to, :] = jnp.where(odd_y, down, up)
        y_b[to, :] = jnp.where(odd_y, up, down)
    for t in range(2):
        for k in range(8):
            line = fault[min(k, 5), t, 0:1, :]
            row = nx + 8 + 8 * t + k
            y_a[row : row + 1, :] = line
            y_b[row : row + 1, :] = line


def inner_kernel(first, final, m, v_in, s_in, v, s, *outs):
    ny, width = m.shape[2], m.shape[4]
    nx = m.shape[3] - 16
    lanes = lane_index((8, width))

    if not first:

        def ends(y, carry):
            for row in (0, nx - 8, cross_row(nx)):
                stress_tile(v, s, m, y, row, lanes)
            return carry

        lax.fori_loop(1, ny - 1, ends, 0)

    def trials(y, carry):
        for row in row_tiles(nx):
            new = trial_tile(
                v, s, m, y, row, lambda c, t, row=row: at(s, c, t, y - 1, row), lanes
            )
            for t in range(2):
                for c in range(3):
                    v[c, t, y, pl.ds(PAD + row, 8), :] = new[t][c]
        return carry

    lax.fori_loop(1, ny, trials, 0)
    copies = []
    if final:
        new_v, new_s, sems = outs
        for c in range(3):
            part = v.at[c, 0, pl.ds(1, ny - 1), pl.ds(PAD + 8, nx - 16), :]
            to = new_v.at[c, pl.ds(1, ny - 1), pl.ds(8, nx - 16), :]
            copies.append(pltpu.make_async_copy(part, to, sems.at[c]))
            copies[-1].start()

    def stresses(y, carry):
        for row in range(8, nx - 8, 8):
            stress_tile(v, s, m, y, row, lanes)
        return carry

    lax.fori_loop(1, ny - 1, stresses, 0)
    if final:
        for c in range(6):
            part = s.at[c, 0, pl.ds(1, ny - 2), pl.ds(PAD + 8, nx - 16), :]
            to = new_s.at[c, pl.ds(1, ny - 2), pl.ds(8, nx - 16), :]
            copies.append(pltpu.make_async_copy(part, to, sems.at[3 + c]))
            copies[-1].start()
        for copy in copies:
            copy.wait()


def boundary_kernel(first, final, flags, eighths, *refs):
    refs = list(refs)

    def pop(n):
        out = refs[:n]
        del refs[:n]
        return out

    early_a, early_b = pop(2) if first else (None, None)
    r_a, r_b, m = pop(3)
    if not first:
        (ahead_b,) = pop(1)
    pop(3)
    if final:
        pop(2)
    v, s, fault = pop(3)
    if first:
        (ahead_b,) = pop(1)
    if final:
        new_v, new_s, slip_out, rows, sems = refs
    else:
        y_a, y_b, rows = refs
    ny, width = m.shape[2], m.shape[4]
    nx = m.shape[3] - 16
    cross = cross_row(nx)
    span = nx + 8
    odd = flags[1] == 1
    lanes = lane_index((8, width))
    halos = eighths[...]

    def received(row):
        at_row = packed_row(row, nx)
        if not first:
            from_a = [r_a[pl.ds(k * span + at_row, 8), :] for k in range(4)]
            from_b = [r_b[pl.ds(k * span + at_row, 8), :] for k in range(4)]
        else:
            from_a = [early_a[pl.ds(k * span + at_row, 8), :] for k in range(4)]
            from_b = [early_b[pl.ds(k * span + at_row, 8), :] for k in range(4)]
            from_a.append(r_a[pl.ds(at_row, 8), :])
            from_b.append(r_b[pl.ds(at_row, 8), :])
        low = [jnp.where(odd, a, b) for a, b in zip(from_a, from_b)]
        high = [jnp.where(odd, b, a) for a, b in zip(from_a, from_b)]
        if first:
            for c in range(3):
                column = roll(high[-1], -(STRIP * c + 2 * HALO))
                high[c] = jnp.where(lanes == 0, column, high[c])
        return low, high

    if first:
        for t in range(2):
            to = pl.ds(span + 8 * t, 8)
            lines = jnp.where(odd, r_b[to, :], r_a[to, :])
            for k in range(6):
                fault[k, t, ny : ny + 1, :] = lines[k : k + 1, :]
    for row in row_tiles(nx):
        low, high = received(row)
        if first:
            ahead_b[0, pl.ds(row, 8), :] = high[3]
            ahead_b[1, pl.ds(row, 8), :] = strip_take(high[-1], 3)
        for t in range(2):
            scale = DT * m[B, t, 0, pl.ds(row, 8), :]
            scale_ahead = DT * ahead_b[t, pl.ds(row, 8), :]
            for c in range(3):
                low_c = low[c] if t == 0 else strip_take(low[-1], c)
                high_c = high[c] if t == 0 else strip_take(high[-1], c)
                v[c, t, 0, pl.ds(PAD + row, 8), :] = at(v, c, t, 0, row) - scale * low_c
                v[c, t, ny, pl.ds(PAD + row, 8), :] = high_c - scale_ahead * at(
                    s, ALONG_Y[c], t, ny - 1, row
                )

    places = ((0, (nx - 1, cross)), (1, (0, cross + 7)))
    for side, pair in places:

        @pl.when(flags[0] == side)
        def _(pair=pair):
            for which, row in enumerate(pair):
                for t in range(2):
                    for y in range(ny + 1):
                        for c in range(3):
                            rows[which, c, t, y : y + 1, :] = v[
                                c, t, y, PAD + row : PAD + row + 1, :
                            ]
                        if first:
                            if y < ny:
                                line = m[B, t, y, row : row + 1, :]
                            else:
                                line = ahead_b[t, row : row + 1, :]
                            fault[OWN_B + which, t, y : y + 1, :] = line

    minus = flags[0] == 0
    sign = jnp.where(minus, DT, -DT)
    for t in range(2):
        for half in range(0, fault.shape[2], 8):
            part = slice(half, half + 8)
            own = [rows[0, c, t, part, :] for c in range(3)]
            other = [rows[1, c, t, part, :] for c in range(3)]
            par = [fault[k, t, part, :] for k in range(8)]
            m_side = [jnp.where(minus, a, b) for a, b in zip(own, other)]
            p_side = [jnp.where(minus, b, a) for a, b in zip(own, other)]
            m_b = jnp.where(minus, par[OWN_B], par[OTHER_B])
            p_b = jnp.where(minus, par[OTHER_B], par[OWN_B])
            traction, slip = friction(m_side, p_side, m_b, p_b, par)
            fault[SLIP, t, part, :] = slip
            for c in range(3):
                rows[0, c, t, part, :] = own[c] + sign * par[OWN_B] * traction[c]
                rows[1, c, t, part, :] = other[c] - sign * par[OTHER_B] * traction[c]
    for side, pair in places:

        @pl.when(flags[0] == side)
        def _(pair=pair):
            for which, row in enumerate(pair):
                for c in range(3):
                    for t in range(2):
                        for y in range(ny + 1):
                            v[c, t, y, PAD + row : PAD + row + 1, :] = rows[
                                which, c, t, y : y + 1, :
                            ]

    def planes(i, carry):
        for row in row_tiles(nx)[:-1] if final else row_tiles(nx):
            stress_tile(v, s, m, i * (ny - 1), row, lanes)
        return carry

    lax.fori_loop(0, 2, planes, 0)
    if not final:
        partial_trials(v, s, m, nx, lanes)
        write_messages(v, s, halos, odd, y_a, y_b, nx)
        return

    def ends(y, carry):
        for row in (0, nx - 8):
            stress_tile(v, s, m, y, row, lanes)
        return carry

    lax.fori_loop(1, ny - 1, ends, 0)
    slip_out[...] = fault[SLIP, 0, 0:ny, :]
    copies = []
    for ref, out, fields, whole in ((v, new_v, 3, (0,)), (s, new_s, 6, (0, ny - 1))):
        inside = ny - len(whole)
        for c in range(fields):
            for y in whole:
                copies.append((ref.at[c, 0, y, pl.ds(PAD, nx), :], out.at[c, y]))
            for row in (0, nx - 8):
                copies.append(
                    (
                        ref.at[c, 0, pl.ds(1, inside), pl.ds(PAD + row, 8), :],
                        out.at[c, pl.ds(1, inside), pl.ds(row, 8), :],
                    )
                )
    copies = [pltpu.make_async_copy(a, b, sems.at[k]) for k, (a, b) in enumerate(copies)]
    for copy in copies:
        copy.start()
    for copy in copies:
        copy.wait()


def inverse_sinh(values):
    size = jnp.abs(values)
    sign = jnp.where(values > 0.0, 1.0, jnp.where(values < 0.0, -1.0, 0.0))
    return sign * jnp.log(size + jnp.sqrt(size * size + 1.0))


def friction(minus_side, plus_side, minus_b, plus_b, par):
    total = DT * (minus_b + plus_b)
    impedance = 1.0 / jnp.where(total > 0.0, total, 1.0)
    jump = [p - q for p, q in zip(plus_side, minus_side)]
    locked_y = par[PRE_Y] + impedance * jump[1]
    locked_z = par[PRE_Z] + impedance * jump[2]
    magnitude = jnp.sqrt(locked_y * locked_y + locked_z * locked_z + 1.0)
    rate, strength, slip = par[RATE], par[STRENGTH], par[SLIP]
    for _ in range(NEWTON):
        scaled = rate * slip
        residual = magnitude - impedance * slip - strength * inverse_sinh(scaled)
        tangent = -impedance - strength * rate / jnp.sqrt(1.0 + scaled * scaled)
        slip = slip - residual / tangent
    slip = slip * par[MASK]
    retained = 1.0 - impedance * slip / magnitude
    traction = (
        impedance * jump[0],
        retained * locked_y - par[PRE_Y],
        retained * locked_z - par[PRE_Z],
    )
    return traction, slip


def f32(*shape):
    return VMEM(shape, jnp.float32)


def call(kernel, name, outs, in_specs, aliases, scratch=(), flops=0, out_specs=None):
    return pl.pallas_call(
        kernel,
        out_shape=tuple(outs),
        in_specs=in_specs,
        out_specs=tuple(out_specs or [in_vmem() for _ in outs]),
        input_output_aliases=aliases,
        scratch_shapes=list(scratch),
        compiler_params=pltpu.CompilerParams(vmem_limit_bytes=8 << 20),
        cost_estimate=pl.CostEstimate(flops=flops, bytes_accessed=0, transcendentals=0),
        name=name,
    )


def pair_swaps(a, b, axis):
    size = lax.axis_size(axis)
    out = []
    for value, start in ((a, 0), (b, 1)):
        pairs = []
        for i in range(start, size - 1, 2):
            pairs += [(i, i + 1), (i + 1, i)]
        out.append(lax.ppermute(value, axis, pairs))
    return out


def local(
    velocity,
    stress,
    buoyancy,
    stiff_xx,
    stiff_xz,
    stiff_zz,
    shear_vert,
    shear_horiz,
    prestress,
    fault_mask,
    region_ids,
    inverse_rate,
    slip_prev,
    region_a,
    region_normal,
):
    ny, nx, width = buoyancy.shape
    across, along, dip = (lax.axis_index(k) for k in ("gx", "gy", "gz"))
    flags = jnp.stack([across, along % 2, dip % 2]).astype(jnp.int32)
    lanes = jnp.broadcast_to(jnp.arange(width, dtype=jnp.int32), (8, width))
    thirds, eighths = lanes // HALO, lanes // STRIP
    rows = cross_row(nx) + 8
    high = 8 * ((ny + 1 + 7) // 8)
    v_shape = f32(3, 2, ny + 1, rows + 2 * PAD, width)
    s_shape = f32(6, 2, ny, rows + 2 * PAD, width)
    m_shape = f32(6, 2, ny, rows, width)
    fault_shape = f32(8, 2, high, width)
    planes = z_slots(ny, width)[1]
    z_shape = f32(planes, nx + 16, width)
    unit = ny * nx * width
    vm, hb, sm = in_vmem(), in_hbm(), in_smem()
    raw = [velocity, stress, buoyancy, stiff_xx, stiff_xz, stiff_zz, shear_vert, shear_horiz]
    raw += [prestress, region_ids, fault_mask, inverse_rate, slip_prev, region_a, region_normal]
    raw = [pltpu.with_memory_space_constraint(k, HBM) for k in raw]

    f_shape = f32(len(FIELDS), ny // 2, 8, width)
    (f_own,) = call(
        edge_kernel,
        "edge",
        (f_shape,),
        [sm] + [hb] * 8,
        {},
        [pltpu.SemaphoreType.DMA((2 * len(FIELDS),))],
        flops=unit,
    )(flags, *raw[:8])
    f_other = lax.ppermute(f_own, "gx", [(i, i ^ 1) for i in range(lax.axis_size("gx"))])
    v, s, m, fault, z_a, z_b = call(
        load_kernel,
        "load",
        (v_shape, s_shape, m_shape, fault_shape, z_shape, z_shape),
        [sm, vm] + [hb] * 15,
        {},
        [
            pltpu.VMEM(prestress.shape, jnp.float32),
            pltpu.VMEM(region_ids.shape, jnp.int32),
            pltpu.VMEM(fault_mask.shape, jnp.int32),
            pltpu.VMEM(inverse_rate.shape, jnp.float32),
            pltpu.VMEM(slip_prev.shape, jnp.float32),
            pltpu.SMEM(region_a.shape, jnp.float32),
            pltpu.SMEM(region_normal.shape, jnp.float32),
            pltpu.SemaphoreType.DMA((22,)),
        ],
        flops=100 * unit,
    )(flags, thirds, *raw)
    v, s, m, z_a, z_b = call(
        cross_kernel,
        "cross",
        (v_shape, s_shape, m_shape, z_shape, z_shape),
        [sm] + [vm] * 8,
        {4: 0, 5: 1, 6: 2, 7: 3, 8: 4},
        flops=10 * unit,
    )(flags, thirds, f_other, fault, v, s, m, z_a, z_b)
    z_a, z_b = pair_swaps(z_a, z_b, "gz")
    y_shape = f32(4 * (nx + 8), width)
    early_a, early_b = call(
        early_kernel, "early", (y_shape, y_shape), [sm] + [vm] * 3, {}, flops=10 * unit
    )(flags, v, s, m)
    early_a, early_b = pair_swaps(early_a, early_b, "gy")
    y_shape = f32(nx + 8 + 16, width)
    v, s, m, fault, y_a, y_b = call(
        widen_kernel,
        "widen",
        (v_shape, s_shape, m_shape, fault_shape, y_shape, y_shape),
        [sm] + [vm] * 8,
        {5: 0, 6: 1, 7: 2, 8: 3},
        flops=50 * unit,
    )(flags, thirds, eighths, z_a, z_b, v, s, m, fault)
    v, s, m = call(
        rest_kernel,
        "rest",
        (v_shape, s_shape, m_shape),
        [sm] + [vm] * 6,
        {4: 0, 5: 1, 6: 2},
        flops=50 * unit,
    )(flags, thirds, z_a, z_b, v, s, m)
    y_shape = f32(4 * (nx + 8), width)
    ahead_b = None
    out_shapes = (HBM((3, ny, nx, width), jnp.float32), HBM((6, ny, nx, width), jnp.float32))
    for step in range(STEPS):
        first, final = step == 0, step == STEPS - 1
        y_a, y_b = pair_swaps(y_a, y_b, "gy")
        v, s, *outs = call(
            functools.partial(inner_kernel, first, final),
            "inner",
            (v_shape, s_shape) + (out_shapes if final else ()),
            [vm] * 3,
            {1: 0, 2: 1},
            [pltpu.SemaphoreType.DMA((9,))] if final else [],
            flops=200 * unit,
            out_specs=[vm, vm] + ([hb, hb] if final else []),
        )(m, v, s)
        args = [flags, eighths] + ([early_a, early_b] if first else []) + [y_a, y_b, m]
        args += ([] if first else [ahead_b]) + [v, s, fault] + outs
        at_state = len(args) - len(outs) - 3
        aliases = {at_state + k: k for k in range(3)}
        shapes, specs = [v_shape, s_shape, fault_shape], [vm, vm, vm]
        scratch = [pltpu.VMEM((2, 3, 2, high, width), jnp.float32)]
        if first:
            shapes.append(f32(2, rows, width))
            specs.append(vm)
        if final:
            shapes += [*out_shapes, jax.ShapeDtypeStruct((ny, width), jnp.float32)]
            specs += [hb, hb, vm]
            scratch.append(pltpu.SemaphoreType.DMA((3 * 3 + 6 * 4,)))
            aliases.update({at_state + 3: 3, at_state + 4: 4})
        else:
            shapes += [y_shape, y_shape]
            specs += [vm, vm]
        v, s, fault, *more = call(
            functools.partial(boundary_kernel, first, final),
            "boundary",
            shapes,
            [sm] + [vm] * (len(args) - 1 - len(outs)) + [hb] * len(outs),
            aliases,
            scratch,
            flops=50 * unit,
            out_specs=specs,
        )(*args)
        if final:
            return tuple(more)
        if first:
            ahead_b, *more = more
        y_a, y_b = more


def solution(mesh):
    in_specs = (
        P(None, "gy", "gx", "gz"),
        P(None, "gy", "gx", "gz"),
        P("gy", "gx", "gz"),
        P("gy", "gx", "gz"),
        P("gy", "gx", "gz"),
        P("gy", "gx", "gz"),
        P("gy", "gx", "gz"),
        P("gy", "gx", "gz"),
        P(None, "gy", "gz"),
        P("gy", "gz"),
        P("gy", "gz"),
        P("gy", "gz"),
        P("gy", "gz"),
        P(),
        P(),
    )
    out_specs = (P(None, "gy", "gx", "gz"), P(None, "gy", "gx", "gz"), P("gy", "gz"))
    return jax.shard_map(local, mesh=mesh, in_specs=in_specs, out_specs=out_specs, check_vma=False)
```

```python
import functools

import jax
import jax.numpy as jnp
from jax import lax
from jax.experimental import pallas as pl
from jax.experimental.pallas import tpu as pltpu
from jax.sharding import PartitionSpec as P

STEPS = 3
NEWTON = 3
DT = 0.2

PAD = 8
HALO = 3
CROSS = 4
STRIP = 8

XX, YY, ZZ, YZ, XZ, XY = range(6)
ALONG_Y = (XY, YY, YZ)
B, C11, C13, C33, C44, C66 = range(6)
FIELDS = [("v", c) for c in range(3)] + [("s", c) for c in range(6)] + [("m", c) for c in range(6)]
PRE_Y, PRE_Z, MASK, STRENGTH, RATE, SLIP, OWN_B, OTHER_B = range(8)

VMEM = pltpu.MemorySpace.VMEM
HBM = pltpu.MemorySpace.HBM
SMEM = pltpu.MemorySpace.SMEM


def in_vmem():
    return pl.BlockSpec(memory_space=VMEM)


def in_hbm():
    return pl.BlockSpec(memory_space=HBM)


def in_smem():
    return pl.BlockSpec(memory_space=SMEM)


def roll(values, by):
    by = by % values.shape[-1]
    return values if by == 0 else pltpu.roll(values, by, values.ndim - 1)


def at(ref, field, tile, y, row):
    return ref[field, tile, y, pl.ds(PAD + row, 8), :]


def z_below(pair, lanes):
    one, two = roll(pair[0], 1), roll(pair[1], 1)
    first = lanes == 0
    return jnp.where(first, two, one), jnp.where(first, one, two)


def z_above(pair, lanes):
    one, two = roll(pair[0], -1), roll(pair[1], -1)
    last = lanes == pair[0].shape[-1] - 1
    return jnp.where(last, two, one), jnp.where(last, one, two)


def trial_tile(v, s, m, y, row, below, lanes):
    both = (0, 1)
    behind = {c: z_below([at(s, c, t, y, row) for t in both], lanes) for c in (XZ, YZ, ZZ)}
    out = []
    for t in both:
        own = {c: at(s, c, t, y, row) for c in range(6)}
        lower_x = {c: own[c] - at(s, c, t, y, row - 1) for c in (XX, XY, XZ)}
        if below is None:
            lower_y = {c: own[c] for c in ALONG_Y}
        else:
            lower_y = {c: own[c] - below(c, t) for c in ALONG_Y}
        scale = DT * m[B, t, y, pl.ds(row, 8), :]
        total = (
            lower_x[XX] + lower_y[XY] + (own[XZ] - behind[XZ][t]),
            lower_x[XY] + lower_y[YY] + (own[YZ] - behind[YZ][t]),
            lower_x[XZ] + lower_y[YZ] + (own[ZZ] - behind[ZZ][t]),
        )
        out.append([at(v, c, t, y, row) + scale * total[c] for c in range(3)])
    return out


def stress_tile(v, s, m, y, row, lanes, tiles=(0, 1)):
    both = (0, 1)
    own = [[at(v, c, t, y, row) for t in both] for c in range(3)]
    ahead = [z_above(own[c], lanes) for c in range(3)]
    for t in tiles:
        vx, vy, vz = own[0][t], own[1][t], own[2][t]
        over_x = [at(v, c, t, y, row + 1) for c in range(3)]
        over_y = [at(v, c, t, y + 1, row) for c in range(3)]
        exx, eyy, ezz = over_x[0] - vx, over_y[1] - vy, ahead[2][t] - vz
        c11, c13, c33, c44, c66 = (m[k, t, y, pl.ds(row, 8), :] for k in (C11, C13, C33, C44, C66))
        c12 = c11 - 2.0 * c66
        third = c13 * ezz
        change = {
            XX: c11 * exx + c12 * eyy + third,
            YY: c12 * exx + c11 * eyy + third,
            ZZ: c13 * (exx + eyy) + c33 * ezz,
            YZ: c44 * ((ahead[1][t] - vy) + (over_y[2] - vz)),
            XZ: c44 * ((ahead[0][t] - vx) + (over_x[2] - vz)),
            XY: c66 * ((over_y[0] - vx) + (over_x[1] - vy)),
        }
        for c, gain in change.items():
            s[c, t, y, pl.ds(PAD + row, 8), :] = at(s, c, t, y, row) + DT * gain


def lane_index(like):
    return lax.broadcasted_iota(jnp.int32, like, len(like) - 1)


SLOTS = 4


def strip_tile(up, down, eighths):
    packed = jnp.zeros_like(up[0])
    for start, pieces in ((0, up), (SLOTS, down)):
        for k, piece in enumerate(pieces):
            moved = roll(piece, STRIP * (start + k) + HALO)
            packed = jnp.where(eighths == start + k, moved, packed)
    return packed


def strip_take(packed, slot):
    return roll(packed, -(STRIP * slot + HALO))


def strip_send(strips, cross_tile, count, odd, y_a, y_b, base):
    turned = strips[...].T
    for j in range(0, STRIP * count, 8):
        up = turned[j : j + 8, :]
        down = turned[STRIP * SLOTS + j : STRIP * SLOTS + j + 8, :]
        y_a[base + j : base + j + 8, :] = jnp.where(odd, down, up)
        y_b[base + j : base + j + 8, :] = jnp.where(odd, up, down)
    other = roll(cross_tile, -STRIP * SLOTS)
    last = base + STRIP * count
    y_a[last : last + 8, :] = jnp.where(odd, other, cross_tile)
    y_b[last : last + 8, :] = jnp.where(odd, cross_tile, other)


def strip_receive(r_a, r_b, base, count, odd, turned, strips, lanes):
    turned[...] = jnp.zeros_like(turned)
    for j in range(0, STRIP * count, 8):
        from_a, from_b = r_a[base + j : base + j + 8, :], r_b[base + j : base + j + 8, :]
        turned[j : j + 8, :] = jnp.where(odd, from_a, from_b)
        start = STRIP * SLOTS + j
        turned[start : start + 8, :] = jnp.where(odd, from_b, from_a)
    strips[...] = turned[...].T
    last = base + STRIP * count
    from_a, from_b = r_a[last : last + 8, :], r_b[last : last + 8, :]
    low, high = jnp.where(odd, from_a, from_b), jnp.where(odd, from_b, from_a)
    return jnp.where(lanes < STRIP * SLOTS, low, roll(high, STRIP * SLOTS))


def field_ref(kind, v, s, m):
    return {"v": v, "s": s, "m": m}[kind]


def fields_per_plane(ny, width):
    return (width - 5) // HALO // ny


def z_slots(ny, width):
    per_plane = fields_per_plane(ny, width)
    slots = {}
    for f in range(len(FIELDS)):
        for y in range(ny):
            slots[f, y] = (f // per_plane, f % per_plane * ny + y)
    return slots, -(-len(FIELDS) // per_plane)


def row_tiles(nx):
    return [*range(0, nx, 8), cross_row(nx)]


def cross_row(nx):
    return nx + PAD


def packed_row(row, nx):
    return row if row < nx else nx


def edge_kernel(flags, velocity, stress, *rest):
    raw_m, out, sem = rest[:6], rest[6], rest[7]
    ny, nx = velocity.shape[1:3]
    sources = [velocity.at[c] for c in range(3)] + [stress.at[c] for c in range(6)] + list(raw_m)
    for side, row in ((0, nx - CROSS), (1, 0)):

        @pl.when(flags[0] == side)
        def _(row=row):
            copies = []
            for f, source in enumerate(sources):
                for half in range(2):
                    part = source.at[pl.ds(half * (ny // 2), ny // 2), pl.ds(row, CROSS), :]
                    to = out.at[f, :, pl.ds(half * CROSS, CROSS), :]
                    copies.append(pltpu.make_async_copy(part, to, sem.at[2 * f + half]))
            for copy in copies:
                copy.start()
            for copy in copies:
                copy.wait()


def load_kernel(flags, thirds, velocity, stress, *rest):
    raw_m, small = rest[:6], rest[6:13]
    v, s, m, fault, z_a, z_b = rest[13:19]
    pre, ids, mask, rate, slip, region_a, region_normal, sems = rest[19:]
    ny, nx, width = velocity.shape[1:]
    cross = cross_row(nx)
    big = {}
    for c in range(3):
        big["v", c] = (velocity.at[c], v.at[c, 0, pl.ds(0, ny), pl.ds(PAD, nx), :])
    for c in range(6):
        big["s", c] = (stress.at[c], s.at[c, 0, :, pl.ds(PAD, nx), :])
    for c in range(6):
        big["m", c] = (raw_m[c], m.at[c, 0, :, pl.ds(0, nx), :])
    big = {
        key: pltpu.make_async_copy(a, b, sems.at[k]) for k, (key, (a, b)) in enumerate(big.items())
    }
    held = (pre, ids, mask, rate, slip, region_a, region_normal)
    little = [
        pltpu.make_async_copy(a, b, sems.at[len(big) + k])
        for k, (a, b) in enumerate(zip(small, held))
    ]
    for copy in big.values():
        copy.start()
    for copy in little:
        copy.start()
    zeros = jnp.zeros((PAD, width), jnp.float32)
    for t in range(2):
        for y in range(ny):
            for c in (XX, XY, XZ):
                s[c, t, y, 0:PAD, :] = zeros
                s[c, t, y, cross : cross + PAD, :] = zeros
            for c in range(3):
                v[c, t, y, PAD + nx : PAD + nx + PAD, :] = zeros
                v[c, t, y, PAD + cross + 8 : 2 * PAD + cross + 8, :] = zeros

    per_plane = fields_per_plane(ny, width)
    odd = flags[2] == 1
    group = thirds[...]
    for plane in range(z_slots(ny, width)[1]):
        for key in FIELDS[plane * per_plane : (plane + 1) * per_plane]:
            big[key].wait()

        def pack(i, carry, plane=plane):
            for part in range(UNROLL):
                row = pl.multiple_of((i * UNROLL + part) * 8, 8)
                z_emit(z_a, z_b, odd, group, z_pieces(plane, v, s, m, row), plane, row)
            return carry

        lax.fori_loop(0, nx // (8 * UNROLL), pack, 0)
    for copy in little:
        copy.wait()
    kinds = ids[...]
    a_part = jnp.zeros((ny, width), jnp.float32)
    n_part = jnp.zeros((ny, width), jnp.float32)
    for k in range(region_a.shape[0]):
        a_part = jnp.where(kinds == k, region_a[k], a_part)
        n_part = jnp.where(kinds == k, region_normal[k], n_part)
    fault[PRE_Y, 0, 0:ny, :] = pre[0]
    fault[PRE_Z, 0, 0:ny, :] = pre[1]
    fault[MASK, 0, 0:ny, :] = mask[...].astype(jnp.float32)
    fault[STRENGTH, 0, 0:ny, :] = a_part * n_part
    fault[RATE, 0, 0:ny, :] = rate[...]
    fault[SLIP, 0, 0:ny, :] = slip[...]


def early_kernel(flags, v, s, m, y_a, y_b):
    ny, width = m.shape[2], m.shape[4]
    nx = m.shape[3] - 16
    odd = flags[1] == 1
    lanes = lane_index((8, width))
    first = lanes == 0
    span = nx + 8
    for row in row_tiles(nx):
        up = [at(s, c, 0, ny - 1, row) for c in ALONG_Y]
        own = {c: at(s, c, 0, 0, row) for c in range(6)}
        behind = {c: jnp.where(first, 0.0, roll(own[c], 1)) for c in (XZ, YZ, ZZ)}
        lower_x = {c: own[c] - at(s, c, 0, 0, row - 1) for c in (XX, XY, XZ)}
        buoyancy = m[B, 0, 0, pl.ds(row, 8), :]
        total = (
            lower_x[XX] + own[XY] + (own[XZ] - behind[XZ]),
            lower_x[XY] + own[YY] + (own[YZ] - behind[YZ]),
            lower_x[XZ] + own[YZ] + (own[ZZ] - behind[ZZ]),
        )
        at_row = packed_row(row, nx)
        for c in range(3):
            down = at(v, c, 0, 0, row) + DT * buoyancy * total[c]
            to = pl.ds(c * span + at_row, 8)
            y_a[to, :] = jnp.where(odd, down, up[c])
            y_b[to, :] = jnp.where(odd, up[c], down)
        to = pl.ds(3 * span + at_row, 8)
        y_a[to, :] = buoyancy
        y_b[to, :] = buoyancy


UNROLL = 4


def z_emit(z_a, z_b, odd, group, pieces, plane, row):
    up = jnp.zeros_like(pieces[0][1])
    down = up
    for pos, piece in pieces:
        moved = roll(piece, HALO * pos + HALO)
        up = jnp.where(group == pos, moved, up)
        down = jnp.where(group == pos + 1, moved, down)
    z_a[plane, pl.ds(row, 8), :] = jnp.where(odd, down, up)
    z_b[plane, pl.ds(row, 8), :] = jnp.where(odd, up, down)


def z_pieces(plane, v, s, m, row):
    ny, width = m.shape[2], m.shape[4]
    per_plane = fields_per_plane(ny, width)
    pieces = []
    for f, (kind, c) in enumerate(FIELDS[plane * per_plane : (plane + 1) * per_plane]):
        shift = 0 if kind == "m" else PAD
        ref = field_ref(kind, v, s, m)
        for y in range(ny):
            pieces.append((f * ny + y, ref[c, 0, y, pl.ds(row + shift, 8), :]))
    return pieces


def cross_kernel(flags, thirds, f_other, fault, v_in, s_in, m_in, za_in, zb_in, v, s, m, z_a, z_b):
    ny, width = m.shape[2], m.shape[4]
    nx = z_a.shape[1] - 16
    cross = cross_row(nx)
    odd = flags[2] == 1
    group = thirds[...]
    planes = z_slots(ny, width)[1]
    rows = lax.broadcasted_iota(jnp.int32, (8, width), 0)
    minus = flags[0] == 0
    keep = jnp.where(minus, 7 - rows, rows) >= 8 - CROSS
    for f, (kind, c) in enumerate(FIELDS):
        shift = 0 if kind == "m" else PAD
        ref = field_ref(kind, v, s, m)
        for y in range(ny // 2):
            tile = f_other[f, y]
            turned = pltpu.roll(tile, CROSS, 0)
            ref[c, 0, y, cross + shift : cross + shift + 8, :] = jnp.where(
                keep, jnp.where(minus, tile, turned), 0.0
            )
            ref[c, 0, y + ny // 2, cross + shift : cross + shift + 8, :] = jnp.where(
                keep, jnp.where(minus, turned, tile), 0.0
            )
    for plane in range(planes):
        z_emit(z_a, z_b, odd, group, z_pieces(plane, v, s, m, cross), plane, nx)
    z_emit(z_a, z_b, odd, group, [(k, fault[k, 0, 0:8, :]) for k in range(6)], 0, nx + 8)
    zeros = jnp.zeros((8, width), jnp.float32)
    for plane in range(1, planes):
        z_a[plane, pl.ds(nx + 8, 8), :] = zeros
        z_b[plane, pl.ds(nx + 8, 8), :] = zeros


def write_messages(v, s, eighths, odd, y_a, y_b, strips, nx):
    last = s.shape[2] - 1
    span = nx + 8
    for row in row_tiles(nx):
        up = [at(s, c, 0, last, row) for c in ALONG_Y]
        down = [at(v, c, 0, 0, row) for c in range(3)]
        for k in range(3):
            to = pl.ds(k * span + packed_row(row, nx), 8)
            y_a[to, :] = jnp.where(odd, down[k], up[k])
            y_b[to, :] = jnp.where(odd, up[k], down[k])
        up = [at(s, c, 1, last, row) for c in ALONG_Y]
        down = [at(v, c, 1, 0, row) for c in range(3)]
        tile = strip_tile(up, down, eighths)
        if row < nx:
            strips[row : row + 8, :] = tile
    strip_send(strips, tile, 3, odd, y_a, y_b, 3 * span)


def partial_trials(v, s, m, nx, lanes):
    for row in row_tiles(nx):
        new = trial_tile(v, s, m, 0, row, None, lanes)
        for t in range(2):
            for c in range(3):
                v[c, t, 0, pl.ds(PAD + row, 8), :] = new[t][c]


class ZHalo:
    def __init__(self, odd, group, r_a, r_b, planes):
        self.odd, self.group, self.r_a, self.r_b, self.planes = odd, group, r_a, r_b, planes

    def take(self, row, wanted):
        for plane in range(self.planes):
            chosen = [(pos, store) for (p, pos), store in wanted if p == plane]
            if chosen:
                from_a = self.r_a[plane, pl.ds(row, 8), :]
                from_b = self.r_b[plane, pl.ds(row, 8), :]
                low = jnp.where(self.odd, from_a, from_b)
                high = jnp.where(self.odd, from_b, from_a)
                for pos, store in chosen:
                    both = jnp.where(self.group == pos, low, high)
                    store(roll(both, -(HALO * pos + HALO)))


def needed_first(kind, c, y, ny):
    if y == 0:
        return kind != "m" or c == B
    return y == ny - 1 and kind == "s" and c in ALONG_Y


def unpack_fields(halo, v, s, m, nx, first):
    ny, width = m.shape[2], m.shape[4]
    slots = z_slots(ny, width)[0]

    def store_to(ref, c, y, row):
        def store(value):
            ref[c, 1, y, pl.ds(row, 8), :] = value

        return store

    def fields(row):
        wanted = []
        for f, (kind, c) in enumerate(FIELDS):
            shift = 0 if kind == "m" else PAD
            ref = field_ref(kind, v, s, m)
            for y in range(ny):
                if needed_first(kind, c, y, ny) == first:
                    wanted.append((slots[f, y], store_to(ref, c, y, row + shift)))
        return wanted

    def unpack(i, carry):
        for part in range(UNROLL):
            row = pl.multiple_of((i * UNROLL + part) * 8, 8)
            halo.take(row, fields(row))
        return carry

    lax.fori_loop(0, nx // (8 * UNROLL), unpack, 0)
    halo.take(nx, fields(cross_row(nx)))


def rest_kernel(flags, thirds, r_a, r_b, v_in, s_in, m_in, v, s, m):
    nx = r_a.shape[1] - 16
    planes = z_slots(m.shape[2], m.shape[4])[1]
    halo = ZHalo(flags[2] == 1, thirds[...], r_a, r_b, planes)
    unpack_fields(halo, v, s, m, nx, False)


def widen_kernel(
    flags, thirds, eighths, r_a, r_b, v_in, s_in, m_in, f_in, v, s, m, fault, y_a, y_b, strips
):
    ny, width = m.shape[2], m.shape[4]
    nx = r_a.shape[1] - 16
    planes = z_slots(ny, width)[1]
    odd_y = flags[1] == 1
    lanes = lane_index((8, width))
    halo = ZHalo(flags[2] == 1, thirds[...], r_a, r_b, planes)
    unpack_fields(halo, v, s, m, nx, True)

    def store_fault(k):
        def store(value):
            fault[k, 1, 0:8, :] = value

        return store

    halo.take(nx + 8, [((0, k), store_fault(k)) for k in range(6)])
    partial_trials(v, s, m, nx, lanes)
    last = ny - 1
    halos = eighths[...]
    for row in row_tiles(nx):
        buoyancy = m[B, 1, 0, pl.ds(row, 8), :]
        up = [at(s, c, 1, last, row) for c in ALONG_Y] + [buoyancy]
        down = [
            jnp.where(lanes == HALO, roll(at(v, c, 0, 0, row), HALO), at(v, c, 1, 0, row))
            for c in range(3)
        ] + [buoyancy]
        tile = strip_tile(up, down, halos)
        if row < nx:
            strips[row : row + 8, :] = tile
    strip_send(strips, tile, SLOTS, odd_y, y_a, y_b, 0)
    for t in range(2):
        for k in range(8):
            line = fault[min(k, 5), t, 0:1, :]
            row = STRIP * SLOTS + 8 + 8 * t + k
            y_a[row : row + 1, :] = line
            y_b[row : row + 1, :] = line


def inner_kernel(first, final, m, v_in, s_in, v, s, *outs):
    ny, width = m.shape[2], m.shape[4]
    nx = m.shape[3] - 16
    lanes = lane_index((8, width))

    if not first:

        def ends(y, carry):
            for row in (0, nx - 8, cross_row(nx)):
                stress_tile(v, s, m, y, row, lanes)
            return carry

        lax.fori_loop(1, ny - 1, ends, 0)

    def trials(y, carry):
        for row in row_tiles(nx):
            new = trial_tile(
                v, s, m, y, row, lambda c, t, row=row: at(s, c, t, y - 1, row), lanes
            )
            for t in range(2):
                for c in range(3):
                    v[c, t, y, pl.ds(PAD + row, 8), :] = new[t][c]
        return carry

    lax.fori_loop(1, ny, trials, 0)
    copies = []
    if final:
        new_v, new_s, sems = outs
        for c in range(3):
            part = v.at[c, 0, pl.ds(1, ny - 1), pl.ds(PAD + 8, nx - 16), :]
            to = new_v.at[c, pl.ds(1, ny - 1), pl.ds(8, nx - 16), :]
            copies.append(pltpu.make_async_copy(part, to, sems.at[c]))
            copies[-1].start()

    def out_copy(c, y):
        part = s.at[c, 0, y, pl.ds(PAD + 8, nx - 16), :]
        to = new_s.at[c, y, pl.ds(8, nx - 16), :]
        return pltpu.make_async_copy(part, to, sems.at[3 + c * ny + y])

    def stresses(y, carry):
        for row in range(8, nx - 8, 8):
            stress_tile(v, s, m, y, row, lanes, (0,) if final else (0, 1))
        if final:
            for c in range(6):
                out_copy(c, y).start()
        return carry

    lax.fori_loop(1, ny - 1, stresses, 0)
    if final:
        for copy in copies:
            copy.wait()

        def wait(y, carry):
            for c in range(6):
                out_copy(c, y).wait()
            return carry

        lax.fori_loop(1, ny - 1, wait, 0)


def boundary_kernel(first, final, flags, eighths, *refs):
    refs = list(refs)

    def pop(n):
        out = refs[:n]
        del refs[:n]
        return out

    early_a, early_b = pop(2) if first else (None, None)
    r_a, r_b, m = pop(3)
    if not first:
        (ahead_b,) = pop(1)
    pop(3)
    if final:
        pop(2)
    v, s, fault = pop(3)
    if first:
        (ahead_b,) = pop(1)
    if final:
        new_v, new_s, slip_out, rows, turned, strips, sems = refs
    else:
        y_a, y_b, rows, turned, strips = refs
    ny, width = m.shape[2], m.shape[4]
    nx = m.shape[3] - 16
    cross = cross_row(nx)
    span = nx + 8
    odd = flags[1] == 1
    lanes = lane_index((8, width))
    halos = eighths[...]

    count = SLOTS if first else 3
    main_a, main_b = (early_a, early_b) if first else (r_a, r_b)
    cross_tile = strip_receive(
        r_a, r_b, 0 if first else 3 * span, count, odd, turned, strips, lanes
    )

    def received(row):
        at_row = packed_row(row, nx)
        from_a = [main_a[pl.ds(k * span + at_row, 8), :] for k in range(count)]
        from_b = [main_b[pl.ds(k * span + at_row, 8), :] for k in range(count)]
        low = [jnp.where(odd, a, b) for a, b in zip(from_a, from_b)]
        high = [jnp.where(odd, b, a) for a, b in zip(from_a, from_b)]
        packed = strips[row : row + 8, :] if row < nx else cross_tile
        if first:
            for c in range(3):
                column = roll(packed, -(STRIP * (SLOTS + c) + 2 * HALO))
                high[c] = jnp.where(lanes == 0, column, high[c])
        return low, high, packed

    if first:
        for t in range(2):
            to = pl.ds(STRIP * SLOTS + 8 + 8 * t, 8)
            lines = jnp.where(odd, r_b[to, :], r_a[to, :])
            for k in range(6):
                fault[k, t, ny : ny + 1, :] = lines[k : k + 1, :]
    for row in row_tiles(nx):
        low, high, packed = received(row)
        if first:
            ahead_b[0, pl.ds(row, 8), :] = high[3]
            ahead_b[1, pl.ds(row, 8), :] = strip_take(packed, SLOTS + 3)
        for t in range(2):
            scale = DT * m[B, t, 0, pl.ds(row, 8), :]
            scale_ahead = DT * ahead_b[t, pl.ds(row, 8), :]
            for c in range(3):
                low_c = low[c] if t == 0 else strip_take(packed, c)
                high_c = high[c] if t == 0 else strip_take(packed, SLOTS + c)
                v[c, t, 0, pl.ds(PAD + row, 8), :] = at(v, c, t, 0, row) - scale * low_c
                v[c, t, ny, pl.ds(PAD + row, 8), :] = high_c - scale_ahead * at(
                    s, ALONG_Y[c], t, ny - 1, row
                )

    places = ((0, (nx - 1, cross)), (1, (0, cross + 7)))
    for side, pair in places:

        @pl.when(flags[0] == side)
        def _(pair=pair):
            for which, row in enumerate(pair):
                for t in range(2):
                    for y in range(ny + 1):
                        for c in range(3):
                            rows[which, c, t, y : y + 1, :] = v[
                                c, t, y, PAD + row : PAD + row + 1, :
                            ]
                        if first:
                            if y < ny:
                                line = m[B, t, y, row : row + 1, :]
                            else:
                                line = ahead_b[t, row : row + 1, :]
                            fault[OWN_B + which, t, y : y + 1, :] = line

    minus = flags[0] == 0
    sign = jnp.where(minus, DT, -DT)
    for t in range(2):
        for half in range(0, fault.shape[2], 8):
            part = slice(half, half + 8)
            own = [rows[0, c, t, part, :] for c in range(3)]
            other = [rows[1, c, t, part, :] for c in range(3)]
            par = [fault[k, t, part, :] for k in range(8)]
            m_side = [jnp.where(minus, a, b) for a, b in zip(own, other)]
            p_side = [jnp.where(minus, b, a) for a, b in zip(own, other)]
            m_b = jnp.where(minus, par[OWN_B], par[OTHER_B])
            p_b = jnp.where(minus, par[OTHER_B], par[OWN_B])
            traction, slip = friction(m_side, p_side, m_b, p_b, par)
            fault[SLIP, t, part, :] = slip
            for c in range(3):
                rows[0, c, t, part, :] = own[c] + sign * par[OWN_B] * traction[c]
                rows[1, c, t, part, :] = other[c] - sign * par[OTHER_B] * traction[c]
    for y in (0, ny - 1):
        for row in range(8, nx - 8, 8):
            stress_tile(v, s, m, y, row, lanes, (0,) if final else (0, 1))
    for side, pair in places:

        @pl.when(flags[0] == side)
        def _(pair=pair):
            for which, row in enumerate(pair):
                for c in range(3):
                    for t in range(2):
                        for y in range(ny + 1):
                            v[c, t, y, PAD + row : PAD + row + 1, :] = rows[
                                which, c, t, y : y + 1, :
                            ]

    if final:
        copies = []

        def send(pairs):
            for part, to in pairs:
                copies.append(pltpu.make_async_copy(part, to, sems.at[len(copies)]))
                copies[-1].start()

        def plane(ref, out, c, y):
            return ref.at[c, 0, y, pl.ds(PAD, nx), :], out.at[c, y]

        def edge(ref, out, c, inside, row):
            part = ref.at[c, 0, pl.ds(1, inside), pl.ds(PAD + row, 8), :]
            return part, out.at[c, pl.ds(1, inside), pl.ds(row, 8), :]

        send([plane(v, new_v, c, 0) for c in range(3)])
        send([edge(v, new_v, c, ny - 1, row) for c in range(3) for row in (0, nx - 8)])
    tiles = (0,) if final else (0, 1)
    for y in (0, ny - 1):
        for row in (0, nx - 8) if final else (0, nx - 8, cross):
            stress_tile(v, s, m, y, row, lanes, tiles)
    if not final:
        partial_trials(v, s, m, nx, lanes)
        write_messages(v, s, halos, odd, y_a, y_b, strips, nx)
        return

    send([plane(s, new_s, c, y) for c in range(6) for y in (0, ny - 1)])

    def ends(y, carry):
        for row in (0, nx - 8):
            stress_tile(v, s, m, y, row, lanes, tiles)
        return carry

    lax.fori_loop(1, ny - 1, ends, 0)
    send([edge(s, new_s, c, ny - 2, row) for c in range(6) for row in (0, nx - 8)])
    slip_out[...] = fault[SLIP, 0, 0:ny, :]
    for copy in copies:
        copy.wait()


def inverse_sinh(values):
    size = jnp.abs(values)
    sign = jnp.where(values > 0.0, 1.0, jnp.where(values < 0.0, -1.0, 0.0))
    return sign * jnp.log(size + jnp.sqrt(size * size + 1.0))


def friction(minus_side, plus_side, minus_b, plus_b, par):
    total = DT * (minus_b + plus_b)
    impedance = 1.0 / jnp.where(total > 0.0, total, 1.0)
    jump = [p - q for p, q in zip(plus_side, minus_side)]
    locked_y = par[PRE_Y] + impedance * jump[1]
    locked_z = par[PRE_Z] + impedance * jump[2]
    magnitude = jnp.sqrt(locked_y * locked_y + locked_z * locked_z + 1.0)
    rate, strength, slip = par[RATE], par[STRENGTH], par[SLIP]
    for _ in range(NEWTON):
        scaled = rate * slip
        residual = magnitude - impedance * slip - strength * inverse_sinh(scaled)
        tangent = -impedance - strength * rate / jnp.sqrt(1.0 + scaled * scaled)
        slip = slip - residual / tangent
    slip = slip * par[MASK]
    retained = 1.0 - impedance * slip / magnitude
    traction = (
        impedance * jump[0],
        retained * locked_y - par[PRE_Y],
        retained * locked_z - par[PRE_Z],
    )
    return traction, slip


def f32(*shape):
    return VMEM(shape, jnp.float32)


def call(kernel, name, outs, in_specs, aliases, scratch=(), flops=0, out_specs=None):
    return pl.pallas_call(
        kernel,
        out_shape=tuple(outs),
        in_specs=in_specs,
        out_specs=tuple(out_specs or [in_vmem() for _ in outs]),
        input_output_aliases=aliases,
        scratch_shapes=list(scratch),
        compiler_params=pltpu.CompilerParams(vmem_limit_bytes=8 << 20),
        cost_estimate=pl.CostEstimate(flops=flops, bytes_accessed=0, transcendentals=0),
        name=name,
    )


def pair_swaps(a, b, axis):
    size = lax.axis_size(axis)
    out = []
    for value, start in ((a, 0), (b, 1)):
        pairs = []
        for i in range(start, size - 1, 2):
            pairs += [(i, i + 1), (i + 1, i)]
        out.append(lax.ppermute(value, axis, pairs))
    return out


def local(
    velocity,
    stress,
    buoyancy,
    stiff_xx,
    stiff_xz,
    stiff_zz,
    shear_vert,
    shear_horiz,
    prestress,
    fault_mask,
    region_ids,
    inverse_rate,
    slip_prev,
    region_a,
    region_normal,
):
    ny, nx, width = buoyancy.shape
    assert nx == width
    across, along, dip = (lax.axis_index(k) for k in ("gx", "gy", "gz"))
    flags = jnp.stack([across, along % 2, dip % 2]).astype(jnp.int32)
    lanes = jnp.broadcast_to(jnp.arange(width, dtype=jnp.int32), (8, width))
    thirds, eighths = lanes // HALO, lanes // STRIP
    rows = cross_row(nx) + 8
    high = 8 * ((ny + 1 + 7) // 8)
    v_shape = f32(3, 2, ny + 1, rows + 2 * PAD, width)
    s_shape = f32(6, 2, ny, rows + 2 * PAD, width)
    m_shape = f32(6, 2, ny, rows, width)
    fault_shape = f32(8, 2, high, width)
    planes = z_slots(ny, width)[1]
    z_shape = f32(planes, nx + 16, width)
    unit = ny * nx * width
    vm, hb, sm = in_vmem(), in_hbm(), in_smem()
    raw = [velocity, stress, buoyancy, stiff_xx, stiff_xz, stiff_zz, shear_vert, shear_horiz]
    raw += [prestress, region_ids, fault_mask, inverse_rate, slip_prev, region_a, region_normal]
    raw = [pltpu.with_memory_space_constraint(k, HBM) for k in raw]

    f_shape = f32(len(FIELDS), ny // 2, 8, width)
    (f_own,) = call(
        edge_kernel,
        "edge",
        (f_shape,),
        [sm] + [hb] * 8,
        {},
        [pltpu.SemaphoreType.DMA((2 * len(FIELDS),))],
        flops=unit,
    )(flags, *raw[:8])
    f_other = lax.ppermute(f_own, "gx", [(i, i ^ 1) for i in range(lax.axis_size("gx"))])
    v, s, m, fault, z_a, z_b = call(
        load_kernel,
        "load",
        (v_shape, s_shape, m_shape, fault_shape, z_shape, z_shape),
        [sm, vm] + [hb] * 15,
        {},
        [
            pltpu.VMEM(prestress.shape, jnp.float32),
            pltpu.VMEM(region_ids.shape, jnp.int32),
            pltpu.VMEM(fault_mask.shape, jnp.int32),
            pltpu.VMEM(inverse_rate.shape, jnp.float32),
            pltpu.VMEM(slip_prev.shape, jnp.float32),
            pltpu.SMEM(region_a.shape, jnp.float32),
            pltpu.SMEM(region_normal.shape, jnp.float32),
            pltpu.SemaphoreType.DMA((22,)),
        ],
        flops=100 * unit,
    )(flags, thirds, *raw)
    v, s, m, z_a, z_b = call(
        cross_kernel,
        "cross",
        (v_shape, s_shape, m_shape, z_shape, z_shape),
        [sm] + [vm] * 8,
        {4: 0, 5: 1, 6: 2, 7: 3, 8: 4},
        flops=10 * unit,
    )(flags, thirds, f_other, fault, v, s, m, z_a, z_b)
    z_a, z_b = pair_swaps(z_a, z_b, "gz")
    y_shape = f32(4 * (nx + 8), width)
    early_a, early_b = call(
        early_kernel, "early", (y_shape, y_shape), [sm] + [vm] * 3, {}, flops=10 * unit
    )(flags, v, s, m)
    early_a, early_b = pair_swaps(early_a, early_b, "gy")
    y_shape = f32(STRIP * SLOTS + 8 + 16, width)
    v, s, m, fault, y_a, y_b = call(
        widen_kernel,
        "widen",
        (v_shape, s_shape, m_shape, fault_shape, y_shape, y_shape),
        [sm] + [vm] * 8,
        {5: 0, 6: 1, 7: 2, 8: 3},
        [pltpu.VMEM((nx, width), jnp.float32)],
        flops=50 * unit,
    )(flags, thirds, eighths, z_a, z_b, v, s, m, fault)
    v, s, m = call(
        rest_kernel,
        "rest",
        (v_shape, s_shape, m_shape),
        [sm] + [vm] * 6,
        {4: 0, 5: 1, 6: 2},
        flops=50 * unit,
    )(flags, thirds, z_a, z_b, v, s, m)
    y_shape = f32(3 * (nx + 8) + STRIP * 3 + 8, width)
    ahead_b = None
    out_shapes = (HBM((3, ny, nx, width), jnp.float32), HBM((6, ny, nx, width), jnp.float32))
    for step in range(STEPS):
        first, final = step == 0, step == STEPS - 1
        y_a, y_b = pair_swaps(y_a, y_b, "gy")
        v, s, *outs = call(
            functools.partial(inner_kernel, first, final),
            "inner",
            (v_shape, s_shape) + (out_shapes if final else ()),
            [vm] * 3,
            {1: 0, 2: 1},
            [pltpu.SemaphoreType.DMA((3 + 6 * ny,))] if final else [],
            flops=200 * unit,
            out_specs=[vm, vm] + ([hb, hb] if final else []),
        )(m, v, s)
        args = [flags, eighths] + ([early_a, early_b] if first else []) + [y_a, y_b, m]
        args += ([] if first else [ahead_b]) + [v, s, fault] + outs
        at_state = len(args) - len(outs) - 3
        aliases = {at_state + k: k for k in range(3)}
        shapes, specs = [v_shape, s_shape, fault_shape], [vm, vm, vm]
        scratch = [pltpu.VMEM((2, 3, 2, high, width), jnp.float32)]
        scratch += [pltpu.VMEM((width, nx), jnp.float32), pltpu.VMEM((nx, width), jnp.float32)]
        if first:
            shapes.append(f32(2, rows, width))
            specs.append(vm)
        if final:
            shapes += [*out_shapes, jax.ShapeDtypeStruct((ny, width), jnp.float32)]
            specs += [hb, hb, vm]
            scratch.append(pltpu.SemaphoreType.DMA((3 * 3 + 6 * 4,)))
            aliases.update({at_state + 3: 3, at_state + 4: 4})
        else:
            shapes += [y_shape, y_shape]
            specs += [vm, vm]
        v, s, fault, *more = call(
            functools.partial(boundary_kernel, first, final),
            "boundary",
            shapes,
            [sm] + [vm] * (len(args) - 1 - len(outs)) + [hb] * len(outs),
            aliases,
            scratch,
            flops=50 * unit,
            out_specs=specs,
        )(*args)
        if final:
            return tuple(more)
        if first:
            ahead_b, *more = more
        y_a, y_b = more


def solution(mesh):
    in_specs = (
        P(None, "gy", "gx", "gz"),
        P(None, "gy", "gx", "gz"),
        P("gy", "gx", "gz"),
        P("gy", "gx", "gz"),
        P("gy", "gx", "gz"),
        P("gy", "gx", "gz"),
        P("gy", "gx", "gz"),
        P("gy", "gx", "gz"),
        P(None, "gy", "gz"),
        P("gy", "gz"),
        P("gy", "gz"),
        P("gy", "gz"),
        P("gy", "gz"),
        P(),
        P(),
    )
    out_specs = (P(None, "gy", "gx", "gz"), P(None, "gy", "gx", "gz"), P("gy", "gz"))
    return jax.shard_map(local, mesh=mesh, in_specs=in_specs, out_specs=out_specs, check_vma=False)
```

```python
import functools

import jax
import jax.numpy as jnp
from jax import lax
from jax.experimental import pallas as pl
from jax.experimental.pallas import tpu as pltpu
from jax.sharding import PartitionSpec as P

STEPS = 3
NEWTON = 3
DT = 0.2

PAD = 8
HALO = 3
CROSS = 4
STRIP = 8

XX, YY, ZZ, YZ, XZ, XY = range(6)
ALONG_Y = (XY, YY, YZ)
B, C11, C13, C33, C44, C66 = range(6)
FIELDS = [("v", c) for c in range(3)] + [("s", c) for c in range(6)] + [("m", c) for c in range(6)]
PRE_Y, PRE_Z, MASK, STRENGTH, RATE, SLIP, OWN_B, OTHER_B = range(8)

VMEM = pltpu.MemorySpace.VMEM
HBM = pltpu.MemorySpace.HBM
SMEM = pltpu.MemorySpace.SMEM


def in_vmem():
    return pl.BlockSpec(memory_space=VMEM)


def in_hbm():
    return pl.BlockSpec(memory_space=HBM)


def in_smem():
    return pl.BlockSpec(memory_space=SMEM)


def roll(values, by):
    by = by % values.shape[-1]
    return values if by == 0 else pltpu.roll(values, by, values.ndim - 1)


def at(ref, field, tile, y, row):
    return ref[field, tile, y, pl.ds(PAD + row, 8), :]


def z_below(pair, lanes):
    one, two = roll(pair[0], 1), roll(pair[1], 1)
    first = lanes == 0
    return jnp.where(first, two, one), jnp.where(first, one, two)


def z_above(pair, lanes):
    one, two = roll(pair[0], -1), roll(pair[1], -1)
    last = lanes == pair[0].shape[-1] - 1
    return jnp.where(last, two, one), jnp.where(last, one, two)


def trial_tile(v, s, m, y, row, below, lanes):
    both = (0, 1)
    behind = {c: z_below([at(s, c, t, y, row) for t in both], lanes) for c in (XZ, YZ, ZZ)}
    out = []
    for t in both:
        own = {c: at(s, c, t, y, row) for c in range(6)}
        lower_x = {c: own[c] - at(s, c, t, y, row - 1) for c in (XX, XY, XZ)}
        if below is None:
            lower_y = {c: own[c] for c in ALONG_Y}
        else:
            lower_y = {c: own[c] - below(c, t) for c in ALONG_Y}
        scale = DT * m[B, t, y, pl.ds(row, 8), :]
        total = (
            lower_x[XX] + lower_y[XY] + (own[XZ] - behind[XZ][t]),
            lower_x[XY] + lower_y[YY] + (own[YZ] - behind[YZ][t]),
            lower_x[XZ] + lower_y[YZ] + (own[ZZ] - behind[ZZ][t]),
        )
        out.append([at(v, c, t, y, row) + scale * total[c] for c in range(3)])
    return out


def stress_tile(v, s, m, y, row, lanes, tiles=(0, 1)):
    both = (0, 1)
    own = [[at(v, c, t, y, row) for t in both] for c in range(3)]
    ahead = [z_above(own[c], lanes) for c in range(3)]
    for t in tiles:
        vx, vy, vz = own[0][t], own[1][t], own[2][t]
        over_x = [at(v, c, t, y, row + 1) for c in range(3)]
        over_y = [at(v, c, t, y + 1, row) for c in range(3)]
        exx, eyy, ezz = over_x[0] - vx, over_y[1] - vy, ahead[2][t] - vz
        c11, c13, c33, c44, c66 = (m[k, t, y, pl.ds(row, 8), :] for k in (C11, C13, C33, C44, C66))
        c12 = c11 - 2.0 * c66
        third = c13 * ezz
        change = {
            XX: c11 * exx + c12 * eyy + third,
            YY: c12 * exx + c11 * eyy + third,
            ZZ: c13 * (exx + eyy) + c33 * ezz,
            YZ: c44 * ((ahead[1][t] - vy) + (over_y[2] - vz)),
            XZ: c44 * ((ahead[0][t] - vx) + (over_x[2] - vz)),
            XY: c66 * ((over_y[0] - vx) + (over_x[1] - vy)),
        }
        for c, gain in change.items():
            s[c, t, y, pl.ds(PAD + row, 8), :] = at(s, c, t, y, row) + DT * gain


def lane_index(like):
    return lax.broadcasted_iota(jnp.int32, like, len(like) - 1)


SLOTS = 4


def strip_tile(up, down, eighths):
    packed = jnp.zeros_like(up[0])
    for start, pieces in ((0, up), (SLOTS, down)):
        for k, piece in enumerate(pieces):
            moved = roll(piece, STRIP * (start + k) + HALO)
            packed = jnp.where(eighths == start + k, moved, packed)
    return packed


def strip_take(packed, slot):
    return roll(packed, -(STRIP * slot + HALO))


def strip_send(strips, cross_tile, count, odd, y_a, y_b, base):
    turned = strips[...].T
    for j in range(0, STRIP * count, 8):
        up = turned[j : j + 8, :]
        down = turned[STRIP * SLOTS + j : STRIP * SLOTS + j + 8, :]
        y_a[base + j : base + j + 8, :] = jnp.where(odd, down, up)
        y_b[base + j : base + j + 8, :] = jnp.where(odd, up, down)
    other = roll(cross_tile, -STRIP * SLOTS)
    last = base + STRIP * count
    y_a[last : last + 8, :] = jnp.where(odd, other, cross_tile)
    y_b[last : last + 8, :] = jnp.where(odd, cross_tile, other)


def strip_receive(r_a, r_b, base, count, odd, turned, strips, lanes):
    turned[...] = jnp.zeros_like(turned)
    for j in range(0, STRIP * count, 8):
        from_a, from_b = r_a[base + j : base + j + 8, :], r_b[base + j : base + j + 8, :]
        turned[j : j + 8, :] = jnp.where(odd, from_a, from_b)
        start = STRIP * SLOTS + j
        turned[start : start + 8, :] = jnp.where(odd, from_b, from_a)
    strips[...] = turned[...].T
    last = base + STRIP * count
    from_a, from_b = r_a[last : last + 8, :], r_b[last : last + 8, :]
    low, high = jnp.where(odd, from_a, from_b), jnp.where(odd, from_b, from_a)
    return jnp.where(lanes < STRIP * SLOTS, low, roll(high, STRIP * SLOTS))


def field_ref(kind, v, s, m):
    return {"v": v, "s": s, "m": m}[kind]


def fields_per_plane(ny, width):
    return (width - 5) // HALO // ny


def z_slots(ny, width):
    per_plane = fields_per_plane(ny, width)
    slots = {}
    for f in range(len(FIELDS)):
        for y in range(ny):
            slots[f, y] = (f // per_plane, f % per_plane * ny + y)
    return slots, -(-len(FIELDS) // per_plane)


def row_tiles(nx):
    return [*range(0, nx, 8), cross_row(nx)]


def cross_row(nx):
    return nx + PAD


def packed_row(row, nx):
    return row if row < nx else nx


def edge_kernel(flags, velocity, stress, *rest):
    raw_m, out, sem = rest[:6], rest[6], rest[7]
    ny, nx = velocity.shape[1:3]
    sources = [velocity.at[c] for c in range(3)] + [stress.at[c] for c in range(6)] + list(raw_m)
    for side, row in ((0, nx - CROSS), (1, 0)):

        @pl.when(flags[0] == side)
        def _(row=row):
            copies = []
            for f, source in enumerate(sources):
                for half in range(2):
                    part = source.at[pl.ds(half * (ny // 2), ny // 2), pl.ds(row, CROSS), :]
                    to = out.at[f, :, pl.ds(half * CROSS, CROSS), :]
                    copies.append(pltpu.make_async_copy(part, to, sem.at[2 * f + half]))
            for copy in copies:
                copy.start()
            for copy in copies:
                copy.wait()


def load_kernel(flags, thirds, velocity, stress, *rest):
    raw_m, small = rest[:6], rest[6:13]
    v, s, m, fault, z_a, z_b = rest[13:19]
    pre, ids, mask, rate, slip, region_a, region_normal, sems = rest[19:]
    ny, nx, width = velocity.shape[1:]
    cross = cross_row(nx)
    big = {}
    for c in range(3):
        big["v", c] = (velocity.at[c], v.at[c, 0, pl.ds(0, ny), pl.ds(PAD, nx), :])
    for c in range(6):
        big["s", c] = (stress.at[c], s.at[c, 0, :, pl.ds(PAD, nx), :])
    for c in range(6):
        big["m", c] = (raw_m[c], m.at[c, 0, :, pl.ds(0, nx), :])
    big = {
        key: pltpu.make_async_copy(a, b, sems.at[k]) for k, (key, (a, b)) in enumerate(big.items())
    }
    held = (pre, ids, mask, rate, slip, region_a, region_normal)
    little = [
        pltpu.make_async_copy(a, b, sems.at[len(big) + k])
        for k, (a, b) in enumerate(zip(small, held))
    ]
    for copy in big.values():
        copy.start()
    for copy in little:
        copy.start()
    zeros = jnp.zeros((PAD, width), jnp.float32)
    for t in range(2):
        for y in range(ny):
            for c in (XX, XY, XZ):
                s[c, t, y, 0:PAD, :] = zeros
                s[c, t, y, cross : cross + PAD, :] = zeros
            for c in range(3):
                v[c, t, y, PAD + nx : PAD + nx + PAD, :] = zeros
                v[c, t, y, PAD + cross + 8 : 2 * PAD + cross + 8, :] = zeros

    per_plane = fields_per_plane(ny, width)
    odd = flags[2] == 1
    group = thirds[...]
    for plane in range(z_slots(ny, width)[1]):
        for key in FIELDS[plane * per_plane : (plane + 1) * per_plane]:
            big[key].wait()

        def pack(i, carry, plane=plane):
            for part in range(UNROLL):
                row = pl.multiple_of((i * UNROLL + part) * 8, 8)
                z_emit(z_a, z_b, odd, group, z_pieces(plane, v, s, m, row), plane, row)
            return carry

        lax.fori_loop(0, nx // (8 * UNROLL), pack, 0)
    for copy in little:
        copy.wait()
    kinds = ids[...]
    a_part = jnp.zeros((ny, width), jnp.float32)
    n_part = jnp.zeros((ny, width), jnp.float32)
    for k in range(region_a.shape[0]):
        a_part = jnp.where(kinds == k, region_a[k], a_part)
        n_part = jnp.where(kinds == k, region_normal[k], n_part)
    fault[PRE_Y, 0, 0:ny, :] = pre[0]
    fault[PRE_Z, 0, 0:ny, :] = pre[1]
    fault[MASK, 0, 0:ny, :] = mask[...].astype(jnp.float32)
    fault[STRENGTH, 0, 0:ny, :] = a_part * n_part
    fault[RATE, 0, 0:ny, :] = rate[...]
    fault[SLIP, 0, 0:ny, :] = slip[...]


UNROLL = 4


def z_emit(z_a, z_b, odd, group, pieces, plane, row):
    up = jnp.zeros_like(pieces[0][1])
    down = up
    for pos, piece in pieces:
        moved = roll(piece, HALO * pos + HALO)
        up = jnp.where(group == pos, moved, up)
        down = jnp.where(group == pos + 1, moved, down)
    z_a[plane, pl.ds(row, 8), :] = jnp.where(odd, down, up)
    z_b[plane, pl.ds(row, 8), :] = jnp.where(odd, up, down)


def z_pieces(plane, v, s, m, row):
    ny, width = m.shape[2], m.shape[4]
    per_plane = fields_per_plane(ny, width)
    pieces = []
    for f, (kind, c) in enumerate(FIELDS[plane * per_plane : (plane + 1) * per_plane]):
        shift = 0 if kind == "m" else PAD
        ref = field_ref(kind, v, s, m)
        for y in range(ny):
            pieces.append((f * ny + y, ref[c, 0, y, pl.ds(row + shift, 8), :]))
    return pieces


def cross_kernel(flags, thirds, f_other, fault, v_in, s_in, m_in, za_in, zb_in, v, s, m, z_a, z_b):
    ny, width = m.shape[2], m.shape[4]
    nx = z_a.shape[1] - 16
    cross = cross_row(nx)
    odd = flags[2] == 1
    group = thirds[...]
    planes = z_slots(ny, width)[1]
    rows = lax.broadcasted_iota(jnp.int32, (8, width), 0)
    minus = flags[0] == 0
    keep = jnp.where(minus, 7 - rows, rows) >= 8 - CROSS
    for f, (kind, c) in enumerate(FIELDS):
        shift = 0 if kind == "m" else PAD
        ref = field_ref(kind, v, s, m)
        for y in range(ny // 2):
            tile = f_other[f, y]
            turned = pltpu.roll(tile, CROSS, 0)
            ref[c, 0, y, cross + shift : cross + shift + 8, :] = jnp.where(
                keep, jnp.where(minus, tile, turned), 0.0
            )
            ref[c, 0, y + ny // 2, cross + shift : cross + shift + 8, :] = jnp.where(
                keep, jnp.where(minus, turned, tile), 0.0
            )
    for plane in range(planes):
        z_emit(z_a, z_b, odd, group, z_pieces(plane, v, s, m, cross), plane, nx)
    z_emit(z_a, z_b, odd, group, [(k, fault[k, 0, 0:8, :]) for k in range(6)], 0, nx + 8)
    zeros = jnp.zeros((8, width), jnp.float32)
    for plane in range(1, planes):
        z_a[plane, pl.ds(nx + 8, 8), :] = zeros
        z_b[plane, pl.ds(nx + 8, 8), :] = zeros


def write_messages(v, s, buoyancy, eighths, odd, y_a, y_b, strips, nx):
    last = s.shape[2] - 1
    span = nx + 8
    count = 3 if buoyancy is None else SLOTS

    def pieces(t, row):
        up = [at(s, c, t, last, row) for c in ALONG_Y]
        down = [at(v, c, t, 0, row) for c in range(3)]
        if buoyancy is not None:
            up.append(buoyancy[B, t, 0, pl.ds(row, 8), :])
            down.append(up[-1])
        return up, down

    for row in row_tiles(nx):
        up, down = pieces(0, row)
        for k in range(count):
            to = pl.ds(k * span + packed_row(row, nx), 8)
            y_a[to, :] = jnp.where(odd, down[k], up[k])
            y_b[to, :] = jnp.where(odd, up[k], down[k])
        tile = strip_tile(*pieces(1, row), eighths)
        if row < nx:
            strips[row : row + 8, :] = tile
    strip_send(strips, tile, count, odd, y_a, y_b, count * span)


def partial_trials(v, s, m, nx, lanes):
    for row in row_tiles(nx):
        new = trial_tile(v, s, m, 0, row, None, lanes)
        for t in range(2):
            for c in range(3):
                v[c, t, 0, pl.ds(PAD + row, 8), :] = new[t][c]


class ZHalo:
    def __init__(self, odd, group, r_a, r_b, planes):
        self.odd, self.group, self.r_a, self.r_b, self.planes = odd, group, r_a, r_b, planes

    def take(self, row, wanted):
        for plane in range(self.planes):
            chosen = [(pos, store) for (p, pos), store in wanted if p == plane]
            if chosen:
                from_a = self.r_a[plane, pl.ds(row, 8), :]
                from_b = self.r_b[plane, pl.ds(row, 8), :]
                low = jnp.where(self.odd, from_a, from_b)
                high = jnp.where(self.odd, from_b, from_a)
                for pos, store in chosen:
                    both = jnp.where(self.group == pos, low, high)
                    store(roll(both, -(HALO * pos + HALO)))


def needed_first(kind, c, y, ny):
    if y == 0:
        return kind != "m" or c == B
    return y == ny - 1 and kind == "s" and c in ALONG_Y


def unpack_fields(halo, v, s, m, nx, first):
    ny, width = m.shape[2], m.shape[4]
    slots = z_slots(ny, width)[0]

    def store_to(ref, c, y, row):
        def store(value):
            ref[c, 1, y, pl.ds(row, 8), :] = value

        return store

    def fields(row):
        wanted = []
        for f, (kind, c) in enumerate(FIELDS):
            shift = 0 if kind == "m" else PAD
            ref = field_ref(kind, v, s, m)
            for y in range(ny):
                if needed_first(kind, c, y, ny) == first:
                    wanted.append((slots[f, y], store_to(ref, c, y, row + shift)))
        return wanted

    def unpack(i, carry):
        for part in range(UNROLL):
            row = pl.multiple_of((i * UNROLL + part) * 8, 8)
            halo.take(row, fields(row))
        return carry

    lax.fori_loop(0, nx // (8 * UNROLL), unpack, 0)
    halo.take(nx, fields(cross_row(nx)))


def rest_kernel(flags, thirds, r_a, r_b, v_in, s_in, m_in, v, s, m):
    nx = r_a.shape[1] - 16
    planes = z_slots(m.shape[2], m.shape[4])[1]
    halo = ZHalo(flags[2] == 1, thirds[...], r_a, r_b, planes)
    unpack_fields(halo, v, s, m, nx, False)


def widen_kernel(
    flags, thirds, eighths, r_a, r_b, v_in, s_in, m_in, f_in, v, s, m, fault, y_a, y_b, strips
):
    ny, width = m.shape[2], m.shape[4]
    nx = r_a.shape[1] - 16
    planes = z_slots(ny, width)[1]
    odd_y = flags[1] == 1
    lanes = lane_index((8, width))
    halo = ZHalo(flags[2] == 1, thirds[...], r_a, r_b, planes)
    unpack_fields(halo, v, s, m, nx, True)

    def store_fault(k):
        def store(value):
            fault[k, 1, 0:8, :] = value

        return store

    halo.take(nx + 8, [((0, k), store_fault(k)) for k in range(6)])
    partial_trials(v, s, m, nx, lanes)
    write_messages(v, s, m, eighths[...], odd_y, y_a, y_b, strips, nx)
    for t in range(2):
        for k in range(8):
            line = fault[min(k, 5), t, 0:1, :]
            row = SLOTS * (nx + 8 + STRIP) + 8 + 8 * t + k
            y_a[row : row + 1, :] = line
            y_b[row : row + 1, :] = line


def inner_kernel(first, final, m, v_in, s_in, v, s, *outs):
    ny, width = m.shape[2], m.shape[4]
    nx = m.shape[3] - 16
    lanes = lane_index((8, width))

    if not first:

        def ends(y, carry):
            for row in (0, nx - 8, cross_row(nx)):
                stress_tile(v, s, m, y, row, lanes)
            return carry

        lax.fori_loop(1, ny - 1, ends, 0)

    def trials(y, carry):
        for row in row_tiles(nx):
            new = trial_tile(
                v, s, m, y, row, lambda c, t, row=row: at(s, c, t, y - 1, row), lanes
            )
            for t in range(2):
                for c in range(3):
                    v[c, t, y, pl.ds(PAD + row, 8), :] = new[t][c]
        return carry

    lax.fori_loop(1, ny, trials, 0)
    copies = []
    if final:
        new_v, new_s, sems = outs
        for c in range(3):
            part = v.at[c, 0, pl.ds(1, ny - 1), pl.ds(PAD + 8, nx - 16), :]
            to = new_v.at[c, pl.ds(1, ny - 1), pl.ds(8, nx - 16), :]
            copies.append(pltpu.make_async_copy(part, to, sems.at[c]))
            copies[-1].start()

    def out_copy(c, y):
        part = s.at[c, 0, y, pl.ds(PAD + 8, nx - 16), :]
        to = new_s.at[c, y, pl.ds(8, nx - 16), :]
        return pltpu.make_async_copy(part, to, sems.at[3 + c * ny + y])

    def stresses(y, carry):
        for row in range(8, nx - 8, 8):
            stress_tile(v, s, m, y, row, lanes, (0,) if final else (0, 1))
        if final:
            for c in range(6):
                out_copy(c, y).start()
        return carry

    lax.fori_loop(1, ny - 1, stresses, 0)
    if final:
        for copy in copies:
            copy.wait()

        def wait(y, carry):
            for c in range(6):
                out_copy(c, y).wait()
            return carry

        lax.fori_loop(1, ny - 1, wait, 0)


def boundary_kernel(first, final, flags, eighths, *refs):
    refs = list(refs)

    def pop(n):
        out = refs[:n]
        del refs[:n]
        return out

    r_a, r_b, m = pop(3)
    if not first:
        (ahead_b,) = pop(1)
    pop(3)
    if final:
        pop(2)
    v, s, fault = pop(3)
    if first:
        (ahead_b,) = pop(1)
    if final:
        new_v, new_s, slip_out, rows, turned, strips, sems = refs
    else:
        y_a, y_b, rows, turned, strips = refs
    ny, width = m.shape[2], m.shape[4]
    nx = m.shape[3] - 16
    cross = cross_row(nx)
    span = nx + 8
    odd = flags[1] == 1
    lanes = lane_index((8, width))
    halos = eighths[...]

    count = SLOTS if first else 3
    cross_tile = strip_receive(r_a, r_b, count * span, count, odd, turned, strips, lanes)

    def received(row):
        at_row = packed_row(row, nx)
        from_a = [r_a[pl.ds(k * span + at_row, 8), :] for k in range(count)]
        from_b = [r_b[pl.ds(k * span + at_row, 8), :] for k in range(count)]
        low = [jnp.where(odd, a, b) for a, b in zip(from_a, from_b)]
        high = [jnp.where(odd, b, a) for a, b in zip(from_a, from_b)]
        packed = strips[row : row + 8, :] if row < nx else cross_tile
        return low, high, packed

    if first:
        for t in range(2):
            to = pl.ds(SLOTS * (span + STRIP) + 8 + 8 * t, 8)
            lines = jnp.where(odd, r_b[to, :], r_a[to, :])
            for k in range(6):
                fault[k, t, ny : ny + 1, :] = lines[k : k + 1, :]
    for row in row_tiles(nx):
        low, high, packed = received(row)
        if first:
            ahead_b[0, pl.ds(row, 8), :] = high[3]
            ahead_b[1, pl.ds(row, 8), :] = strip_take(packed, SLOTS + 3)
        for t in range(2):
            scale = DT * m[B, t, 0, pl.ds(row, 8), :]
            scale_ahead = DT * ahead_b[t, pl.ds(row, 8), :]
            for c in range(3):
                low_c = low[c] if t == 0 else strip_take(packed, c)
                high_c = high[c] if t == 0 else strip_take(packed, SLOTS + c)
                v[c, t, 0, pl.ds(PAD + row, 8), :] = at(v, c, t, 0, row) - scale * low_c
                v[c, t, ny, pl.ds(PAD + row, 8), :] = high_c - scale_ahead * at(
                    s, ALONG_Y[c], t, ny - 1, row
                )

    places = ((0, (nx - 1, cross)), (1, (0, cross + 7)))
    for side, pair in places:

        @pl.when(flags[0] == side)
        def _(pair=pair):
            for which, row in enumerate(pair):
                for t in range(2):
                    for y in range(ny + 1):
                        for c in range(3):
                            rows[which, c, t, y : y + 1, :] = v[
                                c, t, y, PAD + row : PAD + row + 1, :
                            ]
                        if first:
                            if y < ny:
                                line = m[B, t, y, row : row + 1, :]
                            else:
                                line = ahead_b[t, row : row + 1, :]
                            fault[OWN_B + which, t, y : y + 1, :] = line

    minus = flags[0] == 0
    sign = jnp.where(minus, DT, -DT)
    for t in range(2):
        for half in range(0, fault.shape[2], 8):
            part = slice(half, half + 8)
            own = [rows[0, c, t, part, :] for c in range(3)]
            other = [rows[1, c, t, part, :] for c in range(3)]
            par = [fault[k, t, part, :] for k in range(8)]
            m_side = [jnp.where(minus, a, b) for a, b in zip(own, other)]
            p_side = [jnp.where(minus, b, a) for a, b in zip(own, other)]
            m_b = jnp.where(minus, par[OWN_B], par[OTHER_B])
            p_b = jnp.where(minus, par[OTHER_B], par[OWN_B])
            traction, slip = friction(m_side, p_side, m_b, p_b, par)
            fault[SLIP, t, part, :] = slip
            for c in range(3):
                rows[0, c, t, part, :] = own[c] + sign * par[OWN_B] * traction[c]
                rows[1, c, t, part, :] = other[c] - sign * par[OTHER_B] * traction[c]
    for y in (0, ny - 1):
        for row in range(8, nx - 8, 8):
            stress_tile(v, s, m, y, row, lanes, (0,) if final else (0, 1))
    for side, pair in places:

        @pl.when(flags[0] == side)
        def _(pair=pair):
            for which, row in enumerate(pair):
                for c in range(3):
                    for t in range(2):
                        for y in range(ny + 1):
                            v[c, t, y, PAD + row : PAD + row + 1, :] = rows[
                                which, c, t, y : y + 1, :
                            ]

    if final:
        copies = []

        def send(pairs):
            for part, to in pairs:
                copies.append(pltpu.make_async_copy(part, to, sems.at[len(copies)]))
                copies[-1].start()

        def plane(ref, out, c, y):
            return ref.at[c, 0, y, pl.ds(PAD, nx), :], out.at[c, y]

        def edge(ref, out, c, inside, row):
            part = ref.at[c, 0, pl.ds(1, inside), pl.ds(PAD + row, 8), :]
            return part, out.at[c, pl.ds(1, inside), pl.ds(row, 8), :]

        send([plane(v, new_v, c, 0) for c in range(3)])
        send([edge(v, new_v, c, ny - 1, row) for c in range(3) for row in (0, nx - 8)])
    tiles = (0,) if final else (0, 1)
    for y in (0, ny - 1):
        for row in (0, nx - 8) if final else (0, nx - 8, cross):
            stress_tile(v, s, m, y, row, lanes, tiles)
    if not final:
        partial_trials(v, s, m, nx, lanes)
        write_messages(v, s, None, halos, odd, y_a, y_b, strips, nx)
        return

    send([plane(s, new_s, c, y) for c in range(6) for y in (0, ny - 1)])

    def ends(y, carry):
        for row in (0, nx - 8):
            stress_tile(v, s, m, y, row, lanes, tiles)
        return carry

    lax.fori_loop(1, ny - 1, ends, 0)
    send([edge(s, new_s, c, ny - 2, row) for c in range(6) for row in (0, nx - 8)])
    slip_out[...] = fault[SLIP, 0, 0:ny, :]
    for copy in copies:
        copy.wait()


def inverse_sinh(values):
    size = jnp.abs(values)
    sign = jnp.where(values > 0.0, 1.0, jnp.where(values < 0.0, -1.0, 0.0))
    return sign * jnp.log(size + jnp.sqrt(size * size + 1.0))


def friction(minus_side, plus_side, minus_b, plus_b, par):
    total = DT * (minus_b + plus_b)
    impedance = 1.0 / jnp.where(total > 0.0, total, 1.0)
    jump = [p - q for p, q in zip(plus_side, minus_side)]
    locked_y = par[PRE_Y] + impedance * jump[1]
    locked_z = par[PRE_Z] + impedance * jump[2]
    magnitude = jnp.sqrt(locked_y * locked_y + locked_z * locked_z + 1.0)
    rate, strength, slip = par[RATE], par[STRENGTH], par[SLIP]
    for _ in range(NEWTON):
        scaled = rate * slip
        residual = magnitude - impedance * slip - strength * inverse_sinh(scaled)
        tangent = -impedance - strength * rate / jnp.sqrt(1.0 + scaled * scaled)
        slip = slip - residual / tangent
    slip = slip * par[MASK]
    retained = 1.0 - impedance * slip / magnitude
    traction = (
        impedance * jump[0],
        retained * locked_y - par[PRE_Y],
        retained * locked_z - par[PRE_Z],
    )
    return traction, slip


def f32(*shape):
    return VMEM(shape, jnp.float32)


def call(kernel, name, outs, in_specs, aliases, scratch=(), flops=0, out_specs=None):
    return pl.pallas_call(
        kernel,
        out_shape=tuple(outs),
        in_specs=in_specs,
        out_specs=tuple(out_specs or [in_vmem() for _ in outs]),
        input_output_aliases=aliases,
        scratch_shapes=list(scratch),
        compiler_params=pltpu.CompilerParams(vmem_limit_bytes=8 << 20),
        cost_estimate=pl.CostEstimate(flops=flops, bytes_accessed=0, transcendentals=0),
        name=name,
    )


def pair_swaps(a, b, axis):
    size = lax.axis_size(axis)
    out = []
    for value, start in ((a, 0), (b, 1)):
        pairs = []
        for i in range(start, size - 1, 2):
            pairs += [(i, i + 1), (i + 1, i)]
        out.append(lax.ppermute(value, axis, pairs))
    return out


def local(
    velocity,
    stress,
    buoyancy,
    stiff_xx,
    stiff_xz,
    stiff_zz,
    shear_vert,
    shear_horiz,
    prestress,
    fault_mask,
    region_ids,
    inverse_rate,
    slip_prev,
    region_a,
    region_normal,
):
    ny, nx, width = buoyancy.shape
    assert nx == width
    across, along, dip = (lax.axis_index(k) for k in ("gx", "gy", "gz"))
    flags = jnp.stack([across, along % 2, dip % 2]).astype(jnp.int32)
    lanes = jnp.broadcast_to(jnp.arange(width, dtype=jnp.int32), (8, width))
    thirds, eighths = lanes // HALO, lanes // STRIP
    rows = cross_row(nx) + 8
    high = 8 * ((ny + 1 + 7) // 8)
    v_shape = f32(3, 2, ny + 1, rows + 2 * PAD, width)
    s_shape = f32(6, 2, ny, rows + 2 * PAD, width)
    m_shape = f32(6, 2, ny, rows, width)
    fault_shape = f32(8, 2, high, width)
    planes = z_slots(ny, width)[1]
    z_shape = f32(planes, nx + 16, width)
    unit = ny * nx * width
    vm, hb, sm = in_vmem(), in_hbm(), in_smem()
    raw = [velocity, stress, buoyancy, stiff_xx, stiff_xz, stiff_zz, shear_vert, shear_horiz]
    raw += [prestress, region_ids, fault_mask, inverse_rate, slip_prev, region_a, region_normal]
    raw = [pltpu.with_memory_space_constraint(k, HBM) for k in raw]

    f_shape = f32(len(FIELDS), ny // 2, 8, width)
    (f_own,) = call(
        edge_kernel,
        "edge",
        (f_shape,),
        [sm] + [hb] * 8,
        {},
        [pltpu.SemaphoreType.DMA((2 * len(FIELDS),))],
        flops=unit,
    )(flags, *raw[:8])
    f_other = lax.ppermute(f_own, "gx", [(i, i ^ 1) for i in range(lax.axis_size("gx"))])
    v, s, m, fault, z_a, z_b = call(
        load_kernel,
        "load",
        (v_shape, s_shape, m_shape, fault_shape, z_shape, z_shape),
        [sm, vm] + [hb] * 15,
        {},
        [
            pltpu.VMEM(prestress.shape, jnp.float32),
            pltpu.VMEM(region_ids.shape, jnp.int32),
            pltpu.VMEM(fault_mask.shape, jnp.int32),
            pltpu.VMEM(inverse_rate.shape, jnp.float32),
            pltpu.VMEM(slip_prev.shape, jnp.float32),
            pltpu.SMEM(region_a.shape, jnp.float32),
            pltpu.SMEM(region_normal.shape, jnp.float32),
            pltpu.SemaphoreType.DMA((22,)),
        ],
        flops=100 * unit,
    )(flags, thirds, *raw)
    v, s, m, z_a, z_b = call(
        cross_kernel,
        "cross",
        (v_shape, s_shape, m_shape, z_shape, z_shape),
        [sm] + [vm] * 8,
        {4: 0, 5: 1, 6: 2, 7: 3, 8: 4},
        flops=10 * unit,
    )(flags, thirds, f_other, fault, v, s, m, z_a, z_b)
    z_a, z_b = pair_swaps(z_a, z_b, "gz")
    y_shape = f32(SLOTS * (nx + 8 + STRIP) + 8 + 16, width)
    v, s, m, fault, y_a, y_b = call(
        widen_kernel,
        "widen",
        (v_shape, s_shape, m_shape, fault_shape, y_shape, y_shape),
        [sm] + [vm] * 8,
        {5: 0, 6: 1, 7: 2, 8: 3},
        [pltpu.VMEM((nx, width), jnp.float32)],
        flops=50 * unit,
    )(flags, thirds, eighths, z_a, z_b, v, s, m, fault)
    v, s, m = call(
        rest_kernel,
        "rest",
        (v_shape, s_shape, m_shape),
        [sm] + [vm] * 6,
        {4: 0, 5: 1, 6: 2},
        flops=50 * unit,
    )(flags, thirds, z_a, z_b, v, s, m)
    y_shape = f32(3 * (nx + 8) + STRIP * 3 + 8, width)
    ahead_b = None
    out_shapes = (HBM((3, ny, nx, width), jnp.float32), HBM((6, ny, nx, width), jnp.float32))
    for step in range(STEPS):
        first, final = step == 0, step == STEPS - 1
        y_a, y_b = pair_swaps(y_a, y_b, "gy")
        v, s, *outs = call(
            functools.partial(inner_kernel, first, final),
            "inner",
            (v_shape, s_shape) + (out_shapes if final else ()),
            [vm] * 3,
            {1: 0, 2: 1},
            [pltpu.SemaphoreType.DMA((3 + 6 * ny,))] if final else [],
            flops=200 * unit,
            out_specs=[vm, vm] + ([hb, hb] if final else []),
        )(m, v, s)
        args = [flags, eighths, y_a, y_b, m]
        args += ([] if first else [ahead_b]) + [v, s, fault] + outs
        at_state = len(args) - len(outs) - 3
        aliases = {at_state + k: k for k in range(3)}
        shapes, specs = [v_shape, s_shape, fault_shape], [vm, vm, vm]
        scratch = [pltpu.VMEM((2, 3, 2, high, width), jnp.float32)]
        scratch += [pltpu.VMEM((width, nx), jnp.float32), pltpu.VMEM((nx, width), jnp.float32)]
        if first:
            shapes.append(f32(2, rows, width))
            specs.append(vm)
        if final:
            shapes += [*out_shapes, jax.ShapeDtypeStruct((ny, width), jnp.float32)]
            specs += [hb, hb, vm]
            scratch.append(pltpu.SemaphoreType.DMA((3 * 3 + 6 * 4,)))
            aliases.update({at_state + 3: 3, at_state + 4: 4})
        else:
            shapes += [y_shape, y_shape]
            specs += [vm, vm]
        v, s, fault, *more = call(
            functools.partial(boundary_kernel, first, final),
            "boundary",
            shapes,
            [sm] + [vm] * (len(args) - 1 - len(outs)) + [hb] * len(outs),
            aliases,
            scratch,
            flops=50 * unit,
            out_specs=specs,
        )(*args)
        if final:
            return tuple(more)
        if first:
            ahead_b, *more = more
        y_a, y_b = more


def solution(mesh):
    in_specs = (
        P(None, "gy", "gx", "gz"),
        P(None, "gy", "gx", "gz"),
        P("gy", "gx", "gz"),
        P("gy", "gx", "gz"),
        P("gy", "gx", "gz"),
        P("gy", "gx", "gz"),
        P("gy", "gx", "gz"),
        P("gy", "gx", "gz"),
        P(None, "gy", "gz"),
        P("gy", "gz"),
        P("gy", "gz"),
        P("gy", "gz"),
        P("gy", "gz"),
        P(),
        P(),
    )
    out_specs = (P(None, "gy", "gx", "gz"), P(None, "gy", "gx", "gz"), P("gy", "gz"))
    return jax.shard_map(local, mesh=mesh, in_specs=in_specs, out_specs=out_specs, check_vma=False)
```

```python
import functools

import jax
import jax.numpy as jnp
from jax import lax
from jax.experimental import pallas as pl
from jax.experimental.pallas import tpu as pltpu
from jax.sharding import PartitionSpec as P

STEPS = 3
NEWTON = 3
DT = 0.2

PAD = 8
HALO = 3
CROSS = 4
STRIP = 8

XX, YY, ZZ, YZ, XZ, XY = range(6)
ALONG_Y = (XY, YY, YZ)
B, C11, C13, C33, C44, C66 = range(6)
FIELDS = [("v", c) for c in range(3)] + [("s", c) for c in range(6)] + [("m", c) for c in range(6)]
PRE_Y, PRE_Z, MASK, STRENGTH, RATE, SLIP, OWN_B, OTHER_B = range(8)

VMEM = pltpu.MemorySpace.VMEM
HBM = pltpu.MemorySpace.HBM


def odd_on(axis):
    return lax.rem(lax.axis_index(axis), 2) == 1


def in_vmem():
    return pl.BlockSpec(memory_space=VMEM)


def in_hbm():
    return pl.BlockSpec(memory_space=HBM)


def roll(values, by):
    by = by % values.shape[-1]
    return values if by == 0 else pltpu.roll(values, by, values.ndim - 1)


def at(ref, field, tile, y, row):
    return ref[field, tile, y, pl.ds(PAD + row, 8), :]


def z_below(pair, lanes):
    one, two = roll(pair[0], 1), roll(pair[1], 1)
    first = lanes == 0
    return jnp.where(first, two, one), jnp.where(first, one, two)


def z_above(pair, lanes):
    one, two = roll(pair[0], -1), roll(pair[1], -1)
    last = lanes == pair[0].shape[-1] - 1
    return jnp.where(last, two, one), jnp.where(last, one, two)


def trial_tile(v, s, m, y, row, below, lanes):
    both = (0, 1)
    behind = {c: z_below([at(s, c, t, y, row) for t in both], lanes) for c in (XZ, YZ, ZZ)}
    out = []
    for t in both:
        own = {c: at(s, c, t, y, row) for c in range(6)}
        lower_x = {c: own[c] - at(s, c, t, y, row - 1) for c in (XX, XY, XZ)}
        if below is None:
            lower_y = {c: own[c] for c in ALONG_Y}
        else:
            lower_y = {c: own[c] - below(c, t) for c in ALONG_Y}
        scale = DT * m[B, t, y, pl.ds(row, 8), :]
        total = (
            lower_x[XX] + lower_y[XY] + (own[XZ] - behind[XZ][t]),
            lower_x[XY] + lower_y[YY] + (own[YZ] - behind[YZ][t]),
            lower_x[XZ] + lower_y[YZ] + (own[ZZ] - behind[ZZ][t]),
        )
        out.append([at(v, c, t, y, row) + scale * total[c] for c in range(3)])
    return out


def stress_tile(v, s, m, y, row, lanes, tiles=(0, 1)):
    both = (0, 1)
    own = [[at(v, c, t, y, row) for t in both] for c in range(3)]
    ahead = [z_above(own[c], lanes) for c in range(3)]
    for t in tiles:
        vx, vy, vz = own[0][t], own[1][t], own[2][t]
        over_x = [at(v, c, t, y, row + 1) for c in range(3)]
        over_y = [at(v, c, t, y + 1, row) for c in range(3)]
        exx, eyy, ezz = over_x[0] - vx, over_y[1] - vy, ahead[2][t] - vz
        c11, c13, c33, c44, c66 = (m[k, t, y, pl.ds(row, 8), :] for k in (C11, C13, C33, C44, C66))
        c12 = c11 - 2.0 * c66
        third = c13 * ezz
        change = {
            XX: c11 * exx + c12 * eyy + third,
            YY: c12 * exx + c11 * eyy + third,
            ZZ: c13 * (exx + eyy) + c33 * ezz,
            YZ: c44 * ((ahead[1][t] - vy) + (over_y[2] - vz)),
            XZ: c44 * ((ahead[0][t] - vx) + (over_x[2] - vz)),
            XY: c66 * ((over_y[0] - vx) + (over_x[1] - vy)),
        }
        for c, gain in change.items():
            s[c, t, y, pl.ds(PAD + row, 8), :] = at(s, c, t, y, row) + DT * gain


def lane_index(like):
    return lax.broadcasted_iota(jnp.int32, like, len(like) - 1)


SLOTS = 4


def strip_tile(up, down, eighths):
    packed = jnp.zeros_like(up[0])
    for start, pieces in ((0, up), (SLOTS, down)):
        for k, piece in enumerate(pieces):
            moved = roll(piece, STRIP * (start + k) + HALO)
            packed = jnp.where(eighths == start + k, moved, packed)
    return packed


def strip_take(packed, slot):
    return roll(packed, -(STRIP * slot + HALO))


def strip_send(strips, cross_tile, count, odd, y_a, y_b, base):
    turned = strips[...].T
    for j in range(0, STRIP * count, 8):
        up = turned[j : j + 8, :]
        down = turned[STRIP * SLOTS + j : STRIP * SLOTS + j + 8, :]
        y_a[base + j : base + j + 8, :] = jnp.where(odd, down, up)
        y_b[base + j : base + j + 8, :] = jnp.where(odd, up, down)
    other = roll(cross_tile, -STRIP * SLOTS)
    last = base + STRIP * count
    y_a[last : last + 8, :] = jnp.where(odd, other, cross_tile)
    y_b[last : last + 8, :] = jnp.where(odd, cross_tile, other)


def strip_receive(r_a, r_b, base, count, odd, turned, strips, lanes):
    turned[...] = jnp.zeros_like(turned)
    for j in range(0, STRIP * count, 8):
        from_a, from_b = r_a[base + j : base + j + 8, :], r_b[base + j : base + j + 8, :]
        turned[j : j + 8, :] = jnp.where(odd, from_a, from_b)
        start = STRIP * SLOTS + j
        turned[start : start + 8, :] = jnp.where(odd, from_b, from_a)
    strips[...] = turned[...].T
    last = base + STRIP * count
    from_a, from_b = r_a[last : last + 8, :], r_b[last : last + 8, :]
    low, high = jnp.where(odd, from_a, from_b), jnp.where(odd, from_b, from_a)
    return jnp.where(lanes < STRIP * SLOTS, low, roll(high, STRIP * SLOTS))


def field_ref(kind, v, s, m):
    return {"v": v, "s": s, "m": m}[kind]


def fields_per_plane(ny, width):
    return (width - 5) // HALO // ny


def z_slots(ny, width):
    per_plane = fields_per_plane(ny, width)
    slots = {}
    for f in range(len(FIELDS)):
        for y in range(ny):
            slots[f, y] = (f // per_plane, f % per_plane * ny + y)
    return slots, -(-len(FIELDS) // per_plane)


def row_tiles(nx):
    return [*range(0, nx, 8), cross_row(nx)]


def cross_row(nx):
    return nx + PAD


def packed_row(row, nx):
    return row if row < nx else nx


def edge_kernel(velocity, stress, *rest):
    raw_m, out, sem = rest[:6], rest[6], rest[7]
    ny, nx = velocity.shape[1:3]
    sources = [velocity.at[c] for c in range(3)] + [stress.at[c] for c in range(6)] + list(raw_m)
    for side, row in ((0, nx - CROSS), (1, 0)):

        @pl.when(lax.axis_index("gx") == side)
        def _(row=row):
            copies = []
            for f, source in enumerate(sources):
                for half in range(2):
                    part = source.at[pl.ds(half * (ny // 2), ny // 2), pl.ds(row, CROSS), :]
                    to = out.at[f, :, pl.ds(half * CROSS, CROSS), :]
                    copies.append(pltpu.make_async_copy(part, to, sem.at[2 * f + half]))
            for copy in copies:
                copy.start()
            for copy in copies:
                copy.wait()


def load_kernel(thirds, velocity, stress, *rest):
    raw_m, small = rest[:6], rest[6:13]
    v, s, m, fault, z_a, z_b = rest[13:19]
    pre, ids, mask, rate, slip, region_a, region_normal, sems = rest[19:]
    ny, nx, width = velocity.shape[1:]
    cross = cross_row(nx)
    big = {}
    for c in range(3):
        big["v", c] = (velocity.at[c], v.at[c, 0, pl.ds(0, ny), pl.ds(PAD, nx), :])
    for c in range(6):
        big["s", c] = (stress.at[c], s.at[c, 0, :, pl.ds(PAD, nx), :])
    for c in range(6):
        big["m", c] = (raw_m[c], m.at[c, 0, :, pl.ds(0, nx), :])
    big = {
        key: pltpu.make_async_copy(a, b, sems.at[k]) for k, (key, (a, b)) in enumerate(big.items())
    }
    held = (pre, ids, mask, rate, slip, region_a, region_normal)
    little = [
        pltpu.make_async_copy(a, b, sems.at[len(big) + k])
        for k, (a, b) in enumerate(zip(small, held))
    ]
    for copy in big.values():
        copy.start()
    for copy in little:
        copy.start()
    zeros = jnp.zeros((PAD, width), jnp.float32)
    for t in range(2):
        for y in range(ny):
            for c in (XX, XY, XZ):
                s[c, t, y, 0:PAD, :] = zeros
                s[c, t, y, cross : cross + PAD, :] = zeros
            for c in range(3):
                v[c, t, y, PAD + nx : PAD + nx + PAD, :] = zeros
                v[c, t, y, PAD + cross + 8 : 2 * PAD + cross + 8, :] = zeros

    per_plane = fields_per_plane(ny, width)
    odd = odd_on("gz")
    group = thirds[...]
    for plane in range(z_slots(ny, width)[1]):
        for key in FIELDS[plane * per_plane : (plane + 1) * per_plane]:
            big[key].wait()

        def pack(i, carry, plane=plane):
            for part in range(UNROLL):
                row = pl.multiple_of((i * UNROLL + part) * 8, 8)
                z_emit(z_a, z_b, odd, group, z_pieces(plane, v, s, m, row), plane, row)
            return carry

        lax.fori_loop(0, nx // (8 * UNROLL), pack, 0)
    for copy in little:
        copy.wait()
    kinds = ids[...]
    a_part = jnp.zeros((ny, width), jnp.float32)
    n_part = jnp.zeros((ny, width), jnp.float32)
    for k in range(region_a.shape[0]):
        a_part = jnp.where(kinds == k, region_a[k], a_part)
        n_part = jnp.where(kinds == k, region_normal[k], n_part)
    fault[PRE_Y, 0, 0:ny, :] = pre[0]
    fault[PRE_Z, 0, 0:ny, :] = pre[1]
    fault[MASK, 0, 0:ny, :] = mask[...].astype(jnp.float32)
    fault[STRENGTH, 0, 0:ny, :] = a_part * n_part
    fault[RATE, 0, 0:ny, :] = rate[...]
    fault[SLIP, 0, 0:ny, :] = slip[...]


UNROLL = 4


def z_emit(z_a, z_b, odd, group, pieces, plane, row):
    up = jnp.zeros_like(pieces[0][1])
    down = up
    for pos, piece in pieces:
        moved = roll(piece, HALO * pos + HALO)
        up = jnp.where(group == pos, moved, up)
        down = jnp.where(group == pos + 1, moved, down)
    z_a[plane, pl.ds(row, 8), :] = jnp.where(odd, down, up)
    z_b[plane, pl.ds(row, 8), :] = jnp.where(odd, up, down)


def z_pieces(plane, v, s, m, row):
    ny, width = m.shape[2], m.shape[4]
    per_plane = fields_per_plane(ny, width)
    pieces = []
    for f, (kind, c) in enumerate(FIELDS[plane * per_plane : (plane + 1) * per_plane]):
        shift = 0 if kind == "m" else PAD
        ref = field_ref(kind, v, s, m)
        for y in range(ny):
            pieces.append((f * ny + y, ref[c, 0, y, pl.ds(row + shift, 8), :]))
    return pieces


def cross_kernel(thirds, f_other, fault, v_in, s_in, m_in, za_in, zb_in, v, s, m, z_a, z_b):
    ny, width = m.shape[2], m.shape[4]
    nx = z_a.shape[1] - 16
    cross = cross_row(nx)
    odd = odd_on("gz")
    group = thirds[...]
    planes = z_slots(ny, width)[1]
    rows = lax.broadcasted_iota(jnp.int32, (8, width), 0)
    minus = lax.axis_index("gx") == 0
    keep = jnp.where(minus, 7 - rows, rows) >= 8 - CROSS
    for f, (kind, c) in enumerate(FIELDS):
        shift = 0 if kind == "m" else PAD
        ref = field_ref(kind, v, s, m)
        for y in range(ny // 2):
            tile = f_other[f, y]
            turned = pltpu.roll(tile, CROSS, 0)
            ref[c, 0, y, cross + shift : cross + shift + 8, :] = jnp.where(
                keep, jnp.where(minus, tile, turned), 0.0
            )
            ref[c, 0, y + ny // 2, cross + shift : cross + shift + 8, :] = jnp.where(
                keep, jnp.where(minus, turned, tile), 0.0
            )
    for plane in range(planes):
        z_emit(z_a, z_b, odd, group, z_pieces(plane, v, s, m, cross), plane, nx)
    z_emit(z_a, z_b, odd, group, [(k, fault[k, 0, 0:8, :]) for k in range(6)], 0, nx + 8)
    zeros = jnp.zeros((8, width), jnp.float32)
    for plane in range(1, planes):
        z_a[plane, pl.ds(nx + 8, 8), :] = zeros
        z_b[plane, pl.ds(nx + 8, 8), :] = zeros


def write_messages(v, s, buoyancy, eighths, odd, y_a, y_b, strips, nx):
    last = s.shape[2] - 1
    span = nx + 8
    count = 3 if buoyancy is None else SLOTS

    def pieces(t, row):
        up = [at(s, c, t, last, row) for c in ALONG_Y]
        down = [at(v, c, t, 0, row) for c in range(3)]
        if buoyancy is not None:
            up.append(buoyancy[B, t, 0, pl.ds(row, 8), :])
            down.append(up[-1])
        return up, down

    for row in row_tiles(nx):
        up, down = pieces(0, row)
        for k in range(count):
            to = pl.ds(k * span + packed_row(row, nx), 8)
            y_a[to, :] = jnp.where(odd, down[k], up[k])
            y_b[to, :] = jnp.where(odd, up[k], down[k])
        tile = strip_tile(*pieces(1, row), eighths)
        if row < nx:
            strips[row : row + 8, :] = tile
    strip_send(strips, tile, count, odd, y_a, y_b, count * span)


def partial_trials(v, s, m, nx, lanes):
    for row in row_tiles(nx):
        new = trial_tile(v, s, m, 0, row, None, lanes)
        for t in range(2):
            for c in range(3):
                v[c, t, 0, pl.ds(PAD + row, 8), :] = new[t][c]


class ZHalo:
    def __init__(self, odd, group, r_a, r_b, planes):
        self.odd, self.group, self.r_a, self.r_b, self.planes = odd, group, r_a, r_b, planes

    def take(self, row, wanted):
        for plane in range(self.planes):
            chosen = [(pos, store) for (p, pos), store in wanted if p == plane]
            if chosen:
                from_a = self.r_a[plane, pl.ds(row, 8), :]
                from_b = self.r_b[plane, pl.ds(row, 8), :]
                low = jnp.where(self.odd, from_a, from_b)
                high = jnp.where(self.odd, from_b, from_a)
                for pos, store in chosen:
                    both = jnp.where(self.group == pos, low, high)
                    store(roll(both, -(HALO * pos + HALO)))


def needed_first(kind, c, y, ny):
    if y == 0:
        return kind != "m" or c == B
    return y == ny - 1 and kind == "s" and c in ALONG_Y


def unpack_fields(halo, v, s, m, nx, first):
    ny, width = m.shape[2], m.shape[4]
    slots = z_slots(ny, width)[0]

    def store_to(ref, c, y, row):
        def store(value):
            ref[c, 1, y, pl.ds(row, 8), :] = value

        return store

    def fields(row):
        wanted = []
        for f, (kind, c) in enumerate(FIELDS):
            shift = 0 if kind == "m" else PAD
            ref = field_ref(kind, v, s, m)
            for y in range(ny):
                if needed_first(kind, c, y, ny) == first:
                    wanted.append((slots[f, y], store_to(ref, c, y, row + shift)))
        return wanted

    def unpack(i, carry):
        for part in range(UNROLL):
            row = pl.multiple_of((i * UNROLL + part) * 8, 8)
            halo.take(row, fields(row))
        return carry

    lax.fori_loop(0, nx // (8 * UNROLL), unpack, 0)
    halo.take(nx, fields(cross_row(nx)))


def rest_kernel(thirds, r_a, r_b, v_in, s_in, m_in, v, s, m):
    nx = r_a.shape[1] - 16
    planes = z_slots(m.shape[2], m.shape[4])[1]
    halo = ZHalo(odd_on("gz"), thirds[...], r_a, r_b, planes)
    unpack_fields(halo, v, s, m, nx, False)


def widen_kernel(
    thirds, eighths, r_a, r_b, v_in, s_in, m_in, f_in, v, s, m, fault, y_a, y_b, strips
):
    ny, width = m.shape[2], m.shape[4]
    nx = r_a.shape[1] - 16
    planes = z_slots(ny, width)[1]
    odd_y = odd_on("gy")
    lanes = lane_index((8, width))
    halo = ZHalo(odd_on("gz"), thirds[...], r_a, r_b, planes)
    unpack_fields(halo, v, s, m, nx, True)

    def store_fault(k):
        def store(value):
            fault[k, 1, 0:8, :] = value

        return store

    halo.take(nx + 8, [((0, k), store_fault(k)) for k in range(6)])
    partial_trials(v, s, m, nx, lanes)
    write_messages(v, s, m, eighths[...], odd_y, y_a, y_b, strips, nx)
    for t in range(2):
        for k in range(8):
            line = fault[min(k, 5), t, 0:1, :]
            row = SLOTS * (nx + 8 + STRIP) + 8 + 8 * t + k
            y_a[row : row + 1, :] = line
            y_b[row : row + 1, :] = line


def inner_kernel(first, final, m, v_in, s_in, v, s, *outs):
    ny, width = m.shape[2], m.shape[4]
    nx = m.shape[3] - 16
    lanes = lane_index((8, width))

    if not first:

        def ends(y, carry):
            for row in (0, nx - 8, cross_row(nx)):
                stress_tile(v, s, m, y, row, lanes)
            return carry

        lax.fori_loop(1, ny - 1, ends, 0)

    def trials(y, carry):
        for row in row_tiles(nx):
            new = trial_tile(
                v, s, m, y, row, lambda c, t, row=row: at(s, c, t, y - 1, row), lanes
            )
            for t in range(2):
                for c in range(3):
                    v[c, t, y, pl.ds(PAD + row, 8), :] = new[t][c]
        return carry

    lax.fori_loop(1, ny, trials, 0)
    copies = []
    if final:
        new_v, new_s, sems = outs
        for c in range(3):
            part = v.at[c, 0, pl.ds(1, ny - 1), pl.ds(PAD + 8, nx - 16), :]
            to = new_v.at[c, pl.ds(1, ny - 1), pl.ds(8, nx - 16), :]
            copies.append(pltpu.make_async_copy(part, to, sems.at[c]))
            copies[-1].start()

    def out_copy(c, y):
        part = s.at[c, 0, y, pl.ds(PAD + 8, nx - 16), :]
        to = new_s.at[c, y, pl.ds(8, nx - 16), :]
        return pltpu.make_async_copy(part, to, sems.at[3 + c * ny + y])

    def stresses(y, carry):
        for row in range(8, nx - 8, 8):
            stress_tile(v, s, m, y, row, lanes, (0,) if final else (0, 1))
        if final:
            for c in range(6):
                out_copy(c, y).start()
        return carry

    lax.fori_loop(1, ny - 1, stresses, 0)
    if final:
        for copy in copies:
            copy.wait()

        def wait(y, carry):
            for c in range(6):
                out_copy(c, y).wait()
            return carry

        lax.fori_loop(1, ny - 1, wait, 0)


def boundary_kernel(first, final, eighths, *refs):
    refs = list(refs)

    def pop(n):
        out = refs[:n]
        del refs[:n]
        return out

    r_a, r_b, m = pop(3)
    if not first:
        (ahead_b,) = pop(1)
    pop(3)
    if final:
        pop(2)
    v, s, fault = pop(3)
    if first:
        (ahead_b,) = pop(1)
    if final:
        new_v, new_s, slip_out, rows, turned, strips, sems = refs
    else:
        y_a, y_b, rows, turned, strips = refs
    ny, width = m.shape[2], m.shape[4]
    nx = m.shape[3] - 16
    cross = cross_row(nx)
    span = nx + 8
    odd = odd_on("gy")
    lanes = lane_index((8, width))
    halos = eighths[...]

    count = SLOTS if first else 3
    cross_tile = strip_receive(r_a, r_b, count * span, count, odd, turned, strips, lanes)

    def received(row):
        at_row = packed_row(row, nx)
        from_a = [r_a[pl.ds(k * span + at_row, 8), :] for k in range(count)]
        from_b = [r_b[pl.ds(k * span + at_row, 8), :] for k in range(count)]
        low = [jnp.where(odd, a, b) for a, b in zip(from_a, from_b)]
        high = [jnp.where(odd, b, a) for a, b in zip(from_a, from_b)]
        packed = strips[row : row + 8, :] if row < nx else cross_tile
        return low, high, packed

    if first:
        for t in range(2):
            to = pl.ds(SLOTS * (span + STRIP) + 8 + 8 * t, 8)
            lines = jnp.where(odd, r_b[to, :], r_a[to, :])
            for k in range(6):
                fault[k, t, ny : ny + 1, :] = lines[k : k + 1, :]
    for row in row_tiles(nx):
        low, high, packed = received(row)
        if first:
            ahead_b[0, pl.ds(row, 8), :] = high[3]
            ahead_b[1, pl.ds(row, 8), :] = strip_take(packed, SLOTS + 3)
        for t in range(2):
            scale = DT * m[B, t, 0, pl.ds(row, 8), :]
            scale_ahead = DT * ahead_b[t, pl.ds(row, 8), :]
            for c in range(3):
                low_c = low[c] if t == 0 else strip_take(packed, c)
                high_c = high[c] if t == 0 else strip_take(packed, SLOTS + c)
                v[c, t, 0, pl.ds(PAD + row, 8), :] = at(v, c, t, 0, row) - scale * low_c
                v[c, t, ny, pl.ds(PAD + row, 8), :] = high_c - scale_ahead * at(
                    s, ALONG_Y[c], t, ny - 1, row
                )

    places = ((0, (nx - 1, cross)), (1, (0, cross + 7)))
    for side, pair in places:

        @pl.when(lax.axis_index("gx") == side)
        def _(pair=pair):
            for which, row in enumerate(pair):
                for t in range(2):
                    for y in range(ny + 1):
                        for c in range(3):
                            rows[which, c, t, y : y + 1, :] = v[
                                c, t, y, PAD + row : PAD + row + 1, :
                            ]
                        if first:
                            if y < ny:
                                line = m[B, t, y, row : row + 1, :]
                            else:
                                line = ahead_b[t, row : row + 1, :]
                            fault[OWN_B + which, t, y : y + 1, :] = line

    minus = lax.axis_index("gx") == 0
    sign = jnp.where(minus, DT, -DT)
    for t in range(2):
        for half in range(0, fault.shape[2], 8):
            part = slice(half, half + 8)
            own = [rows[0, c, t, part, :] for c in range(3)]
            other = [rows[1, c, t, part, :] for c in range(3)]
            par = [fault[k, t, part, :] for k in range(8)]
            m_side = [jnp.where(minus, a, b) for a, b in zip(own, other)]
            p_side = [jnp.where(minus, b, a) for a, b in zip(own, other)]
            m_b = jnp.where(minus, par[OWN_B], par[OTHER_B])
            p_b = jnp.where(minus, par[OTHER_B], par[OWN_B])
            traction, slip = friction(m_side, p_side, m_b, p_b, par)
            fault[SLIP, t, part, :] = slip
            for c in range(3):
                rows[0, c, t, part, :] = own[c] + sign * par[OWN_B] * traction[c]
                rows[1, c, t, part, :] = other[c] - sign * par[OTHER_B] * traction[c]
    for y in (0, ny - 1):
        for row in range(8, nx - 8, 8):
            stress_tile(v, s, m, y, row, lanes, (0,) if final else (0, 1))
    for side, pair in places:

        @pl.when(lax.axis_index("gx") == side)
        def _(pair=pair):
            for which, row in enumerate(pair):
                for c in range(3):
                    for t in range(2):
                        for y in range(ny + 1):
                            v[c, t, y, PAD + row : PAD + row + 1, :] = rows[
                                which, c, t, y : y + 1, :
                            ]

    if final:
        copies = []

        def send(pairs):
            for part, to in pairs:
                copies.append(pltpu.make_async_copy(part, to, sems.at[len(copies)]))
                copies[-1].start()

        def plane(ref, out, c, y):
            return ref.at[c, 0, y, pl.ds(PAD, nx), :], out.at[c, y]

        def edge(ref, out, c, inside, row):
            part = ref.at[c, 0, pl.ds(1, inside), pl.ds(PAD + row, 8), :]
            return part, out.at[c, pl.ds(1, inside), pl.ds(row, 8), :]

        send([plane(v, new_v, c, 0) for c in range(3)])
        send([edge(v, new_v, c, ny - 1, row) for c in range(3) for row in (0, nx - 8)])
    tiles = (0,) if final else (0, 1)
    for y in (0, ny - 1):
        for row in (0, nx - 8) if final else (0, nx - 8, cross):
            stress_tile(v, s, m, y, row, lanes, tiles)
    if not final:
        partial_trials(v, s, m, nx, lanes)
        write_messages(v, s, None, halos, odd, y_a, y_b, strips, nx)
        return

    send([plane(s, new_s, c, y) for c in range(6) for y in (0, ny - 1)])

    def ends(y, carry):
        for row in (0, nx - 8):
            stress_tile(v, s, m, y, row, lanes, tiles)
        return carry

    lax.fori_loop(1, ny - 1, ends, 0)
    send([edge(s, new_s, c, ny - 2, row) for c in range(6) for row in (0, nx - 8)])
    slip_out[...] = fault[SLIP, 0, 0:ny, :]
    for copy in copies:
        copy.wait()


def inverse_sinh(values):
    size = jnp.abs(values)
    sign = jnp.where(values > 0.0, 1.0, jnp.where(values < 0.0, -1.0, 0.0))
    return sign * jnp.log(size + jnp.sqrt(size * size + 1.0))


def friction(minus_side, plus_side, minus_b, plus_b, par):
    total = DT * (minus_b + plus_b)
    impedance = 1.0 / jnp.where(total > 0.0, total, 1.0)
    jump = [p - q for p, q in zip(plus_side, minus_side)]
    locked_y = par[PRE_Y] + impedance * jump[1]
    locked_z = par[PRE_Z] + impedance * jump[2]
    magnitude = jnp.sqrt(locked_y * locked_y + locked_z * locked_z + 1.0)
    rate, strength, slip = par[RATE], par[STRENGTH], par[SLIP]
    for _ in range(NEWTON):
        scaled = rate * slip
        residual = magnitude - impedance * slip - strength * inverse_sinh(scaled)
        tangent = -impedance - strength * rate / jnp.sqrt(1.0 + scaled * scaled)
        slip = slip - residual / tangent
    slip = slip * par[MASK]
    retained = 1.0 - impedance * slip / magnitude
    traction = (
        impedance * jump[0],
        retained * locked_y - par[PRE_Y],
        retained * locked_z - par[PRE_Z],
    )
    return traction, slip


def f32(*shape):
    return VMEM(shape, jnp.float32)


def call(kernel, name, outs, in_specs, aliases, scratch=(), flops=0, out_specs=None):
    return pl.pallas_call(
        kernel,
        out_shape=tuple(outs),
        in_specs=in_specs,
        out_specs=tuple(out_specs or [in_vmem() for _ in outs]),
        input_output_aliases=aliases,
        scratch_shapes=list(scratch),
        compiler_params=pltpu.CompilerParams(vmem_limit_bytes=8 << 20),
        cost_estimate=pl.CostEstimate(flops=flops, bytes_accessed=0, transcendentals=0),
        name=name,
    )


def pair_swaps(a, b, axis):
    size = lax.axis_size(axis)
    out = []
    for value, start in ((a, 0), (b, 1)):
        pairs = []
        for i in range(start, size - 1, 2):
            pairs += [(i, i + 1), (i + 1, i)]
        out.append(lax.ppermute(value, axis, pairs))
    return out


def local(
    velocity,
    stress,
    buoyancy,
    stiff_xx,
    stiff_xz,
    stiff_zz,
    shear_vert,
    shear_horiz,
    prestress,
    fault_mask,
    region_ids,
    inverse_rate,
    slip_prev,
    region_a,
    region_normal,
):
    ny, nx, width = buoyancy.shape
    assert nx == width
    lanes = jnp.broadcast_to(jnp.arange(width, dtype=jnp.int32), (8, width))
    thirds, eighths = lanes // HALO, lanes // STRIP
    rows = cross_row(nx) + 8
    high = 8 * ((ny + 1 + 7) // 8)
    v_shape = f32(3, 2, ny + 1, rows + 2 * PAD, width)
    s_shape = f32(6, 2, ny, rows + 2 * PAD, width)
    m_shape = f32(6, 2, ny, rows, width)
    fault_shape = f32(8, 2, high, width)
    planes = z_slots(ny, width)[1]
    z_shape = f32(planes, nx + 16, width)
    unit = ny * nx * width
    vm, hb = in_vmem(), in_hbm()
    raw = [velocity, stress, buoyancy, stiff_xx, stiff_xz, stiff_zz, shear_vert, shear_horiz]
    raw += [prestress, region_ids, fault_mask, inverse_rate, slip_prev, region_a, region_normal]
    raw = [pltpu.with_memory_space_constraint(k, HBM) for k in raw]

    f_shape = f32(len(FIELDS), ny // 2, 8, width)
    (f_own,) = call(
        edge_kernel,
        "edge",
        (f_shape,),
        [hb] * 8,
        {},
        [pltpu.SemaphoreType.DMA((2 * len(FIELDS),))],
        flops=unit,
    )(*raw[:8])
    f_other = lax.ppermute(f_own, "gx", [(i, i ^ 1) for i in range(lax.axis_size("gx"))])
    v, s, m, fault, z_a, z_b = call(
        load_kernel,
        "load",
        (v_shape, s_shape, m_shape, fault_shape, z_shape, z_shape),
        [vm] + [hb] * 15,
        {},
        [
            pltpu.VMEM(prestress.shape, jnp.float32),
            pltpu.VMEM(region_ids.shape, jnp.int32),
            pltpu.VMEM(fault_mask.shape, jnp.int32),
            pltpu.VMEM(inverse_rate.shape, jnp.float32),
            pltpu.VMEM(slip_prev.shape, jnp.float32),
            pltpu.SMEM(region_a.shape, jnp.float32),
            pltpu.SMEM(region_normal.shape, jnp.float32),
            pltpu.SemaphoreType.DMA((22,)),
        ],
        flops=100 * unit,
    )(thirds, *raw)
    v, s, m, z_a, z_b = call(
        cross_kernel,
        "cross",
        (v_shape, s_shape, m_shape, z_shape, z_shape),
        [vm] * 8,
        {3: 0, 4: 1, 5: 2, 6: 3, 7: 4},
        flops=10 * unit,
    )(thirds, f_other, fault, v, s, m, z_a, z_b)
    z_a, z_b = pair_swaps(z_a, z_b, "gz")
    y_shape = f32(SLOTS * (nx + 8 + STRIP) + 8 + 16, width)
    v, s, m, fault, y_a, y_b = call(
        widen_kernel,
        "widen",
        (v_shape, s_shape, m_shape, fault_shape, y_shape, y_shape),
        [vm] * 8,
        {4: 0, 5: 1, 6: 2, 7: 3},
        [pltpu.VMEM((nx, width), jnp.float32)],
        flops=50 * unit,
    )(thirds, eighths, z_a, z_b, v, s, m, fault)
    v, s, m = call(
        rest_kernel,
        "rest",
        (v_shape, s_shape, m_shape),
        [vm] * 6,
        {3: 0, 4: 1, 5: 2},
        flops=50 * unit,
    )(thirds, z_a, z_b, v, s, m)
    y_shape = f32(3 * (nx + 8) + STRIP * 3 + 8, width)
    ahead_b = None
    out_shapes = (HBM((3, ny, nx, width), jnp.float32), HBM((6, ny, nx, width), jnp.float32))
    for step in range(STEPS):
        first, final = step == 0, step == STEPS - 1
        y_a, y_b = pair_swaps(y_a, y_b, "gy")
        v, s, *outs = call(
            functools.partial(inner_kernel, first, final),
            "inner",
            (v_shape, s_shape) + (out_shapes if final else ()),
            [vm] * 3,
            {1: 0, 2: 1},
            [pltpu.SemaphoreType.DMA((3 + 6 * ny,))] if final else [],
            flops=200 * unit,
            out_specs=[vm, vm] + ([hb, hb] if final else []),
        )(m, v, s)
        args = [eighths, y_a, y_b, m]
        args += ([] if first else [ahead_b]) + [v, s, fault] + outs
        at_state = len(args) - len(outs) - 3
        aliases = {at_state + k: k for k in range(3)}
        shapes, specs = [v_shape, s_shape, fault_shape], [vm, vm, vm]
        scratch = [pltpu.VMEM((2, 3, 2, high, width), jnp.float32)]
        scratch += [pltpu.VMEM((width, nx), jnp.float32), pltpu.VMEM((nx, width), jnp.float32)]
        if first:
            shapes.append(f32(2, rows, width))
            specs.append(vm)
        if final:
            shapes += [*out_shapes, jax.ShapeDtypeStruct((ny, width), jnp.float32)]
            specs += [hb, hb, vm]
            scratch.append(pltpu.SemaphoreType.DMA((3 * 3 + 6 * 4,)))
            aliases.update({at_state + 3: 3, at_state + 4: 4})
        else:
            shapes += [y_shape, y_shape]
            specs += [vm, vm]
        v, s, fault, *more = call(
            functools.partial(boundary_kernel, first, final),
            "boundary",
            shapes,
            [vm] * (len(args) - len(outs)) + [hb] * len(outs),
            aliases,
            scratch,
            flops=50 * unit,
            out_specs=specs,
        )(*args)
        if final:
            return tuple(more)
        if first:
            ahead_b, *more = more
        y_a, y_b = more


def solution(mesh):
    in_specs = (
        P(None, "gy", "gx", "gz"),
        P(None, "gy", "gx", "gz"),
        P("gy", "gx", "gz"),
        P("gy", "gx", "gz"),
        P("gy", "gx", "gz"),
        P("gy", "gx", "gz"),
        P("gy", "gx", "gz"),
        P("gy", "gx", "gz"),
        P(None, "gy", "gz"),
        P("gy", "gz"),
        P("gy", "gz"),
        P("gy", "gz"),
        P("gy", "gz"),
        P(),
        P(),
    )
    out_specs = (P(None, "gy", "gx", "gz"), P(None, "gy", "gx", "gz"), P("gy", "gz"))
    return jax.shard_map(local, mesh=mesh, in_specs=in_specs, out_specs=out_specs, check_vma=False)
```

```python
import functools

import jax
import jax.numpy as jnp
from jax import lax
from jax.experimental import pallas as pl
from jax.experimental.pallas import tpu as pltpu
from jax.sharding import PartitionSpec as P


STEPS = 3
NEWTON = 3
DT = 0.2

PAD = 8
HALO = 3
CROSS = 4
STRIP = 8

XX, YY, ZZ, YZ, XZ, XY = range(6)
ALONG_Y = (XY, YY, YZ)
B, C11, C13, C33, C44, C66 = range(6)
FIELDS = [("v", c) for c in range(3)] + [("s", c) for c in range(6)] + [("m", c) for c in range(6)]
PRE_Y, PRE_Z, MASK, STRENGTH, RATE, SLIP, OWN_B, OTHER_B = range(8)

VMEM = pltpu.MemorySpace.VMEM
HBM = pltpu.MemorySpace.HBM


def odd_on(axis):
    return lax.rem(lax.axis_index(axis), 2) == 1


def in_vmem():
    return pl.BlockSpec(memory_space=VMEM)


def in_hbm():
    return pl.BlockSpec(memory_space=HBM)


def roll(values, by):
    by = by % values.shape[-1]
    return values if by == 0 else pltpu.roll(values, by, values.ndim - 1)


def at(ref, field, tile, y, row):
    return ref[field, tile, y, pl.ds(PAD + row, 8), :]


def z_below(pair, lanes):
    one, two = roll(pair[0], 1), roll(pair[1], 1)
    first = lanes == 0
    return jnp.where(first, two, one), jnp.where(first, one, two)


def z_above(pair, lanes):
    one, two = roll(pair[0], -1), roll(pair[1], -1)
    last = lanes == pair[0].shape[-1] - 1
    return jnp.where(last, two, one), jnp.where(last, one, two)


def trial_tile(v, s, m, y, row, below, lanes):
    both = (0, 1)
    behind = {c: z_below([at(s, c, t, y, row) for t in both], lanes) for c in (XZ, YZ, ZZ)}
    out = []
    for t in both:
        own = {c: at(s, c, t, y, row) for c in range(6)}
        lower_x = {c: own[c] - at(s, c, t, y, row - 1) for c in (XX, XY, XZ)}
        if below is None:
            lower_y = {c: own[c] for c in ALONG_Y}
        else:
            lower_y = {c: own[c] - below(c, t) for c in ALONG_Y}
        scale = DT * m[B, t, y, pl.ds(row, 8), :]
        total = (
            lower_x[XX] + lower_y[XY] + (own[XZ] - behind[XZ][t]),
            lower_x[XY] + lower_y[YY] + (own[YZ] - behind[YZ][t]),
            lower_x[XZ] + lower_y[YZ] + (own[ZZ] - behind[ZZ][t]),
        )
        out.append([at(v, c, t, y, row) + scale * total[c] for c in range(3)])
    return out


def stress_tile(v, s, m, y, row, lanes, tiles=(0, 1)):
    both = (0, 1)
    own = [[at(v, c, t, y, row) for t in both] for c in range(3)]
    ahead = [z_above(own[c], lanes) for c in range(3)]
    for t in tiles:
        vx, vy, vz = own[0][t], own[1][t], own[2][t]
        over_x = [at(v, c, t, y, row + 1) for c in range(3)]
        over_y = [at(v, c, t, y + 1, row) for c in range(3)]
        exx, eyy, ezz = over_x[0] - vx, over_y[1] - vy, ahead[2][t] - vz
        c11, c13, c33, c44, c66 = (m[k, t, y, pl.ds(row, 8), :] for k in (C11, C13, C33, C44, C66))
        c12 = c11 - 2.0 * c66
        third = c13 * ezz
        change = {
            XX: c11 * exx + c12 * eyy + third,
            YY: c12 * exx + c11 * eyy + third,
            ZZ: c13 * (exx + eyy) + c33 * ezz,
            YZ: c44 * ((ahead[1][t] - vy) + (over_y[2] - vz)),
            XZ: c44 * ((ahead[0][t] - vx) + (over_x[2] - vz)),
            XY: c66 * ((over_y[0] - vx) + (over_x[1] - vy)),
        }
        for c, gain in change.items():
            s[c, t, y, pl.ds(PAD + row, 8), :] = at(s, c, t, y, row) + DT * gain


def lane_index(like):
    return lax.broadcasted_iota(jnp.int32, like, len(like) - 1)


SLOTS = 4


def strip_tile(up, down, eighths):
    packed = jnp.zeros_like(up[0])
    for start, pieces in ((0, up), (SLOTS, down)):
        for k, piece in enumerate(pieces):
            moved = roll(piece, STRIP * (start + k) + HALO)
            packed = jnp.where(eighths == start + k, moved, packed)
    return packed


def strip_take(packed, slot):
    return roll(packed, -(STRIP * slot + HALO))


def strip_send(strips, cross_tile, count, odd, y_a, y_b, base):
    turned = strips[...].T
    for j in range(0, STRIP * count, 8):
        up = turned[j : j + 8, :]
        down = turned[STRIP * SLOTS + j : STRIP * SLOTS + j + 8, :]
        y_a[base + j : base + j + 8, :] = jnp.where(odd, down, up)
        y_b[base + j : base + j + 8, :] = jnp.where(odd, up, down)
    other = roll(cross_tile, -STRIP * SLOTS)
    last = base + STRIP * count
    y_a[last : last + 8, :] = jnp.where(odd, other, cross_tile)
    y_b[last : last + 8, :] = jnp.where(odd, cross_tile, other)


def strip_receive(r_a, r_b, base, count, odd, turned, strips, lanes):
    turned[...] = jnp.zeros_like(turned)
    for j in range(0, STRIP * count, 8):
        from_a, from_b = r_a[base + j : base + j + 8, :], r_b[base + j : base + j + 8, :]
        turned[j : j + 8, :] = jnp.where(odd, from_a, from_b)
        start = STRIP * SLOTS + j
        turned[start : start + 8, :] = jnp.where(odd, from_b, from_a)
    strips[...] = turned[...].T
    last = base + STRIP * count
    from_a, from_b = r_a[last : last + 8, :], r_b[last : last + 8, :]
    low, high = jnp.where(odd, from_a, from_b), jnp.where(odd, from_b, from_a)
    return jnp.where(lanes < STRIP * SLOTS, low, roll(high, STRIP * SLOTS))


def field_ref(kind, v, s, m):
    return {"v": v, "s": s, "m": m}[kind]


def fields_per_plane(ny, width):
    return (width - 5) // HALO // ny


def z_slots(ny, width):
    per_plane = fields_per_plane(ny, width)
    slots = {}
    for f in range(len(FIELDS)):
        for y in range(ny):
            slots[f, y] = (f // per_plane, f % per_plane * ny + y)
    return slots, -(-len(FIELDS) // per_plane)


def row_tiles(nx):
    return [*range(0, nx, 8), cross_row(nx)]


def cross_row(nx):
    return nx + PAD


def packed_row(row, nx):
    return row if row < nx else nx


def edge_kernel(velocity, stress, *rest):
    raw_m, out, sem = rest[:6], rest[6], rest[7]
    ny, nx = velocity.shape[1:3]
    sources = [velocity.at[c] for c in range(3)] + [stress.at[c] for c in range(6)] + list(raw_m)
    for side, row in ((0, nx - CROSS), (1, 0)):

        @pl.when(lax.axis_index("gx") == side)
        def _(row=row):
            copies = []
            for f, source in enumerate(sources):
                for half in range(2):
                    part = source.at[pl.ds(half * (ny // 2), ny // 2), pl.ds(row, CROSS), :]
                    to = out.at[f, :, pl.ds(half * CROSS, CROSS), :]
                    copies.append(pltpu.make_async_copy(part, to, sem.at[2 * f + half]))
            for copy in copies:
                copy.start()
            for copy in copies:
                copy.wait()


def load_kernel(thirds, velocity, stress, *rest):
    raw_m, small = rest[:6], rest[6:13]
    v, s, m, fault, z_a, z_b = rest[13:19]
    pre, ids, mask, rate, slip, region_a, region_normal, sems = rest[19:]
    ny, nx, width = velocity.shape[1:]
    cross = cross_row(nx)
    big = {}
    for c in range(3):
        big["v", c] = (velocity.at[c], v.at[c, 0, pl.ds(0, ny), pl.ds(PAD, nx), :])
    for c in range(6):
        big["s", c] = (stress.at[c], s.at[c, 0, :, pl.ds(PAD, nx), :])
    for c in range(6):
        big["m", c] = (raw_m[c], m.at[c, 0, :, pl.ds(0, nx), :])
    big = {
        key: pltpu.make_async_copy(a, b, sems.at[k]) for k, (key, (a, b)) in enumerate(big.items())
    }
    held = (pre, ids, mask, rate, slip, region_a, region_normal)
    little = [
        pltpu.make_async_copy(a, b, sems.at[len(big) + k])
        for k, (a, b) in enumerate(zip(small, held))
    ]
    for copy in big.values():
        copy.start()
    for copy in little:
        copy.start()
    zeros = jnp.zeros((PAD, width), jnp.float32)
    for t in range(2):
        for y in range(ny):
            for c in (XX, XY, XZ):
                s[c, t, y, 0:PAD, :] = zeros
                s[c, t, y, cross : cross + PAD, :] = zeros
            for c in range(3):
                v[c, t, y, PAD + nx : PAD + nx + PAD, :] = zeros
                v[c, t, y, PAD + cross + 8 : 2 * PAD + cross + 8, :] = zeros

    per_plane = fields_per_plane(ny, width)
    odd = odd_on("gz")
    group = thirds[...]
    for plane in range(z_slots(ny, width)[1]):
        for key in FIELDS[plane * per_plane : (plane + 1) * per_plane]:
            big[key].wait()

        def pack(i, carry, plane=plane):
            for part in range(UNROLL):
                row = pl.multiple_of((i * UNROLL + part) * 8, 8)
                z_emit(z_a, z_b, odd, group, z_pieces(plane, v, s, m, row), plane, row)
            return carry

        lax.fori_loop(0, nx // (8 * UNROLL), pack, 0)
    for copy in little:
        copy.wait()
    kinds = ids[...]
    a_part = jnp.zeros((ny, width), jnp.float32)
    n_part = jnp.zeros((ny, width), jnp.float32)
    for k in range(region_a.shape[0]):
        a_part = jnp.where(kinds == k, region_a[k], a_part)
        n_part = jnp.where(kinds == k, region_normal[k], n_part)
    fault[PRE_Y, 0, 0:ny, :] = pre[0]
    fault[PRE_Z, 0, 0:ny, :] = pre[1]
    fault[MASK, 0, 0:ny, :] = mask[...].astype(jnp.float32)
    fault[STRENGTH, 0, 0:ny, :] = a_part * n_part
    fault[RATE, 0, 0:ny, :] = rate[...]
    fault[SLIP, 0, 0:ny, :] = slip[...]


UNROLL = 8


def z_emit(z_a, z_b, odd, group, pieces, plane, row):
    up = jnp.zeros_like(pieces[0][1])
    down = up
    for pos, piece in pieces:
        moved = roll(piece, HALO * pos + HALO)
        up = jnp.where(group == pos, moved, up)
        down = jnp.where(group == pos + 1, moved, down)
    z_a[plane, pl.ds(row, 8), :] = jnp.where(odd, down, up)
    z_b[plane, pl.ds(row, 8), :] = jnp.where(odd, up, down)


def z_pieces(plane, v, s, m, row):
    ny, width = m.shape[2], m.shape[4]
    per_plane = fields_per_plane(ny, width)
    pieces = []
    for f, (kind, c) in enumerate(FIELDS[plane * per_plane : (plane + 1) * per_plane]):
        shift = 0 if kind == "m" else PAD
        ref = field_ref(kind, v, s, m)
        for y in range(ny):
            pieces.append((f * ny + y, ref[c, 0, y, pl.ds(row + shift, 8), :]))
    return pieces


def cross_kernel(thirds, f_other, fault, v_in, s_in, m_in, za_in, zb_in, v, s, m, z_a, z_b):
    ny, width = m.shape[2], m.shape[4]
    nx = z_a.shape[1] - 16
    cross = cross_row(nx)
    odd = odd_on("gz")
    group = thirds[...]
    planes = z_slots(ny, width)[1]
    rows = lax.broadcasted_iota(jnp.int32, (8, width), 0)
    minus = lax.axis_index("gx") == 0
    keep = jnp.where(minus, 7 - rows, rows) >= 8 - CROSS
    for f, (kind, c) in enumerate(FIELDS):
        shift = 0 if kind == "m" else PAD
        ref = field_ref(kind, v, s, m)
        for y in range(ny // 2):
            tile = f_other[f, y]
            turned = pltpu.roll(tile, CROSS, 0)
            ref[c, 0, y, cross + shift : cross + shift + 8, :] = jnp.where(
                keep, jnp.where(minus, tile, turned), 0.0
            )
            ref[c, 0, y + ny // 2, cross + shift : cross + shift + 8, :] = jnp.where(
                keep, jnp.where(minus, turned, tile), 0.0
            )
    for plane in range(planes):
        z_emit(z_a, z_b, odd, group, z_pieces(plane, v, s, m, cross), plane, nx)
    z_emit(z_a, z_b, odd, group, [(k, fault[k, 0, 0:8, :]) for k in range(6)], 0, nx + 8)
    zeros = jnp.zeros((8, width), jnp.float32)
    for plane in range(1, planes):
        z_a[plane, pl.ds(nx + 8, 8), :] = zeros
        z_b[plane, pl.ds(nx + 8, 8), :] = zeros


def write_messages(v, s, buoyancy, eighths, odd, y_a, y_b, strips, nx):
    last = s.shape[2] - 1
    span = nx + 8
    count = 3 if buoyancy is None else SLOTS

    def pieces(t, row):
        up = [at(s, c, t, last, row) for c in ALONG_Y]
        down = [at(v, c, t, 0, row) for c in range(3)]
        if t == 1 and buoyancy is not None:
            up.append(buoyancy[B, t, 0, pl.ds(row, 8), :])
            down.append(up[-1])
        return up, down

    for row in row_tiles(nx):
        up, down = pieces(0, row)
        for k in range(3):
            to = pl.ds(k * span + packed_row(row, nx), 8)
            y_a[to, :] = jnp.where(odd, down[k], up[k])
            y_b[to, :] = jnp.where(odd, up[k], down[k])
        tile = strip_tile(*pieces(1, row), eighths)
        if row < nx:
            strips[row : row + 8, :] = tile
    strip_send(strips, tile, count, odd, y_a, y_b, 3 * span)


def partial_trials(v, s, m, nx, lanes):
    for row in row_tiles(nx):
        new = trial_tile(v, s, m, 0, row, None, lanes)
        for t in range(2):
            for c in range(3):
                v[c, t, 0, pl.ds(PAD + row, 8), :] = new[t][c]


class ZHalo:
    def __init__(self, odd, group, r_a, r_b, planes):
        self.odd, self.group, self.r_a, self.r_b, self.planes = odd, group, r_a, r_b, planes

    def take(self, row, wanted):
        for plane in range(self.planes):
            chosen = [(pos, store) for (p, pos), store in wanted if p == plane]
            if chosen:
                from_a = self.r_a[plane, pl.ds(row, 8), :]
                from_b = self.r_b[plane, pl.ds(row, 8), :]
                low = jnp.where(self.odd, from_a, from_b)
                high = jnp.where(self.odd, from_b, from_a)
                for pos, store in chosen:
                    both = jnp.where(self.group == pos, low, high)
                    store(roll(both, -(HALO * pos + HALO)))


def needed_first(kind, c, y, ny):
    if y == 0:
        return kind != "m" or c == B
    return y == ny - 1 and kind == "s" and c in ALONG_Y


def unpack_fields(halo, v, s, m, nx, first):
    ny, width = m.shape[2], m.shape[4]
    slots = z_slots(ny, width)[0]

    def store_to(ref, c, y, row):
        def store(value):
            ref[c, 1, y, pl.ds(row, 8), :] = value

        return store

    def fields(row):
        wanted = []
        for f, (kind, c) in enumerate(FIELDS):
            shift = 0 if kind == "m" else PAD
            ref = field_ref(kind, v, s, m)
            for y in range(ny):
                if needed_first(kind, c, y, ny) == first:
                    wanted.append((slots[f, y], store_to(ref, c, y, row + shift)))
        return wanted

    def unpack(i, carry):
        for part in range(UNROLL):
            row = pl.multiple_of((i * UNROLL + part) * 8, 8)
            halo.take(row, fields(row))
        return carry

    lax.fori_loop(0, nx // (8 * UNROLL), unpack, 0)
    halo.take(nx, fields(cross_row(nx)))


def rest_kernel(thirds, r_a, r_b, v_in, s_in, m_in, v, s, m):
    nx = r_a.shape[1] - 16
    planes = z_slots(m.shape[2], m.shape[4])[1]
    halo = ZHalo(odd_on("gz"), thirds[...], r_a, r_b, planes)
    unpack_fields(halo, v, s, m, nx, False)


def widen_kernel(
    thirds, eighths, r_a, r_b, v_in, s_in, m_in, f_in, v, s, m, fault, y_a, y_b, strips
):
    ny, width = m.shape[2], m.shape[4]
    nx = r_a.shape[1] - 16
    planes = z_slots(ny, width)[1]
    odd_y = odd_on("gy")
    lanes = lane_index((8, width))
    halo = ZHalo(odd_on("gz"), thirds[...], r_a, r_b, planes)
    unpack_fields(halo, v, s, m, nx, True)

    def store_fault(k):
        def store(value):
            fault[k, 1, 0:8, :] = value

        return store

    halo.take(nx + 8, [((0, k), store_fault(k)) for k in range(6)])
    partial_trials(v, s, m, nx, lanes)
    write_messages(v, s, m, eighths[...], odd_y, y_a, y_b, strips, nx)
    for t in range(2):
        for k in range(8):
            line = fault[min(k, 5), t, 0:1, :]
            row = 3 * (nx + 8) + SLOTS * STRIP + 8 + 8 * t + k
            y_a[row : row + 1, :] = line
            y_b[row : row + 1, :] = line


def inner_kernel(first, final, m, v_in, s_in, v, s, *outs):
    ny, width = m.shape[2], m.shape[4]
    nx = m.shape[3] - 16
    lanes = lane_index((8, width))

    if not first:

        def ends(y, carry):
            for row in (0, nx - 8, cross_row(nx)):
                stress_tile(v, s, m, y, row, lanes)
            return carry

        lax.fori_loop(1, ny - 1, ends, 0)

    def trials(y, carry):
        for row in row_tiles(nx):
            new = trial_tile(
                v, s, m, y, row, lambda c, t, row=row: at(s, c, t, y - 1, row), lanes
            )
            for t in range(2):
                for c in range(3):
                    v[c, t, y, pl.ds(PAD + row, 8), :] = new[t][c]
        return carry

    lax.fori_loop(1, ny, trials, 0)
    copies = []
    if final:
        new_v, new_s, sems = outs
        for c in range(3):
            part = v.at[c, 0, pl.ds(1, ny - 1), pl.ds(PAD + 8, nx - 16), :]
            to = new_v.at[c, pl.ds(1, ny - 1), pl.ds(8, nx - 16), :]
            copies.append(pltpu.make_async_copy(part, to, sems.at[c]))
            copies[-1].start()

    def out_copy(c, y):
        part = s.at[c, 0, y, pl.ds(PAD + 8, nx - 16), :]
        to = new_s.at[c, y, pl.ds(8, nx - 16), :]
        return pltpu.make_async_copy(part, to, sems.at[3 + c * ny + y])

    def stresses(y, carry):
        for row in range(8, nx - 8, 8):
            stress_tile(v, s, m, y, row, lanes, (0,) if final else (0, 1))
        if final:
            for c in range(6):
                out_copy(c, y).start()
        return carry

    lax.fori_loop(1, ny - 1, stresses, 0)
    if final:
        for copy in copies:
            copy.wait()

        def wait(y, carry):
            for c in range(6):
                out_copy(c, y).wait()
            return carry

        lax.fori_loop(1, ny - 1, wait, 0)


def boundary_kernel(first, final, eighths, *refs):
    refs = list(refs)

    def pop(n):
        out = refs[:n]
        del refs[:n]
        return out

    if first:
        b_a, b_b = pop(2)
    r_a, r_b, m = pop(3)
    if not first:
        (ahead_b,) = pop(1)
    pop(3)
    if final:
        pop(2)
    v, s, fault = pop(3)
    if first:
        (ahead_b,) = pop(1)
    if final:
        new_v, new_s, slip_out, rows, turned, strips, sems = refs
    else:
        y_a, y_b, rows, turned, strips = refs
    ny, width = m.shape[2], m.shape[4]
    nx = m.shape[3] - 16
    cross = cross_row(nx)
    span = nx + 8
    odd = odd_on("gy")
    lanes = lane_index((8, width))
    halos = eighths[...]

    count = SLOTS if first else 3
    cross_tile = strip_receive(r_a, r_b, 3 * span, count, odd, turned, strips, lanes)

    def received(row):
        at_row = packed_row(row, nx)
        from_a = [r_a[pl.ds(k * span + at_row, 8), :] for k in range(3)]
        from_b = [r_b[pl.ds(k * span + at_row, 8), :] for k in range(3)]
        low = [jnp.where(odd, a, b) for a, b in zip(from_a, from_b)]
        high = [jnp.where(odd, b, a) for a, b in zip(from_a, from_b)]
        packed = strips[row : row + 8, :] if row < nx else cross_tile
        return low, high, packed

    if first:
        for t in range(2):
            to = pl.ds(3 * span + SLOTS * STRIP + 8 + 8 * t, 8)
            lines = jnp.where(odd, r_b[to, :], r_a[to, :])
            for k in range(6):
                fault[k, t, ny : ny + 1, :] = lines[k : k + 1, :]
    for row in row_tiles(nx):
        low, high, packed = received(row)
        if first:
            from_a, from_b = b_a[pl.ds(row, 8), :], b_b[pl.ds(row, 8), :]
            ahead_b[0, pl.ds(row, 8), :] = jnp.where(odd, from_b, from_a)
            ahead_b[1, pl.ds(row, 8), :] = strip_take(packed, SLOTS + 3)
        for t in range(2):
            scale = DT * m[B, t, 0, pl.ds(row, 8), :]
            scale_ahead = DT * ahead_b[t, pl.ds(row, 8), :]
            for c in range(3):
                low_c = low[c] if t == 0 else strip_take(packed, c)
                high_c = high[c] if t == 0 else strip_take(packed, SLOTS + c)
                v[c, t, 0, pl.ds(PAD + row, 8), :] = at(v, c, t, 0, row) - scale * low_c
                v[c, t, ny, pl.ds(PAD + row, 8), :] = high_c - scale_ahead * at(
                    s, ALONG_Y[c], t, ny - 1, row
                )

    places = ((0, (nx - 1, cross)), (1, (0, cross + 7)))
    for side, pair in places:

        @pl.when(lax.axis_index("gx") == side)
        def _(pair=pair):
            for which, row in enumerate(pair):
                for t in range(2):
                    for y in range(ny + 1):
                        for c in range(3):
                            rows[which, c, t, y : y + 1, :] = v[
                                c, t, y, PAD + row : PAD + row + 1, :
                            ]
                        if first:
                            if y < ny:
                                line = m[B, t, y, row : row + 1, :]
                            else:
                                line = ahead_b[t, row : row + 1, :]
                            fault[OWN_B + which, t, y : y + 1, :] = line

    minus = lax.axis_index("gx") == 0
    sign = jnp.where(minus, DT, -DT)
    for t in range(2):
        for half in range(0, fault.shape[2], 8):
            part = slice(half, half + 8)
            own = [rows[0, c, t, part, :] for c in range(3)]
            other = [rows[1, c, t, part, :] for c in range(3)]
            par = [fault[k, t, part, :] for k in range(8)]
            m_side = [jnp.where(minus, a, b) for a, b in zip(own, other)]
            p_side = [jnp.where(minus, b, a) for a, b in zip(own, other)]
            m_b = jnp.where(minus, par[OWN_B], par[OTHER_B])
            p_b = jnp.where(minus, par[OTHER_B], par[OWN_B])
            traction, slip = friction(m_side, p_side, m_b, p_b, par)
            fault[SLIP, t, part, :] = slip
            for c in range(3):
                rows[0, c, t, part, :] = own[c] + sign * par[OWN_B] * traction[c]
                rows[1, c, t, part, :] = other[c] - sign * par[OTHER_B] * traction[c]
    for y in (0, ny - 1):
        for row in range(8, nx - 8, 8):
            stress_tile(v, s, m, y, row, lanes, (0,) if final else (0, 1))
    for side, pair in places:

        @pl.when(lax.axis_index("gx") == side)
        def _(pair=pair):
            for which, row in enumerate(pair):
                for c in range(3):
                    for t in range(2):
                        for y in range(ny + 1):
                            v[c, t, y, PAD + row : PAD + row + 1, :] = rows[
                                which, c, t, y : y + 1, :
                            ]

    if final:
        copies = []

        def send(pairs):
            for part, to in pairs:
                copies.append(pltpu.make_async_copy(part, to, sems.at[len(copies)]))
                copies[-1].start()

        def planes(ref, out, y, first_row, rows):
            part = ref.at[:, 0, y, pl.ds(PAD + first_row, rows), :]
            return part, out.at[:, y, pl.ds(first_row, rows), :]

        def edges(ref, out, inside, row):
            part = ref.at[:, 0, pl.ds(1, inside), pl.ds(PAD + row, 8), :]
            return part, out.at[:, pl.ds(1, inside), pl.ds(row, 8), :]

        send([planes(s, new_s, y, 8, nx - 16) for y in (0, ny - 1)])
        send([planes(v, new_v, 0, 0, nx)])
        send([edges(v, new_v, ny - 1, row) for row in (0, nx - 8)])
    tiles = (0,) if final else (0, 1)
    for y in (0, ny - 1):
        for row in (0, nx - 8) if final else (0, nx - 8, cross):
            stress_tile(v, s, m, y, row, lanes, tiles)
    if not final:
        partial_trials(v, s, m, nx, lanes)
        write_messages(v, s, None, halos, odd, y_a, y_b, strips, nx)
        return

    send([planes(s, new_s, y, row, 8) for y in (0, ny - 1) for row in (0, nx - 8)])

    def ends(y, carry):
        for row in (0, nx - 8):
            stress_tile(v, s, m, y, row, lanes, tiles)
        return carry

    lax.fori_loop(1, ny - 1, ends, 0)
    send([edges(s, new_s, ny - 2, row) for row in (0, nx - 8)])
    slip_out[...] = fault[SLIP, 0, 0:ny, :]
    for copy in copies:
        copy.wait()


def inverse_sinh(values):
    size = jnp.abs(values)
    sign = jnp.where(values > 0.0, 1.0, jnp.where(values < 0.0, -1.0, 0.0))
    return sign * jnp.log(size + jnp.sqrt(size * size + 1.0))


def friction(minus_side, plus_side, minus_b, plus_b, par):
    total = DT * (minus_b + plus_b)
    impedance = 1.0 / jnp.where(total > 0.0, total, 1.0)
    jump = [p - q for p, q in zip(plus_side, minus_side)]
    locked_y = par[PRE_Y] + impedance * jump[1]
    locked_z = par[PRE_Z] + impedance * jump[2]
    magnitude = jnp.sqrt(locked_y * locked_y + locked_z * locked_z + 1.0)
    rate, strength, slip = par[RATE], par[STRENGTH], par[SLIP]
    for _ in range(NEWTON):
        scaled = rate * slip
        residual = magnitude - impedance * slip - strength * inverse_sinh(scaled)
        tangent = -impedance - strength * rate / jnp.sqrt(1.0 + scaled * scaled)
        slip = slip - residual / tangent
    slip = slip * par[MASK]
    retained = 1.0 - impedance * slip / magnitude
    traction = (
        impedance * jump[0],
        retained * locked_y - par[PRE_Y],
        retained * locked_z - par[PRE_Z],
    )
    return traction, slip


def f32(*shape):
    return VMEM(shape, jnp.float32)


def call(kernel, outs, in_specs, aliases, scratch=(), flops=0, out_specs=None):
    return pl.pallas_call(
        kernel,
        out_shape=tuple(outs),
        in_specs=in_specs,
        out_specs=tuple(out_specs or [in_vmem() for _ in outs]),
        input_output_aliases=aliases,
        scratch_shapes=list(scratch),
        compiler_params=pltpu.CompilerParams(vmem_limit_bytes=8 << 20),
        cost_estimate=pl.CostEstimate(flops=flops, bytes_accessed=0, transcendentals=0),
    )


def pair_swaps(a, b, axis):
    size = lax.axis_size(axis)
    out = []
    for value, start in ((a, 0), (b, 1)):
        pairs = []
        for i in range(start, size - 1, 2):
            pairs += [(i, i + 1), (i + 1, i)]
        out.append(lax.ppermute(value, axis, pairs))
    return out


def local(
    velocity,
    stress,
    buoyancy,
    stiff_xx,
    stiff_xz,
    stiff_zz,
    shear_vert,
    shear_horiz,
    prestress,
    fault_mask,
    region_ids,
    inverse_rate,
    slip_prev,
    region_a,
    region_normal,
):
    ny, nx, width = buoyancy.shape
    assert nx == width
    lanes = jnp.broadcast_to(jnp.arange(width, dtype=jnp.int32), (8, width))
    thirds, eighths = lanes // HALO, lanes // STRIP
    rows = cross_row(nx) + 8
    high = 8 * ((ny + 1 + 7) // 8)
    v_shape = f32(3, 2, ny + 1, rows + 2 * PAD, width)
    s_shape = f32(6, 2, ny, rows + 2 * PAD, width)
    m_shape = f32(6, 2, ny, rows, width)
    fault_shape = f32(8, 2, high, width)
    planes = z_slots(ny, width)[1]
    z_shape = f32(planes, nx + 16, width)
    unit = ny * nx * width
    vm, hb = in_vmem(), in_hbm()
    raw = [velocity, stress, buoyancy, stiff_xx, stiff_xz, stiff_zz, shear_vert, shear_horiz]
    raw += [prestress, region_ids, fault_mask, inverse_rate, slip_prev, region_a, region_normal]
    raw = [pltpu.with_memory_space_constraint(k, HBM) for k in raw]

    f_shape = f32(len(FIELDS), ny // 2, 8, width)
    (f_own,) = call(
        edge_kernel,
        (f_shape,),
        [hb] * 8,
        {},
        [pltpu.SemaphoreType.DMA((2 * len(FIELDS),))],
        flops=unit,
    )(*raw[:8])
    f_other = lax.ppermute(f_own, "gx", [(i, i ^ 1) for i in range(lax.axis_size("gx"))])
    v, s, m, fault, z_a, z_b = call(
        load_kernel,
        (v_shape, s_shape, m_shape, fault_shape, z_shape, z_shape),
        [vm] + [hb] * 15,
        {},
        [
            pltpu.VMEM(prestress.shape, jnp.float32),
            pltpu.VMEM(region_ids.shape, jnp.int32),
            pltpu.VMEM(fault_mask.shape, jnp.int32),
            pltpu.VMEM(inverse_rate.shape, jnp.float32),
            pltpu.VMEM(slip_prev.shape, jnp.float32),
            pltpu.SMEM(region_a.shape, jnp.float32),
            pltpu.SMEM(region_normal.shape, jnp.float32),
            pltpu.SemaphoreType.DMA((22,)),
        ],
        flops=100 * unit,
    )(thirds, *raw)
    v, s, m, z_a, z_b = call(
        cross_kernel,
        (v_shape, s_shape, m_shape, z_shape, z_shape),
        [vm] * 8,
        {3: 0, 4: 1, 5: 2, 6: 3, 7: 4},
        flops=10 * unit,
    )(thirds, f_other, fault, v, s, m, z_a, z_b)
    z_a, z_b = pair_swaps(z_a, z_b, "gz")
    b_a, b_b = pair_swaps(m[B, 0, 0], m[B, 0, 0], "gy")
    y_shape = f32(3 * (nx + 8) + SLOTS * STRIP + 8 + 16, width)
    v, s, m, fault, y_a, y_b = call(
        widen_kernel,
        (v_shape, s_shape, m_shape, fault_shape, y_shape, y_shape),
        [vm] * 8,
        {4: 0, 5: 1, 6: 2, 7: 3},
        [pltpu.VMEM((nx, width), jnp.float32)],
        flops=50 * unit,
    )(thirds, eighths, z_a, z_b, v, s, m, fault)
    v, s, m = call(
        rest_kernel, (v_shape, s_shape, m_shape), [vm] * 6, {3: 0, 4: 1, 5: 2}, flops=50 * unit
    )(thirds, z_a, z_b, v, s, m)
    y_shape = f32(3 * (nx + 8) + STRIP * 3 + 8, width)
    ahead_b = None
    out_shapes = (HBM((3, ny, nx, width), jnp.float32), HBM((6, ny, nx, width), jnp.float32))
    for step in range(STEPS):
        first, final = step == 0, step == STEPS - 1
        y_a, y_b = pair_swaps(y_a, y_b, "gy")
        v, s, *outs = call(
            functools.partial(inner_kernel, first, final),
            (v_shape, s_shape) + (out_shapes if final else ()),
            [vm] * 3,
            {1: 0, 2: 1},
            [pltpu.SemaphoreType.DMA((3 + 6 * ny,))] if final else [],
            flops=200 * unit,
            out_specs=[vm, vm] + ([hb, hb] if final else []),
        )(m, v, s)
        args = [eighths] + ([b_a, b_b] if first else []) + [y_a, y_b, m]
        args += ([] if first else [ahead_b]) + [v, s, fault] + outs
        at_state = len(args) - len(outs) - 3
        aliases = {at_state + k: k for k in range(3)}
        shapes, specs = [v_shape, s_shape, fault_shape], [vm, vm, vm]
        scratch = [pltpu.VMEM((2, 3, 2, high, width), jnp.float32)]
        scratch += [pltpu.VMEM((width, nx), jnp.float32), pltpu.VMEM((nx, width), jnp.float32)]
        if first:
            shapes.append(f32(2, rows, width))
            specs.append(vm)
        if final:
            shapes += [*out_shapes, jax.ShapeDtypeStruct((ny, width), jnp.float32)]
            specs += [hb, hb, vm]
            scratch.append(pltpu.SemaphoreType.DMA((11,)))
            aliases.update({at_state + 3: 3, at_state + 4: 4})
        else:
            shapes += [y_shape, y_shape]
            specs += [vm, vm]
        v, s, fault, *more = call(
            functools.partial(boundary_kernel, first, final),
            shapes,
            [vm] * (len(args) - len(outs)) + [hb] * len(outs),
            aliases,
            scratch,
            flops=50 * unit,
            out_specs=specs,
        )(*args)
        if final:
            return tuple(more)
        if first:
            ahead_b, *more = more
        y_a, y_b = more


def solution(mesh):
    in_specs = (
        P(None, "gy", "gx", "gz"),
        P(None, "gy", "gx", "gz"),
        P("gy", "gx", "gz"),
        P("gy", "gx", "gz"),
        P("gy", "gx", "gz"),
        P("gy", "gx", "gz"),
        P("gy", "gx", "gz"),
        P("gy", "gx", "gz"),
        P(None, "gy", "gz"),
        P("gy", "gz"),
        P("gy", "gz"),
        P("gy", "gz"),
        P("gy", "gz"),
        P(),
        P(),
    )
    out_specs = (P(None, "gy", "gx", "gz"), P(None, "gy", "gx", "gz"), P("gy", "gz"))

    return jax.shard_map(local, mesh=mesh, in_specs=in_specs, out_specs=out_specs, check_vma=False)
```
